256 devices in a mesh: gx: 16 (over z, y_hi), gy: 4 (over y_lo, core), gz: 4 (over x).
Axes of the slice: x: 4, y: 4 (y_hi: 2, y_lo: 2; y = y_hi * 2 + y_lo), z: 8, core: 2. Of those that a mesh axis runs over, the one named last changes fastest.
Arguments:
- node_feat: bfloat16 [128, 32, 32, 128], P('gx', 'gy', 'gz'), may hold values from -6 to 6
- edge_feat: bfloat16 [4, 128, 32, 32, 128], P(None, 'gx', 'gy', 'gz'), may hold values from -6 to 6
- copies: int32 [128, 32, 32], P('gx', 'gy', 'gz'), may hold values from 1 to 8
- offsets: int32 [4, 3], replicated, may hold values from -1 to 1
- w_edge_in: bfloat16 [384, 128], replicated, may hold values from -0.3125 to 0.3125
- w_edge_out: bfloat16 [128, 128], replicated, may hold values from -0.5 to 0.5
- w_node_in: bfloat16 [256, 128], replicated, may hold values from -0.375 to 0.375
- w_node_out: bfloat16 [128, 128], replicated, may hold values from -0.5 to 0.5
- node_cot: bfloat16 [128, 32, 32, 128], P('gx', 'gy', 'gz'), may hold values from -6 to 6
Outputs:
- node_grad: bfloat16 [128, 32, 32, 128], P('gx', 'gy', 'gz')
- edge_grad: bfloat16 [4, 128, 32, 32, 128], P(None, 'gx', 'gy', 'gz')
- grad_edge_in: float32 [384, 128], replicated
- grad_edge_out: float32 [128, 128], replicated
- grad_node_in: float32 [256, 128], replicated
- grad_node_out: float32 [128, 128], replicated
The draws below stay inside these ranges and needn't reach their ends.
Inputs may be any that keep to these rules, and one draw needn't show every extreme that they name: `offsets`: each row is one lattice offset, its three entries along the first, second and third dimension.
All inputs are finite; a program needn't handle non-finite values.
Results may differ from the reference program's by a relative error of at most 0.0068.
Values sent between devices are 32-bit elements; how exact they have to be, the bound alone decides.
No kernel may reach another device: no remote copies, remote signals or barrier semaphores. Data moves between devices by JAX's collectives and lax.ppermute only.
A program may use at most 64 MiB of HBM per device.

```python
import math
import jax
import jax.numpy as jnp
from jax import lax

WIDTH = 128
KINDS = 4
BRICK = 8
NX = 128
NY = 32
NZ = 32
N_GX = 16
N_GY = 4
N_GZ = 4


def place_ends(values, rng, low, high):
    longest = values.shape.index(max(values.shape))
    spots = []
    for shift in (0, 1):
        where = [jax.random.randint(jax.random.fold_in(rng, axis), (), 0, length) for axis, length in enumerate(values.shape)]
        where[longest] = (where[longest] + shift) % values.shape[longest]
        spots.append(tuple(where))
    return values.at[spots[0]].set(low).at[spots[1]].set(high)


def block_levels(own_key, extent, shards, least, top_value):
    level, own = 1.0, jax.random.fold_in(own_key, 6)
    for dim, blocks in shards:
        heights = jnp.exp(jax.random.uniform(jax.random.fold_in(own, dim), (blocks,), jnp.float32, least / len(shards), top_value / len(shards)))
        level = level * jnp.repeat(heights, extent[dim] // blocks).reshape([-1 if axis == dim else 1 for axis in range(len(extent))])
    return level


def bell_draw(rng, dims, scale, most, cuts=(), held_as=jnp.bfloat16):
    values = jax.random.normal(rng, dims, jnp.float32) * scale
    if len(cuts) > 0:
        values = block_levels(rng, dims, cuts, -0.22, 0.18) * values
    return jnp.clip(values, min=-most, max=most).astype(held_as)


def setup_inputs(seed: int = 0) -> dict:
    keys = jax.random.split(jax.random.key(seed), 10)
    node_feat = bell_draw(keys[0], (NX, NY, NZ, WIDTH), 1.0, 6.0, ((0, 16), (1, 4), (2, 4)))
    edge_feat = bell_draw(keys[1], (KINDS, NX, NY, NZ, WIDTH), 1.0, 6.0, ((1, 16), (2, 4), (3, 4)))
    copies = place_ends(jax.random.randint(keys[2], (NX, NY, NZ), 1, 9), jax.random.fold_in(keys[2], 1), 1, 8).astype(jnp.int32)
    offsets = place_ends(jax.random.randint(keys[3], (KINDS, 3), -1, 2), jax.random.fold_in(keys[3], 1), -1, 1).astype(jnp.int32)
    w_edge_in = bell_draw(keys[4], (3 * WIDTH, WIDTH), (3 * WIDTH) ** -0.5, 0.3125)
    w_edge_out = bell_draw(keys[5], (WIDTH, WIDTH), WIDTH ** -0.5, 0.5)
    w_node_in = bell_draw(keys[6], (2 * WIDTH, WIDTH), (2 * WIDTH) ** -0.5, 0.375)
    w_node_out = bell_draw(keys[7], (WIDTH, WIDTH), WIDTH ** -0.5, 0.5)
    node_cot = bell_draw(keys[8], (NX, NY, NZ, WIDTH), 1.0, 6.0, ((0, 16), (1, 4), (2, 4)))
    return dict(node_feat=node_feat, edge_feat=edge_feat, copies=copies, offsets=offsets, w_edge_in=w_edge_in, w_edge_out=w_edge_out, w_node_in=w_node_in, w_node_out=w_node_out, node_cot=node_cot)


def neighbour_valid(offset, brick):
    coords = jnp.arange(brick, dtype=jnp.int32)
    inside = [(coords + offset[which] >= 0) & (coords + offset[which] < brick) for which in range(3)]
    joined = inside[0][:, None, None] & inside[1][None, :, None] & inside[2][None, None, :]
    return joined.astype(jnp.float32).reshape(brick * brick * brick, 1)

def moved_view(field, corner):
    padded = jnp.pad(field, ((1, 1), (1, 1), (1, 1), (0, 0)))
    start = (1 + corner).astype(jnp.int32)
    return lax.dynamic_slice(padded, (start[0], start[1], start[2], jnp.int32(0)), field.shape)

def silu_slope(preact):
    sigma = jax.nn.sigmoid(preact)
    return sigma * (1.0 + preact * (1.0 - sigma))

def outer_product(left, right):
    return lax.dot_general(left, right, (((0,), (0,)), ((), ())), preferred_element_type=jnp.float32)

def edge_preact(sender, receiver, feature, w_edge_in, width):
    total = jnp.dot(sender, w_edge_in[:width], preferred_element_type=jnp.float32)
    total = total + jnp.dot(receiver, w_edge_in[width:2 * width], preferred_element_type=jnp.float32)
    return total + jnp.dot(feature, w_edge_in[2 * width:], preferred_element_type=jnp.float32)

def edge_messages(nodes, edges, offsets, w_edge_in, w_edge_out):
    brick = nodes.shape[0]
    width = nodes.shape[3]
    count = brick * brick * brick
    receiver = nodes.reshape(count, width)
    total = jnp.zeros((count, width), jnp.float32)
    preacts = []
    hiddens = []
    for kind_index in range(edges.shape[0]):
        offset = offsets[kind_index]
        sender = moved_view(nodes, offset).reshape(count, width)
        preact = edge_preact(sender, receiver, edges[kind_index].reshape(count, width), w_edge_in, width)
        hidden = jax.nn.silu(preact).astype(jnp.bfloat16)
        message = jnp.dot(hidden, w_edge_out, preferred_element_type=jnp.float32)
        total = total + neighbour_valid(offset, brick) * message
        preacts.append(preact)
        hiddens.append(hidden)
    return (total.reshape(nodes.shape), jnp.stack(preacts), jnp.stack(hiddens))

def node_backward(nodes, summed, copies, node_cot, w_node_in, w_node_out):
    width = nodes.shape[3]
    count = nodes.shape[0] * nodes.shape[1] * nodes.shape[2]
    receiver = nodes.reshape(count, width)
    scale = copies.reshape(count, 1).astype(jnp.float32)
    gathered = (summed.reshape(count, width) / scale).astype(jnp.bfloat16)
    preact = jnp.dot(receiver, w_node_in[:width], preferred_element_type=jnp.float32)
    preact = preact + jnp.dot(gathered, w_node_in[width:], preferred_element_type=jnp.float32)
    hidden = jax.nn.silu(preact).astype(jnp.bfloat16)
    upstream = node_cot.reshape(count, width)
    grad_out = outer_product(hidden, upstream)
    slope = (jnp.dot(upstream, w_node_out.T, preferred_element_type=jnp.float32) * silu_slope(preact)).astype(jnp.bfloat16)
    grad_in = jnp.concatenate([outer_product(receiver, slope), outer_product(gathered, slope)], axis=0)
    to_nodes = jnp.dot(slope, w_node_in[:width].T, preferred_element_type=jnp.float32)
    to_agg = jnp.dot(slope, w_node_in[width:].T, preferred_element_type=jnp.float32) / scale
    return (to_nodes.reshape(nodes.shape), to_agg.reshape(nodes.shape), grad_in, grad_out)

def edge_backward(nodes, edges, offsets, incoming, w_edge_in, w_edge_out, preacts, hiddens):
    brick = nodes.shape[0]
    width = nodes.shape[3]
    count = brick * brick * brick
    receiver = nodes.reshape(count, width)
    arriving = incoming.reshape(count, width)
    grad_in = jnp.zeros((3 * width, width), jnp.float32)
    grad_out = jnp.zeros((width, width), jnp.float32)
    to_nodes = jnp.zeros((count, width), jnp.float32)
    sent_back = jnp.zeros(nodes.shape, jnp.float32)
    edge_grads = []
    for kind_index in range(edges.shape[0]):
        offset = offsets[kind_index]
        sender = moved_view(nodes, offset).reshape(count, width)
        feature = edges[kind_index].reshape(count, width)
        message_cot = (neighbour_valid(offset, brick) * arriving).astype(jnp.bfloat16)
        grad_out = grad_out + outer_product(hiddens[kind_index], message_cot)
        slope = jnp.dot(message_cot, w_edge_out.T, preferred_element_type=jnp.float32) * silu_slope(preacts[kind_index])
        slope = slope.astype(jnp.bfloat16)
        grad_in = grad_in + jnp.concatenate([outer_product(sender, slope), outer_product(receiver, slope), outer_product(feature, slope)], axis=0)
        to_nodes = to_nodes + jnp.dot(slope, w_edge_in[width:2 * width].T, preferred_element_type=jnp.float32)
        from_sender = jnp.dot(slope, w_edge_in[:width].T, preferred_element_type=jnp.float32).reshape(nodes.shape)
        sent_back = sent_back + moved_view(from_sender, -offset)
        edge_grads.append(jnp.dot(slope, w_edge_in[2 * width:].T, preferred_element_type=jnp.float32).astype(jnp.bfloat16).reshape(nodes.shape))
    return (to_nodes.reshape(nodes.shape) + sent_back, jnp.stack(edge_grads), grad_in, grad_out)

def clip_all(grads):
    squares = sum((jnp.sum(single * single) for single in grads))
    entries = sum((single.size for single in grads))
    factor = math.sqrt(entries) / jnp.sqrt(squares)
    return tuple((single * factor for single in grads))

def to_bricks(array):
    rest = array.shape[3:]
    shaped = array.reshape((N_GX, BRICK, N_GY, BRICK, N_GZ, BRICK) + rest)
    order = (0, 2, 4, 1, 3, 5) + tuple(range(6, 6 + len(rest)))
    return jnp.transpose(shaped, order).reshape((N_GX * N_GY * N_GZ, BRICK, BRICK, BRICK) + rest)

def from_bricks(array):
    rest = array.shape[4:]
    shaped = array.reshape((N_GX, N_GY, N_GZ, BRICK, BRICK, BRICK) + rest)
    order = (0, 3, 1, 4, 2, 5) + tuple(range(6, 6 + len(rest)))
    return jnp.transpose(shaped, order).reshape((N_GX * BRICK, N_GY * BRICK, N_GZ * BRICK) + rest)

def shift_blocks(block, brick_axis, forward):
    length = block.shape[brick_axis]
    empty = jnp.zeros_like(lax.slice_in_dim(block, 0, 1, axis=brick_axis))
    if forward:
        return jnp.concatenate([empty, lax.slice_in_dim(block, 0, length - 1, axis=brick_axis)], axis=brick_axis)
    return jnp.concatenate([lax.slice_in_dim(block, 1, length, axis=brick_axis), empty], axis=brick_axis)

def assemble_all(stacked):
    grid = stacked.reshape((N_GX, N_GY, N_GZ, BRICK, BRICK, BRICK) + stacked.shape[4:])
    for brick_axis in range(3):
        local_axis = brick_axis + 3
        lower = lax.slice_in_dim(grid, 0, 1, axis=local_axis)
        upper = lax.slice_in_dim(grid, BRICK - 1, BRICK, axis=local_axis)
        middle = lax.slice_in_dim(grid, 1, BRICK - 1, axis=local_axis)
        new_lower = lower + shift_blocks(upper, brick_axis, True)
        new_upper = upper + shift_blocks(lower, brick_axis, False)
        grid = jnp.concatenate([new_lower, middle, new_upper], axis=local_axis)
    return grid.reshape(stacked.shape)

def reference(node_feat, edge_feat, copies, offsets, w_edge_in, w_edge_out, w_node_in, w_node_out, node_cot):
    width = node_feat.shape[3]
    nodes_b = to_bricks(node_feat)
    edges_b = jnp.moveaxis(to_bricks(jnp.moveaxis(edge_feat, 0, 3)), 4, 1)
    copies_b = to_bricks(copies)
    cot_b = to_bricks(node_cot)

    def forward_one(items):
        return edge_messages(items[0], items[1], offsets, w_edge_in, w_edge_out)[0]
    local_sum = lax.map(forward_one, (nodes_b, edges_b))
    summed = assemble_all(local_sum)

    def node_step(carry, items):
        to_nodes, to_agg, grad_in, grad_out = node_backward(items[0], items[1], items[2], items[3], w_node_in, w_node_out)
        return ((carry[0] + grad_in, carry[1] + grad_out), (to_nodes, to_agg))
    start_node = (jnp.zeros((2 * width, width), jnp.float32), jnp.zeros((width, width), jnp.float32))
    node_grads, node_outputs = lax.scan(node_step, start_node, (nodes_b, summed, copies_b, cot_b))
    node_part, agg_part = node_outputs
    incoming = assemble_all(agg_part)

    def edge_step(carry, items):
        nodes, edges, arriving = items
        unused, preacts, hiddens = edge_messages(nodes, edges, offsets, w_edge_in, w_edge_out)
        to_nodes, edge_grads, grad_in, grad_out = edge_backward(nodes, edges, offsets, arriving, w_edge_in, w_edge_out, preacts, hiddens)
        return ((carry[0] + grad_in, carry[1] + grad_out), (to_nodes, edge_grads))
    start_edge = (jnp.zeros((3 * width, width), jnp.float32), jnp.zeros((width, width), jnp.float32))
    edge_grads_w, edge_outputs = lax.scan(edge_step, start_edge, (nodes_b, edges_b, incoming))
    edge_part, edge_grad_b = edge_outputs
    local = cot_b.astype(jnp.float32) + node_part + edge_part
    node_grad = from_bricks(assemble_all(local)).astype(jnp.bfloat16)
    edge_grad = jnp.moveaxis(from_bricks(jnp.moveaxis(edge_grad_b, 1, 4)), 3, 0)
    clipped = clip_all((edge_grads_w[0], edge_grads_w[1], node_grads[0], node_grads[1]))
    return (node_grad, edge_grad, clipped[0], clipped[1], clipped[2], clipped[3])
```

```python
import functools
import math

import jax
import jax.numpy as jnp
from jax import lax
from jax.experimental import pallas as pl
from jax.experimental.pallas import tpu as pltpu
from jax.sharding import Mesh
from jax.sharding import PartitionSpec as P

B = 8
W = 128
K = 4
N = B * B * B
CUBE = (B, B, B, W)
FACE = (B, B, W)
F32 = jnp.float32
BF16 = jnp.bfloat16

VMEM = pl.BlockSpec(memory_space=pltpu.VMEM)
SMEM = pl.BlockSpec(memory_space=pltpu.SMEM)


def call(body, outs, specs, name, scratch=(), interpret=False):
    return pl.pallas_call(
        body,
        out_shape=[jax.ShapeDtypeStruct(s, t) for s, t in outs],
        in_specs=specs,
        out_specs=[VMEM] * len(outs),
        scratch_shapes=list(scratch),
        name=name,
        interpret=interpret,
    )


def dot(a, b):
    return jnp.dot(a, b, preferred_element_type=F32)


def dot_t(a, b):
    return lax.dot_general(a, b, (((1,), (1,)), ((), ())), preferred_element_type=F32)


def fill_ring(pad, value):
    pad[1:9, 1:9] = value
    pad[0, 1:9] = value[7]
    pad[9, 1:9] = value[0]
    pad[:, 0] = pad[:, 8]
    pad[:, 9] = pad[:, 1]


def ring_shift(pad, o0, o1, o2):
    moved = pad[pl.ds(1 + o0, B), pl.ds(1 + o1, B)].reshape(B * B, B, W)
    moved = pltpu.roll(moved, lax.rem(B - o2, B), 1)
    return moved.reshape(N, W)


def inside(offs, k):
    ok = None
    for which in range(3):
        at = lax.broadcasted_iota(jnp.int32, CUBE, which) + offs[k, which]
        one = (at >= 0) & (at < B)
        ok = one if ok is None else ok & one
    return ok


def forward_kernel(offs, nodes, edges, w_in, w_out, local, xlo, xhi, preact, hidden, pad):
    node = nodes[...]
    fill_ring(pad, dot(node, w_in[:W]).reshape(CUBE))
    receiver = dot(node, w_in[W : 2 * W])
    total = jnp.zeros((N, W), F32)
    for k in range(K):
        pre = ring_shift(pad, offs[k, 0], offs[k, 1], offs[k, 2]) + receiver + dot(edges[k], w_in[2 * W :])
        preact[k] = pre
        act = pre * jax.nn.sigmoid(pre)
        hid = act.astype(BF16)
        hidden[k] = hid
        kept = jnp.where(inside(offs, k), act.reshape(CUBE), 0.0).reshape(N, W).astype(BF16)
        total = total + dot(kept, w_out[...])
    total = total.reshape(CUBE)
    local[...] = total
    xlo[...] = total[0]
    xhi[...] = total[B - 1]


def prepare_kernel(preact, hidden, nodes, edges, dact, hidden_t, edges_t, nodes_t):
    for k in range(K):
        pre = preact[k]
        sigma = jax.nn.sigmoid(pre)
        dact[k] = sigma * (1.0 + pre * (1.0 - sigma))
        hidden_t[k] = hidden[k].T
        edges_t[k] = edges[k].T
    nodes_t[...] = nodes[...].T


def after_x_kernel(rim, field, rlo, rhi, out, lo, hi):
    out[1 : B - 1] = field[1 : B - 1]
    out[0] = field[0] + jnp.where(rim[0] > 0, rlo[...], 0.0)
    out[B - 1] = field[B - 1] + jnp.where(rim[1] > 0, rhi[...], 0.0)
    lo[...] = out[:, 0]
    hi[...] = out[:, B - 1]


def after_y_kernel(rim, field, rlo, rhi, out, lo, hi):
    out[:, 1 : B - 1] = field[:, 1 : B - 1]
    out[:, 0] = field[:, 0] + jnp.where(rim[2] > 0, rlo[...], 0.0)
    out[:, B - 1] = field[:, B - 1] + jnp.where(rim[3] > 0, rhi[...], 0.0)
    lo[...] = out[:, :, 0, :]
    hi[...] = out[:, :, B - 1, :]


def with_z(rim, field, rlo, rhi, work):
    work[...] = field[...]
    work[:, :, 0, :] = field[:, :, 0, :] + jnp.where(rim[4] > 0, rlo[...], 0.0)
    work[:, :, B - 1, :] = field[:, :, B - 1, :] + jnp.where(rim[5] > 0, rhi[...], 0.0)
    return work[...].reshape(N, W)


def node_kernel(
    rim, field, rlo, rhi, inverse, nodes, cot, w_in, w_out, local, xlo, xhi, gathered, slope, hidden, work
):
    inv = inverse[...]
    agg = (with_z(rim, field, rlo, rhi, work) * inv).astype(BF16)
    gathered[...] = agg
    pre = dot(nodes[...], w_in[:W]) + dot(agg, w_in[W:])
    sigma = jax.nn.sigmoid(pre)
    hidden[...] = (pre * sigma).astype(BF16)
    slo = (dot_t(cot[...], w_out[...]) * (sigma * (1.0 + pre * (1.0 - sigma)))).astype(BF16)
    slope[...] = slo
    part = (dot_t(slo, w_in[W:]) * inv).reshape(CUBE)
    local[...] = part
    xlo[...] = part[0]
    xhi[...] = part[B - 1]


def node_grads_kernel(nodes_t, gathered, slope, hidden, cot, w_in, grads, base):
    slo = slope[...]
    grads[:W] = dot(nodes_t[...], slo)
    grads[W : 2 * W] = dot(gathered[...].T, slo)
    grads[2 * W :] = dot(hidden[...].T, cot[...])
    base[...] = cot[...].astype(F32) + dot_t(slo, w_in[:W])


def edge_kernel(
    rim, offs, field, rlo, rhi, dact, hidden_t, edges_t, nodes_t, base, node_grads, w_in, w_out,
    local, xlo, xhi, slopes, grads, work, pad,
):
    agg = with_z(rim, field, rlo, rhi, work).reshape(CUBE)
    node_t = nodes_t[...]
    part = base[...]
    g_send = jnp.zeros((W, W), F32)
    g_recv = jnp.zeros((W, W), F32)
    g_edge = jnp.zeros((W, W), F32)
    g_out = jnp.zeros((W, W), F32)
    for k in range(K):
        cot = jnp.where(inside(offs, k), agg, 0.0).reshape(N, W).astype(BF16)
        g_out = g_out + dot(hidden_t[k], cot)
        slo = (dot_t(cot, w_out[...]) * dact[k]).astype(BF16)
        slopes[k] = slo
        fill_ring(pad, slo.astype(F32).reshape(CUBE))
        sent = ring_shift(pad, -offs[k, 0], -offs[k, 1], -offs[k, 2]).astype(BF16)
        g_send = g_send + dot(node_t, sent)
        g_recv = g_recv + dot(node_t, slo)
        g_edge = g_edge + dot(edges_t[k], slo)
        part = part + dot_t(slo, w_in[W : 2 * W]) + dot_t(sent, w_in[:W])
    grads[:W] = g_send
    grads[W : 2 * W] = g_recv
    grads[2 * W : 3 * W] = g_edge
    grads[3 * W : 4 * W] = g_out
    grads[4 * W :] = node_grads[...]
    part = part.reshape(CUBE)
    local[...] = part
    xlo[...] = part[0]
    xhi[...] = part[B - 1]


def edge_grad_kernel(slopes, w_in, out):
    for k in range(K):
        out[k] = dot_t(slopes[k], w_in[2 * W :]).astype(BF16)


def last_kernel(rim, field, rlo, rhi, out, work):
    out[...] = with_z(rim, field, rlo, rhi, work).astype(BF16)


def pair_sum(ref, rows, pairs):
    total = ref[: 2 * rows]
    for i in range(1, pairs):
        total = total + ref[2 * rows * i : 2 * rows * (i + 1)]
    return total + jnp.concatenate([total[rows:], total[:rows]], axis=0)


def fold_kernel(rows, pairs, copies, arrived, out):
    total = pair_sum(arrived, rows, pairs)
    for i in range(copies):
        out[2 * rows * i : 2 * rows * (i + 1)] = total


def clip_kernel(grads, edge_in, edge_out, node_in, node_out):
    total = grads[...]
    squares = jnp.sum(jnp.sum(total * total, axis=0, keepdims=True), axis=1, keepdims=True)
    factor = math.sqrt(7 * W * W) / jnp.sqrt(squares)
    edge_in[...] = total[: 3 * W] * factor
    edge_out[...] = total[3 * W : 4 * W] * factor
    node_in[...] = total[4 * W : 6 * W] * factor
    node_out[...] = total[6 * W :] * factor


GX, GY, GZ = ("z", "yh"), ("yl", "c"), ("x",)
NEAR, FAR = ("yh", "yl", "c", "x"), ("z",)


def exchange(lo, hi, axis):
    count = lax.axis_size(axis)
    up = [(i, (i + 1) % count) for i in range(count)]
    down = [(t, s) for s, t in up]
    return lax.ppermute(hi, axis, up), lax.ppermute(lo, axis, down)


def assemble(rim, field, xlo, xhi, tag, interpret):
    rlo, rhi = exchange(xlo, xhi, GX)
    step = [(CUBE, F32), (FACE, F32), (FACE, F32)]
    field, lo, hi = call(after_x_kernel, step, [SMEM] + [VMEM] * 3, "after_x" + tag, interpret=interpret)(
        rim, field, rlo, rhi
    )
    rlo, rhi = exchange(lo, hi, GY)
    field, lo, hi = call(after_y_kernel, step, [SMEM] + [VMEM] * 3, "after_y" + tag, interpret=interpret)(
        rim, field, rlo, rhi
    )
    rlo, rhi = exchange(lo, hi, GZ)
    return field, rlo, rhi


def swap(rows, axes, count):
    return lax.all_to_all(rows.reshape(count, -1), axes, 0, 0, tiled=True).reshape(-1, W)


def reduce_all(grads, interpret):
    near, far = lax.axis_size(NEAR), lax.axis_size(FAR)
    rows = grads.shape[0] // near
    got = swap(grads, NEAR, near)
    (got,) = call(
        functools.partial(fold_kernel, rows, near // 2, far // 2), [((rows * far, W), F32)], [VMEM], "fold_near",
        interpret=interpret,
    )(got)
    got = swap(got, FAR, far)
    (got,) = call(
        functools.partial(fold_kernel, rows, far // 2, near // 2), [((rows * near, W), F32)], [VMEM], "fold_far",
        interpret=interpret,
    )(got)
    return swap(got, NEAR, near)


def on_device(
    node_feat, edge_feat, copies, offsets, w_edge_in, w_edge_out, w_node_in, w_node_out, node_cot, interpret=False
):
    ends = []
    for axis in (GX, GY, GZ):
        at = lax.axis_index(axis)
        ends += [at > 0, at < lax.axis_size(axis) - 1]
    rim = jnp.stack(ends).astype(jnp.int32)
    nodes = node_feat.reshape(N, W)
    edges = edge_feat.reshape(K, N, W)
    cot = node_cot.reshape(N, W)
    inverse = jnp.broadcast_to(1.0 / copies.reshape(N, 1).astype(F32), (N, W))
    cube = [(CUBE, F32), (FACE, F32), (FACE, F32)]
    pad = pltpu.VMEM((B + 2, B + 2, B, W), F32)
    work = pltpu.VMEM(CUBE, F32)
    run = functools.partial(call, interpret=interpret)

    local, xlo, xhi, preact, hidden = run(
        forward_kernel, cube + [((K, N, W), F32), ((K, N, W), BF16)], [SMEM] + [VMEM] * 4, "forward", [pad]
    )(offsets, nodes, edges, w_edge_in, w_edge_out)
    field, rlo, rhi = assemble(rim, local, xlo, xhi, "_1", interpret)
    dact, hidden_t, edges_t, nodes_t = run(
        prepare_kernel,
        [((K, N, W), F32), ((K, W, N), BF16), ((K, W, N), BF16), ((W, N), BF16)],
        [VMEM] * 4,
        "prepare",
    )(preact, hidden, nodes, edges)
    local, xlo, xhi, gathered, slope, node_hidden = run(
        node_kernel, cube + [((N, W), BF16)] * 3, [SMEM] + [VMEM] * 8, "node", [work]
    )(rim, field, rlo, rhi, inverse, nodes, cot, w_node_in, w_node_out)
    field, rlo, rhi = assemble(rim, local, xlo, xhi, "_2", interpret)
    node_grads, base = run(
        node_grads_kernel, [((3 * W, W), F32), ((N, W), F32)], [VMEM] * 6, "node_grads"
    )(nodes_t, gathered, slope, node_hidden, cot, w_node_in)
    local, xlo, xhi, slopes, grads = run(
        edge_kernel,
        cube + [((K, N, W), BF16), ((7 * W, W), F32)],
        [SMEM] * 2 + [VMEM] * 11,
        "edge",
        [work, pad],
    )(rim, offsets, field, rlo, rhi, dact, hidden_t, edges_t, nodes_t, base, node_grads, w_edge_in, w_edge_out)
    total = reduce_all(grads, interpret)
    field, rlo, rhi = assemble(rim, local, xlo, xhi, "_3", interpret)
    (edge_grad,) = run(edge_grad_kernel, [((K, N, W), BF16)], [VMEM] * 2, "edge_grad")(slopes, w_edge_in)
    (node_grad,) = run(last_kernel, [((N, W), BF16)], [SMEM] + [VMEM] * 3, "last", [work])(rim, field, rlo, rhi)
    clipped = run(
        clip_kernel, [((3 * W, W), F32), ((W, W), F32), ((2 * W, W), F32), ((W, W), F32)], [VMEM], "clip"
    )(total)
    return (node_grad.reshape(node_feat.shape), edge_grad.reshape(edge_feat.shape), *clipped)


def solution(mesh):
    split = Mesh(mesh.devices.reshape(8, 2, 2, 2, 4), ("z", "yh", "yl", "c", "x"))
    place = (GX, GY, GZ)
    placed = (
        P(*place, None),
        P(None, *place, None),
        P(*place),
        P(),
        P(),
        P(),
        P(),
        P(),
        P(*place, None),
    )
    return jax.shard_map(
        on_device,
        mesh=split,
        in_specs=placed,
        out_specs=(P(*place, None), P(None, *place, None), P(), P(), P(), P()),
        check_vma=False,
    )
```

```python
import functools
import math

import jax
import jax.numpy as jnp
from jax import lax
from jax.experimental import pallas as pl
from jax.experimental.pallas import tpu as pltpu
from jax.sharding import Mesh
from jax.sharding import PartitionSpec as P

B = 8
W = 128
K = 4
N = B * B * B
CUBE = (B, B, B, W)
FACE = (B, B, W)
F32 = jnp.float32
BF16 = jnp.bfloat16

GRANT = 12 * 1024 * 1024

VMEM = pl.BlockSpec(memory_space=pltpu.VMEM)
SMEM = pl.BlockSpec(memory_space=pltpu.SMEM)


def call(body, outs, specs, name, scratch=(), interpret=False):
    return pl.pallas_call(
        body,
        out_shape=[jax.ShapeDtypeStruct(s, t) for s, t in outs],
        in_specs=specs,
        out_specs=[VMEM] * len(outs),
        scratch_shapes=list(scratch),
        compiler_params=pltpu.CompilerParams(vmem_limit_bytes=GRANT),
        name=name,
        interpret=interpret,
    )


def dot(a, b):
    return jnp.dot(a, b, preferred_element_type=F32)


def dot_t(a, b):
    return lax.dot_general(a, b, (((1,), (1,)), ((), ())), preferred_element_type=F32)


def fill_ring(pad, value):
    pad[1:9, 1:9] = value
    pad[0, 1:9] = value[7]
    pad[9, 1:9] = value[0]
    pad[:, 0] = pad[:, 8]
    pad[:, 9] = pad[:, 1]


def ring_shift(pad, o0, o1, o2):
    moved = pad[pl.ds(1 + o0, B), pl.ds(1 + o1, B)].reshape(B * B, B, W)
    moved = pltpu.roll(moved, lax.rem(B - o2, B), 1)
    return moved.reshape(N, W)


def inside(offs, k):
    ok = None
    for which in range(3):
        at = lax.broadcasted_iota(jnp.int32, CUBE, which) + offs[k, which]
        one = (at >= 0) & (at < B)
        ok = one if ok is None else ok & one
    return ok


def forward_kernel(offs, nodes, edges, w_in, w_out, local, xlo, xhi, preact, hidden, pad):
    node = nodes[...]
    fill_ring(pad, dot(node, w_in[:W]).reshape(CUBE))
    receiver = dot(node, w_in[W : 2 * W])
    total = jnp.zeros((N, W), F32)
    for k in range(K):
        pre = ring_shift(pad, offs[k, 0], offs[k, 1], offs[k, 2]) + receiver + dot(edges[k], w_in[2 * W :])
        preact[k] = pre
        act = pre * jax.nn.sigmoid(pre)
        hid = act.astype(BF16)
        hidden[k] = hid
        kept = jnp.where(inside(offs, k), act.reshape(CUBE), 0.0).reshape(N, W).astype(BF16)
        total = total + dot(kept, w_out[...])
    total = total.reshape(CUBE)
    local[...] = total
    xlo[...] = total[0]
    xhi[...] = total[B - 1]


def prepare_kernel(preact, hidden, nodes, edges, dact, hidden_t, edges_t, nodes_t):
    for k in range(K):
        pre = preact[k]
        sigma = jax.nn.sigmoid(pre)
        dact[k] = sigma * (1.0 + pre * (1.0 - sigma))
        hidden_t[k] = hidden[k].T
        edges_t[k] = edges[k].T
    nodes_t[...] = nodes[...].T


def after_x_kernel(rim, field, rlo, rhi, out, lo, hi):
    out[1 : B - 1] = field[1 : B - 1]
    out[0] = field[0] + jnp.where(rim[0] > 0, rlo[...], 0.0)
    out[B - 1] = field[B - 1] + jnp.where(rim[1] > 0, rhi[...], 0.0)
    lo[...] = out[:, 0]
    hi[...] = out[:, B - 1]


def after_y_kernel(rim, field, rlo, rhi, out, lo, hi):
    out[:, 1 : B - 1] = field[:, 1 : B - 1]
    out[:, 0] = field[:, 0] + jnp.where(rim[2] > 0, rlo[...], 0.0)
    out[:, B - 1] = field[:, B - 1] + jnp.where(rim[3] > 0, rhi[...], 0.0)
    lo[...] = out[:, :, 0, :]
    hi[...] = out[:, :, B - 1, :]


def with_z(rim, field, rlo, rhi, work):
    work[...] = field[...]
    work[:, :, 0, :] = field[:, :, 0, :] + jnp.where(rim[4] > 0, rlo[...], 0.0)
    work[:, :, B - 1, :] = field[:, :, B - 1, :] + jnp.where(rim[5] > 0, rhi[...], 0.0)
    return work[...].reshape(N, W)


def node_kernel(
    rim, field, rlo, rhi, inverse, nodes, cot, w_in, w_out, local, xlo, xhi, gathered, slope, hidden, work
):
    inv = inverse[...]
    agg = (with_z(rim, field, rlo, rhi, work) * inv).astype(BF16)
    gathered[...] = agg
    pre = dot(nodes[...], w_in[:W]) + dot(agg, w_in[W:])
    sigma = jax.nn.sigmoid(pre)
    hidden[...] = (pre * sigma).astype(BF16)
    slo = (dot_t(cot[...], w_out[...]) * (sigma * (1.0 + pre * (1.0 - sigma)))).astype(BF16)
    slope[...] = slo
    part = (dot_t(slo, w_in[W:]) * inv).reshape(CUBE)
    local[...] = part
    xlo[...] = part[0]
    xhi[...] = part[B - 1]


def node_grads_kernel(nodes_t, gathered, slope, hidden, cot, w_in, grads, base):
    slo = slope[...]
    grads[:W] = dot(nodes_t[...], slo)
    grads[W : 2 * W] = dot(gathered[...].T, slo)
    grads[2 * W :] = dot(hidden[...].T, cot[...])
    base[...] = cot[...].astype(F32) + dot_t(slo, w_in[:W])


def edge_kernel(
    rim, offs, field, rlo, rhi, dact, hidden_t, edges_t, nodes_t, base, node_grads, w_in, w_out,
    local, xlo, xhi, slopes, grads, work, pad,
):
    agg = with_z(rim, field, rlo, rhi, work).reshape(CUBE)
    node_t = nodes_t[...]
    part = base[...]
    g_send = jnp.zeros((W, W), F32)
    g_recv = jnp.zeros((W, W), F32)
    g_edge = jnp.zeros((W, W), F32)
    g_out = jnp.zeros((W, W), F32)
    for k in range(K):
        cot = jnp.where(inside(offs, k), agg, 0.0).reshape(N, W).astype(BF16)
        g_out = g_out + dot(hidden_t[k], cot)
        slo = (dot_t(cot, w_out[...]) * dact[k]).astype(BF16)
        slopes[k] = slo
        fill_ring(pad, slo.astype(F32).reshape(CUBE))
        sent = ring_shift(pad, -offs[k, 0], -offs[k, 1], -offs[k, 2]).astype(BF16)
        g_send = g_send + dot(node_t, sent)
        g_recv = g_recv + dot(node_t, slo)
        g_edge = g_edge + dot(edges_t[k], slo)
        part = part + dot_t(slo, w_in[W : 2 * W]) + dot_t(sent, w_in[:W])
    grads[:W] = g_send
    grads[W : 2 * W] = g_recv
    grads[2 * W : 3 * W] = g_edge
    grads[3 * W : 4 * W] = g_out
    grads[4 * W :] = node_grads[...]
    part = part.reshape(CUBE)
    local[...] = part
    xlo[...] = part[0]
    xhi[...] = part[B - 1]


def edge_grad_kernel(slopes, w_in, out):
    for k in range(K):
        out[k] = dot_t(slopes[k], w_in[2 * W :]).astype(BF16)


def last_kernel(rim, field, rlo, rhi, out, work):
    out[...] = with_z(rim, field, rlo, rhi, work).astype(BF16)


def pair_sum(ref, rows, pairs):
    total = ref[: 2 * rows]
    for i in range(1, pairs):
        total = total + ref[2 * rows * i : 2 * rows * (i + 1)]
    return total + jnp.concatenate([total[rows:], total[:rows]], axis=0)


def fold(rows, pairs, copies, arrived, out):
    total = pair_sum(arrived, rows, pairs)
    for i in range(copies):
        out[2 * rows * i : 2 * rows * (i + 1)] = total


def after_x_fold_kernel(rows, pairs, copies, rim, field, rlo, rhi, arrived, out, lo, hi, spread):
    fold(rows, pairs, copies, arrived, spread)
    after_x_kernel(rim, field, rlo, rhi, out, lo, hi)


def after_y_fold_kernel(rows, pairs, copies, rim, field, rlo, rhi, arrived, out, lo, hi, spread):
    fold(rows, pairs, copies, arrived, spread)
    after_y_kernel(rim, field, rlo, rhi, out, lo, hi)


def clip_kernel(grads, edge_in, edge_out, node_in, node_out):
    total = grads[...]
    squares = jnp.sum(jnp.sum(total * total, axis=0, keepdims=True), axis=1, keepdims=True)
    factor = math.sqrt(7 * W * W) / jnp.sqrt(squares)
    edge_in[...] = total[: 3 * W] * factor
    edge_out[...] = total[3 * W : 4 * W] * factor
    node_in[...] = total[4 * W : 6 * W] * factor
    node_out[...] = total[6 * W :] * factor


GX, GY, GZ = ("z", "yh"), ("yl", "c"), ("x",)
NEAR, FAR = ("yh", "yl", "c", "x"), ("z",)


def exchange(lo, hi, axis):
    count = lax.axis_size(axis)
    up = [(i, (i + 1) % count) for i in range(count)]
    down = [(t, s) for s, t in up]
    return lax.ppermute(hi, axis, up), lax.ppermute(lo, axis, down)


def assemble(rim, field, xlo, xhi, tag, interpret):
    rlo, rhi = exchange(xlo, xhi, GX)
    step = [(CUBE, F32), (FACE, F32), (FACE, F32)]
    field, lo, hi = call(after_x_kernel, step, [SMEM] + [VMEM] * 3, "after_x" + tag, interpret=interpret)(
        rim, field, rlo, rhi
    )
    rlo, rhi = exchange(lo, hi, GY)
    field, lo, hi = call(after_y_kernel, step, [SMEM] + [VMEM] * 3, "after_y" + tag, interpret=interpret)(
        rim, field, rlo, rhi
    )
    rlo, rhi = exchange(lo, hi, GZ)
    return field, rlo, rhi


def swap(rows, axes, count):
    return lax.all_to_all(rows.reshape(count, -1), axes, 0, 0, tiled=True).reshape(-1, W)


def assemble_and_reduce(rim, field, xlo, xhi, grads, interpret):
    near, far = lax.axis_size(NEAR), lax.axis_size(FAR)
    rows = grads.shape[0] // near
    step = [(CUBE, F32), (FACE, F32), (FACE, F32)]
    rlo, rhi = exchange(xlo, xhi, GX)
    got = swap(grads, NEAR, near)
    field, lo, hi, spread = call(
        functools.partial(after_x_fold_kernel, rows, near // 2, far // 2),
        step + [((rows * far, W), F32)],
        [SMEM] + [VMEM] * 4,
        "after_x_fold",
        interpret=interpret,
    )(rim, field, rlo, rhi, got)
    rlo, rhi = exchange(lo, hi, GY)
    got = swap(spread, FAR, far)
    field, lo, hi, spread = call(
        functools.partial(after_y_fold_kernel, rows, far // 2, near // 2),
        step + [((rows * near, W), F32)],
        [SMEM] + [VMEM] * 4,
        "after_y_fold",
        interpret=interpret,
    )(rim, field, rlo, rhi, got)
    rlo, rhi = exchange(lo, hi, GZ)
    return field, rlo, rhi, swap(spread, NEAR, near)


def on_device(
    node_feat, edge_feat, copies, offsets, w_edge_in, w_edge_out, w_node_in, w_node_out, node_cot, interpret=False
):
    ends = []
    for axis in (GX, GY, GZ):
        at = lax.axis_index(axis)
        ends += [at > 0, at < lax.axis_size(axis) - 1]
    rim = jnp.stack(ends).astype(jnp.int32)
    nodes = node_feat.reshape(N, W)
    edges = edge_feat.reshape(K, N, W)
    cot = node_cot.reshape(N, W)
    inverse = jnp.broadcast_to(1.0 / copies.reshape(N, 1).astype(F32), (N, W))
    cube = [(CUBE, F32), (FACE, F32), (FACE, F32)]
    pad = pltpu.VMEM((B + 2, B + 2, B, W), F32)
    work = pltpu.VMEM(CUBE, F32)
    run = functools.partial(call, interpret=interpret)

    local, xlo, xhi, preact, hidden = run(
        forward_kernel, cube + [((K, N, W), F32), ((K, N, W), BF16)], [SMEM] + [VMEM] * 4, "forward", [pad]
    )(offsets, nodes, edges, w_edge_in, w_edge_out)
    field, rlo, rhi = assemble(rim, local, xlo, xhi, "_1", interpret)
    dact, hidden_t, edges_t, nodes_t = run(
        prepare_kernel,
        [((K, N, W), F32), ((K, W, N), BF16), ((K, W, N), BF16), ((W, N), BF16)],
        [VMEM] * 4,
        "prepare",
    )(preact, hidden, nodes, edges)
    local, xlo, xhi, gathered, slope, node_hidden = run(
        node_kernel, cube + [((N, W), BF16)] * 3, [SMEM] + [VMEM] * 8, "node", [work]
    )(rim, field, rlo, rhi, inverse, nodes, cot, w_node_in, w_node_out)
    field, rlo, rhi = assemble(rim, local, xlo, xhi, "_2", interpret)
    node_grads, base = run(
        node_grads_kernel, [((3 * W, W), F32), ((N, W), F32)], [VMEM] * 6, "node_grads"
    )(nodes_t, gathered, slope, node_hidden, cot, w_node_in)
    local, xlo, xhi, slopes, grads = run(
        edge_kernel,
        cube + [((K, N, W), BF16), ((7 * W, W), F32)],
        [SMEM] * 2 + [VMEM] * 11,
        "edge",
        [work, pad],
    )(rim, offsets, field, rlo, rhi, dact, hidden_t, edges_t, nodes_t, base, node_grads, w_edge_in, w_edge_out)
    field, rlo, rhi, total = assemble_and_reduce(rim, local, xlo, xhi, grads, interpret)
    (edge_grad,) = run(edge_grad_kernel, [((K, N, W), BF16)], [VMEM] * 2, "edge_grad")(slopes, w_edge_in)
    (node_grad,) = run(last_kernel, [((N, W), BF16)], [SMEM] + [VMEM] * 3, "last", [work])(rim, field, rlo, rhi)
    clipped = run(
        clip_kernel, [((3 * W, W), F32), ((W, W), F32), ((2 * W, W), F32), ((W, W), F32)], [VMEM], "clip"
    )(total)
    return (node_grad.reshape(node_feat.shape), edge_grad.reshape(edge_feat.shape), *clipped)


def solution(mesh):
    split = Mesh(mesh.devices.reshape(8, 2, 2, 2, 4), ("z", "yh", "yl", "c", "x"))
    place = (GX, GY, GZ)
    placed = (
        P(*place, None),
        P(None, *place, None),
        P(*place),
        P(),
        P(),
        P(),
        P(),
        P(),
        P(*place, None),
    )
    return jax.shard_map(
        on_device,
        mesh=split,
        in_specs=placed,
        out_specs=(P(*place, None), P(None, *place, None), P(), P(), P(), P()),
        check_vma=False,
    )
```

```python
import functools
import math

import jax
import jax.numpy as jnp
from jax import lax
from jax.experimental import pallas as pl
from jax.experimental.pallas import tpu as pltpu
from jax.sharding import Mesh
from jax.sharding import PartitionSpec as P

B = 8
W = 128
K = 4
N = B * B * B
CUBE = (B, B, B, W)
FACE = (B, B, W)
F32 = jnp.float32
BF16 = jnp.bfloat16
GRANT = 12 * 1024 * 1024

VMEM = pl.BlockSpec(memory_space=pltpu.VMEM)
SMEM = pl.BlockSpec(memory_space=pltpu.SMEM)
HBM = pl.BlockSpec(memory_space=pltpu.HBM)
PAD = pltpu.VMEM((B + 2, B + 2, B, W), F32)
WORK = pltpu.VMEM(CUBE, F32)

GX, GY, GZ = ("z", "yh"), ("yl", "c"), ("x",)
NEAR, FAR = ("yh", "yl", "c", "x"), ("z",)


def call(body, outs, specs, name, scratch=()):
    return pl.pallas_call(
        body,
        out_shape=[jax.ShapeDtypeStruct(s, t) for s, t in outs],
        in_specs=specs,
        out_specs=[VMEM] * len(outs),
        scratch_shapes=list(scratch),
        compiler_params=pltpu.CompilerParams(vmem_limit_bytes=GRANT),
        name=name,
    )


def in_hbm(array):
    return pltpu.with_memory_space_constraint(array, pltpu.HBM)


def dot(a, b):
    return jnp.dot(a, b, preferred_element_type=F32)


def dot_t(a, b):
    return lax.dot_general(a, b, (((1,), (1,)), ((), ())), preferred_element_type=F32)


def fill_ring(pad, value):
    pad[1:9, 1:9] = value
    pad[0, 1:9] = value[7]
    pad[9, 1:9] = value[0]
    pad[:, 0] = pad[:, 8]
    pad[:, 9] = pad[:, 1]


def ring_shift(pad, o0, o1, o2):
    moved = pad[pl.ds(1 + o0, B), pl.ds(1 + o1, B)].reshape(B * B, B, W)
    moved = pltpu.roll(moved, lax.rem(B - o2, B), 1)
    return moved.reshape(N, W)


def inside(offs, k):
    ok = None
    for which in range(3):
        at = lax.broadcasted_iota(jnp.int32, CUBE, which) + offs[k, which]
        one = (at >= 0) & (at < B)
        ok = one if ok is None else ok & one
    return ok


def forward_kernel(
    nodes_h, edges_h, w_in_h, w_out_h, offs_h,
    local, xlo, xhi, preact, hidden, nodes, edges, w_in, w_out,
    pad, offs, sems,
):
    pairs = [(nodes_h, nodes), (w_in_h, w_in), (offs_h, offs), (w_out_h, w_out)]
    pairs += [(edges_h.at[k], edges.at[k]) for k in range(K)]
    copies = [pltpu.make_async_copy(a, b, sems.at[i]) for i, (a, b) in enumerate(pairs)]
    for copy in copies:
        copy.start()
    for copy in copies[:3]:
        copy.wait()
    node = nodes[...]
    fill_ring(pad, dot(node, w_in[:W]).reshape(CUBE))
    receiver = dot(node, w_in[W : 2 * W])
    copies[3].wait()
    total = jnp.zeros((N, W), F32)
    for k in range(K):
        copies[4 + k].wait()
        pre = ring_shift(pad, offs[k, 0], offs[k, 1], offs[k, 2]) + receiver + dot(edges[k], w_in[2 * W :])
        preact[k] = pre
        act = (pre * jax.nn.sigmoid(pre)).reshape(CUBE)
        kept = jnp.where(inside(offs, k), act, 0.0).reshape(N, W).astype(BF16)
        hidden[k] = kept
        total = total + dot(kept, w_out[...])
    total = total.reshape(CUBE)
    local[...] = total
    xlo[...] = total[0]
    xhi[...] = total[B - 1]


def prepare_node_kernel(nodes, cot, w_in, w_out, pre, upstream, w_back):
    pre[...] = dot(nodes[...], w_in[:W])
    upstream[...] = dot_t(cot[...], w_out[...])
    w_back[...] = w_in[W:].T


def prepare_edge_kernel(offs, preact, hidden, nodes, edges, w_in, w_out, dact, hidden_t, left, w_out_t, w_back, pad):
    node = nodes[...]
    node_t = node.T
    fill_ring(pad, node.astype(F32).reshape(CUBE))
    for k in range(K):
        pre = preact[k]
        sigma = jax.nn.sigmoid(pre)
        rate = (sigma * (1.0 + pre * (1.0 - sigma))).reshape(CUBE)
        dact[k] = jnp.where(inside(offs, k), rate, 0.0).reshape(N, W)
        hidden_t[k * W : (k + 1) * W] = hidden[k].T
        here = pl.ds(k * N, N)
        left[:W, here] = ring_shift(pad, offs[k, 0], offs[k, 1], offs[k, 2]).astype(BF16).T
        left[W : 2 * W, here] = node_t
        left[2 * W :, here] = edges[k].T
    w_out_t[...] = w_out[...].T
    w_back[:W] = w_in[W : 2 * W].T
    w_back[W:] = w_in[:W].T


def shown(rim, which, plane):
    return jnp.where(rim[which] > 0, plane, 0.0)


def add_x(rim, x, out):
    out[0] = out[0] + shown(rim, 0, x[0][...])
    out[B - 1] = out[B - 1] + shown(rim, 1, x[1][...])


def add_y(rim, y, out):
    out[:, 0] = out[:, 0] + shown(rim, 2, y[0][...])
    out[:, B - 1] = out[:, B - 1] + shown(rim, 3, y[1][...])


def add_z(rim, z, out):
    out[:, :, 0, :] = out[:, :, 0, :] + shown(rim, 4, z[0][...])
    out[:, :, B - 1, :] = out[:, :, B - 1, :] + shown(rim, 5, z[1][...])


def y_faces_after_x(rim, field, x0, x1, lo, hi):
    for at, out in ((0, lo), (B - 1, hi)):
        out[...] = field[:, at]
        out[0] = out[0] + shown(rim, 0, x0[at])
        out[B - 1] = out[B - 1] + shown(rim, 1, x1[at])


def z_faces_after_y(rim, field, x0, x1, y0, y1, lo, hi):
    for at, out in ((0, lo), (B - 1, hi)):
        out[...] = field[:, :, at, :]
        out[0] = out[0] + shown(rim, 0, x0[:, at, :])
        out[B - 1] = out[B - 1] + shown(rim, 1, x1[:, at, :])
        out[:, 0, :] = out[:, 0, :] + shown(rim, 2, y0[:, at, :])
        out[:, B - 1, :] = out[:, B - 1, :] + shown(rim, 3, y1[:, at, :])


def y_faces_after_z(rim, field, z0, z1, lo, hi):
    for at, out in ((0, lo), (B - 1, hi)):
        out[...] = field[:, at]
        out[:, 0, :] = out[:, 0, :] + shown(rim, 4, z0[:, at, :])
        out[:, B - 1, :] = out[:, B - 1, :] + shown(rim, 5, z1[:, at, :])


def x_faces_after_y(rim, field, z0, z1, y0, y1, lo, hi):
    for at, out in ((0, lo), (B - 1, hi)):
        out[...] = field[at]
        out[:, 0, :] = out[:, 0, :] + shown(rim, 4, z0[at])
        out[:, B - 1, :] = out[:, B - 1, :] + shown(rim, 5, z1[at])
        out[0] = out[0] + shown(rim, 2, y0[at])
        out[B - 1] = out[B - 1] + shown(rim, 3, y1[at])


def whole(rim, field, x0, x1, y0, y1, z0, z1, work):
    work[...] = field[...]
    add_x(rim, (x0, x1), work)
    add_y(rim, (y0, y1), work)
    add_z(rim, (z0, z1), work)
    return work[...].reshape(N, W)


def node_kernel(
    rim, field, x0, x1, y0, y1, z0, z1, inverse, begun, upstream, w_in, w_back,
    local, xlo, xhi, gathered, slope, hidden, work,
):
    inv = inverse[...]
    agg = (whole(rim, field, x0, x1, y0, y1, z0, z1, work) * inv).astype(BF16)
    gathered[...] = agg
    pre = begun[...] + dot(agg, w_in[W:])
    sigma = jax.nn.sigmoid(pre)
    hidden[...] = (pre * sigma).astype(BF16)
    slo = (upstream[...] * (sigma * (1.0 + pre * (1.0 - sigma)))).astype(BF16)
    slope[...] = slo
    part = (dot(slo, w_back[...]) * inv).reshape(CUBE)
    local[...] = part
    xlo[...] = part[0]
    xhi[...] = part[B - 1]


def node_grads_kernel(nodes, gathered, slope, hidden, cot, w_in, grads, base):
    slo = slope[...]
    grads[:W] = dot(nodes[...].T, slo)
    grads[W : 2 * W] = dot(gathered[...].T, slo)
    grads[2 * W :] = dot(hidden[...].T, cot[...])
    base[...] = cot[...].astype(F32) + dot_t(slo, w_in[:W])


def edge_kernel(
    rim, field, x0, x1, y0, y1, z0, z1, dact, hidden_t, left, w_out_t, node_grads, slopes, grads, work
):
    agg = whole(rim, field, x0, x1, y0, y1, z0, z1, work).astype(BF16)
    back = dot(agg, w_out_t[...])
    for k in range(K):
        slopes[k * N : (k + 1) * N] = (back * dact[k]).astype(BF16)
    outer = dot(hidden_t[...], agg)
    grads[3 * W : 4 * W] = (outer[:W] + outer[W : 2 * W]) + (outer[2 * W : 3 * W] + outer[3 * W :])
    grads[4 * W :] = node_grads[...]
    grads[: 3 * W] = dot(left[...], slopes[...])


def node_part_kernel(offs, slopes, base, w_back, local, zlo, zhi, pad):
    part = base[...]
    for k in range(K):
        slo = slopes[k * N : (k + 1) * N]
        fill_ring(pad, slo.astype(F32).reshape(CUBE))
        sent = ring_shift(pad, -offs[k, 0], -offs[k, 1], -offs[k, 2]).astype(BF16)
        part = part + dot(jnp.concatenate([slo, sent], axis=1), w_back[...])
    local[...] = part.reshape(CUBE)
    zlo[...] = local[:, :, 0, :]
    zhi[...] = local[:, :, B - 1, :]


def edge_grad_kernel(slopes, w_in, out):
    out[...] = dot_t(slopes[...], w_in[2 * W :]).astype(BF16)


def last_kernel(rim, field, z0, z1, y0, y1, x0, x1, clipped, out, work):
    work[...] = field[...]
    add_z(rim, (z0, z1), work)
    add_y(rim, (y0, y1), work)
    add_x(rim, (x0, x1), work)
    out[...] = work[...].reshape(N, W).astype(BF16)


def fold(rows, pairs, copies, arrived, out):
    total = arrived[: 2 * rows]
    for i in range(1, pairs):
        total = total + arrived[2 * rows * i : 2 * rows * (i + 1)]
    total = total + jnp.concatenate([total[rows:], total[:rows]], axis=0)
    for i in range(copies):
        out[2 * rows * i : 2 * rows * (i + 1)] = total


def fold_with_faces_kernel(faces, rows, pairs, copies, arrived, *refs):
    fold(rows, pairs, copies, arrived, refs[-1])
    faces(*refs[:-1])


def clip_kernel(grads, edge_in, edge_out, node_in, node_out):
    total = grads[...]
    squares = jnp.sum(jnp.sum(total * total, axis=0, keepdims=True), axis=1, keepdims=True)
    factor = math.sqrt(7 * W * W) / jnp.sqrt(squares)
    edge_in[...] = total[: 3 * W] * factor
    edge_out[...] = total[3 * W : 4 * W] * factor
    node_in[...] = total[4 * W : 6 * W] * factor
    node_out[...] = total[6 * W :] * factor


def exchange(lo, hi, axis):
    count = lax.axis_size(axis)
    up = [(i, (i + 1) % count) for i in range(count)]
    down = [(t, s) for s, t in up]
    return lax.ppermute(hi, axis, up), lax.ppermute(lo, axis, down)


FACES = [(FACE, F32), (FACE, F32)]


def arrivals(rim, field, xlo, xhi, tag):
    x = exchange(xlo, xhi, GX)
    lo, hi = call(y_faces_after_x, FACES, [VMEM] * 4, "after_x" + tag)(rim, field, *x)
    y = exchange(lo, hi, GY)
    lo, hi = call(z_faces_after_y, FACES, [VMEM] * 6, "after_y" + tag)(rim, field, *x, *y)
    return (*x, *y, *exchange(lo, hi, GZ))


def swap(rows, axes):
    return lax.all_to_all(rows.reshape(lax.axis_size(axes), -1), axes, 0, 0, tiled=True).reshape(-1, W)


def arrivals_and_sum(rim, field, zlo, zhi, grads):
    near, far = lax.axis_size(NEAR), lax.axis_size(FAR)
    rows = grads.shape[0] // near
    got = swap(grads, NEAR)
    z = exchange(zlo, zhi, GZ)
    lo, hi, spread = call(
        functools.partial(fold_with_faces_kernel, y_faces_after_z, rows, near // 2, far // 2),
        FACES + [((rows * far, W), F32)],
        [VMEM] * 5,
        "after_z_fold",
    )(got, rim, field, *z)
    got = swap(spread, FAR)
    y = exchange(lo, hi, GY)
    lo, hi, spread = call(
        functools.partial(fold_with_faces_kernel, x_faces_after_y, rows, far // 2, near // 2),
        FACES + [((rows * near, W), F32)],
        [VMEM] * 7,
        "after_y_fold",
    )(got, rim, field, *z, *y)
    total = swap(spread, NEAR)
    return (*z, *y, *exchange(lo, hi, GX)), total


def on_device(node_feat, edge_feat, copies, offsets, w_edge_in, w_edge_out, w_node_in, w_node_out, node_cot):
    ends = []
    for axis in (GX, GY, GZ):
        at = lax.axis_index(axis)
        ends += [at > 0, at < lax.axis_size(axis) - 1]
    rim = jnp.broadcast_to(jnp.stack(ends).astype(F32)[:, None, None], (6, B, W))
    cot = node_cot.reshape(N, W)
    inverse = jnp.broadcast_to(1.0 / copies.reshape(N, 1).astype(F32), (N, W))
    square = ((W, W), BF16)
    many = ((K, N, W), BF16)

    local, xlo, xhi, preact, hidden, nodes, edges, w_in, w_out = call(
        forward_kernel,
        [(CUBE, F32)] + FACES + [((K, N, W), F32), many, ((N, W), BF16), many, ((3 * W, W), BF16), square],
        [HBM] * 5,
        "forward",
        [PAD, pltpu.SMEM((K, 3), jnp.int32), pltpu.SemaphoreType.DMA((4 + K,))],
    )(*map(in_hbm, (node_feat.reshape(N, W), edge_feat.reshape(K, N, W), w_edge_in, w_edge_out, offsets)))
    begun, upstream, w_node_back = call(
        prepare_node_kernel, [((N, W), F32), ((N, W), F32), square], [VMEM] * 4, "prepare_node"
    )(nodes, cot, w_node_in, w_node_out)
    arrived = arrivals(rim, local, xlo, xhi, "_1")
    dact, hidden_t, left, w_out_t, w_back = call(
        prepare_edge_kernel,
        [((K, N, W), F32), ((K * W, N), BF16), ((3 * W, K * N), BF16), square, ((2 * W, W), BF16)],
        [SMEM] + [VMEM] * 6,
        "prepare_edge",
        [PAD],
    )(offsets, preact, hidden, nodes, edges, w_in, w_out)
    local, xlo, xhi, gathered, slope, node_hidden = call(
        node_kernel, [(CUBE, F32)] + FACES + [((N, W), BF16)] * 3, [VMEM] * 13, "node", [WORK]
    )(rim, local, *arrived, inverse, begun, upstream, w_node_in, w_node_back)
    arrived = arrivals(rim, local, xlo, xhi, "_2")
    node_grads, base = call(node_grads_kernel, [((3 * W, W), F32), ((N, W), F32)], [VMEM] * 6, "node_grads")(
        nodes, gathered, slope, node_hidden, cot, w_node_in
    )
    slopes, grads = call(
        edge_kernel, [((K * N, W), BF16), ((7 * W, W), F32)], [VMEM] * 13, "edge", [WORK]
    )(rim, local, *arrived, dact, hidden_t, left, w_out_t, node_grads)
    local, zlo, zhi = call(
        node_part_kernel, [(CUBE, F32)] + FACES, [SMEM] + [VMEM] * 3, "node_part", [PAD]
    )(offsets, slopes, base, w_back)
    arrived, total = arrivals_and_sum(rim, local, zlo, zhi, grads)
    (edge_grad,) = call(edge_grad_kernel, [((K * N, W), BF16)], [VMEM] * 2, "edge_grad")(slopes, w_in)
    clipped = call(
        clip_kernel, [((3 * W, W), F32), ((W, W), F32), ((2 * W, W), F32), ((W, W), F32)], [VMEM], "clip"
    )(total)
    (node_grad,) = call(last_kernel, [((N, W), BF16)], [VMEM] * 8 + [HBM], "last", [WORK])(
        rim, local, *arrived, in_hbm(clipped[1])
    )
    return (node_grad.reshape(node_feat.shape), edge_grad.reshape(edge_feat.shape), *clipped)


def solution(mesh):
    split = Mesh(mesh.devices.reshape(8, 2, 2, 2, 4), ("z", "yh", "yl", "c", "x"))
    place = (GX, GY, GZ)
    placed = (
        P(*place, None),
        P(None, *place, None),
        P(*place),
        P(),
        P(),
        P(),
        P(),
        P(),
        P(*place, None),
    )
    return jax.shard_map(
        on_device,
        mesh=split,
        in_specs=placed,
        out_specs=(P(*place, None), P(None, *place, None), P(), P(), P(), P()),
        check_vma=False,
    )
```

```python
import functools
import math

import jax
import jax.numpy as jnp
from jax import lax
from jax.experimental import pallas as pl
from jax.experimental.pallas import tpu as pltpu
from jax.sharding import Mesh
from jax.sharding import PartitionSpec as P

B = 8
W = 128
K = 4
N = B * B * B
CUBE = (B, B, B, W)
FACE = (B, B, W)
F32 = jnp.float32
BF16 = jnp.bfloat16
GRANT = 12 * 1024 * 1024

VMEM = pl.BlockSpec(memory_space=pltpu.VMEM)
SMEM = pl.BlockSpec(memory_space=pltpu.SMEM)
HBM = pl.BlockSpec(memory_space=pltpu.HBM)
PAD = pltpu.VMEM((B + 2, B + 2, B, W), F32)
WORK = pltpu.VMEM(CUBE, F32)

GX, GY, GZ = ("z", "yh"), ("yl", "c"), ("x",)
NEAR, FAR = ("yh", "yl", "c", "x"), ("z",)


def call(body, outs, specs, name, scratch=()):
    return pl.pallas_call(
        body,
        out_shape=[jax.ShapeDtypeStruct(s, t) for s, t in outs],
        in_specs=specs,
        out_specs=[VMEM] * len(outs),
        scratch_shapes=list(scratch),
        compiler_params=pltpu.CompilerParams(vmem_limit_bytes=GRANT),
        name=name,
    )


def in_hbm(array):
    return pltpu.with_memory_space_constraint(array, pltpu.HBM)


def dot(a, b):
    return jnp.dot(a, b, preferred_element_type=F32)


def dot_t(a, b):
    return lax.dot_general(a, b, (((1,), (1,)), ((), ())), preferred_element_type=F32)


def fill_ring(pad, value):
    pad[1:9, 1:9] = value
    pad[0, 1:9] = value[7]
    pad[9, 1:9] = value[0]
    pad[:, 0] = pad[:, 8]
    pad[:, 9] = pad[:, 1]


def ring_shift(pad, o0, o1, o2):
    moved = pad[pl.ds(1 + o0, B), pl.ds(1 + o1, B)].reshape(B * B, B, W)
    moved = pltpu.roll(moved, lax.rem(B - o2, B), 1)
    return moved.reshape(N, W)


def inside(offs, k):
    ok = None
    for which in range(3):
        at = lax.broadcasted_iota(jnp.int32, CUBE, which) + offs[k, which]
        one = (at >= 0) & (at < B)
        ok = one if ok is None else ok & one
    return ok


def fill_masks(rim):
    for d, axis in enumerate((GX, GY, GZ)):
        at, count = jnp.int32(0), 1
        for name in axis:
            size = lax.axis_size(name)
            at, count = at * size + lax.axis_index(name), count * size
        odd = at & 1
        flags = (1 - odd, jnp.where(at > 0, 1 - odd, 0), jnp.where(at < count - 1, odd, 0))
        for i, flag in enumerate(flags):
            rim[3 * d + i] = jnp.full((B, W), flag.astype(F32))


def forward_kernel(
    nodes_h, edges_h, w_in_h, w_out_h, offs_h,
    local, xa, xb, preact, hidden, nodes, edges, w_in, w_out, rim,
    pad, offs, sems,
):
    pairs = [(nodes_h, nodes), (w_in_h, w_in), (offs_h, offs), (w_out_h, w_out)]
    pairs += [(edges_h.at[k], edges.at[k]) for k in range(K)]
    copies = [pltpu.make_async_copy(a, b, sems.at[i]) for i, (a, b) in enumerate(pairs)]
    for copy in copies:
        copy.start()
    fill_masks(rim)
    for copy in copies[:3]:
        copy.wait()
    node = nodes[...]
    fill_ring(pad, dot(node, w_in[:W]).reshape(CUBE))
    receiver = dot(node, w_in[W : 2 * W])
    copies[3].wait()
    total = jnp.zeros((N, W), F32)
    for k in range(K):
        copies[4 + k].wait()
        pre = ring_shift(pad, offs[k, 0], offs[k, 1], offs[k, 2]) + receiver + dot(edges[k], w_in[2 * W :])
        preact[k] = pre
        act = (pre * jax.nn.sigmoid(pre)).reshape(CUBE)
        kept = jnp.where(inside(offs, k), act, 0.0).reshape(N, W).astype(BF16)
        hidden[k] = kept
        total = total + dot(kept, w_out[...])
    total = total.reshape(CUBE)
    local[...] = total
    send(rim, 0, total[0], total[B - 1], xa, xb)


def prepare_node_kernel(nodes, cot, w_in, w_out, pre, upstream, w_back):
    pre[...] = dot(nodes[...], w_in[:W])
    upstream[...] = dot_t(cot[...], w_out[...])
    w_back[...] = w_in[W:].T


def prepare_edge_kernel(offs, preact, hidden, nodes, edges, w_in, w_out, dact, hidden_t, left, w_out_t, w_back, pad):
    node = nodes[...]
    node_t = node.T
    fill_ring(pad, node.astype(F32).reshape(CUBE))
    for k in range(K):
        pre = preact[k]
        sigma = jax.nn.sigmoid(pre)
        rate = (sigma * (1.0 + pre * (1.0 - sigma))).reshape(CUBE)
        dact[k] = jnp.where(inside(offs, k), rate, 0.0).reshape(N, W)
        hidden_t[k * W : (k + 1) * W] = hidden[k].T
        here = pl.ds(k * N, N)
        left[:W, here] = ring_shift(pad, offs[k, 0], offs[k, 1], offs[k, 2]).astype(BF16).T
        left[W : 2 * W, here] = node_t
        left[2 * W :, here] = edges[k].T
    w_out_t[...] = w_out[...].T
    w_back[:W] = w_in[W : 2 * W].T
    w_back[W:] = w_in[:W].T


def low(rim, d, a, b):
    return jnp.where(rim[3 * d] > 0, jnp.where(rim[3 * d + 1] > 0, b, 0.0), a)


def high(rim, d, a, b):
    return jnp.where(rim[3 * d] > 0, a, jnp.where(rim[3 * d + 2] > 0, b, 0.0))


def send(rim, d, lo, hi, a, b):
    even = rim[3 * d] > 0
    a[...] = jnp.where(even, hi, lo)
    b[...] = jnp.where(even, lo, hi)


def add_x(rim, x, out):
    out[0] = out[0] + low(rim, 0, x[0][...], x[1][...])
    out[B - 1] = out[B - 1] + high(rim, 0, x[0][...], x[1][...])


def add_y(rim, y, out):
    out[:, 0] = out[:, 0] + low(rim, 1, y[0][...], y[1][...])
    out[:, B - 1] = out[:, B - 1] + high(rim, 1, y[0][...], y[1][...])


def add_z(rim, z, out):
    out[:, :, 0, :] = out[:, :, 0, :] + low(rim, 2, z[0][...], z[1][...])
    out[:, :, B - 1, :] = out[:, :, B - 1, :] + high(rim, 2, z[0][...], z[1][...])


def y_faces_after_x(rim, field, x0, x1, a, b, faces):
    for i, at in enumerate((0, B - 1)):
        faces[i] = field[:, at]
        faces[i, 0] = faces[i, 0] + low(rim, 0, x0[at], x1[at])
        faces[i, B - 1] = faces[i, B - 1] + high(rim, 0, x0[at], x1[at])
    send(rim, 1, faces[0], faces[1], a, b)


def z_faces_after_y(rim, field, x0, x1, y0, y1, a, b, faces):
    for i, at in enumerate((0, B - 1)):
        faces[i] = field[:, :, at, :]
        faces[i, 0] = faces[i, 0] + low(rim, 0, x0[:, at, :], x1[:, at, :])
        faces[i, B - 1] = faces[i, B - 1] + high(rim, 0, x0[:, at, :], x1[:, at, :])
        faces[i, :, 0, :] = faces[i, :, 0, :] + low(rim, 1, y0[:, at, :], y1[:, at, :])
        faces[i, :, B - 1, :] = faces[i, :, B - 1, :] + high(rim, 1, y0[:, at, :], y1[:, at, :])
    send(rim, 2, faces[0], faces[1], a, b)


def y_faces_after_z(rim, field, z0, z1, a, b, faces):
    for i, at in enumerate((0, B - 1)):
        faces[i] = field[:, at]
        faces[i, :, 0, :] = faces[i, :, 0, :] + low(rim, 2, z0[:, at, :], z1[:, at, :])
        faces[i, :, B - 1, :] = faces[i, :, B - 1, :] + high(rim, 2, z0[:, at, :], z1[:, at, :])
    send(rim, 1, faces[0], faces[1], a, b)


def x_faces_after_y(rim, field, z0, z1, y0, y1, a, b, faces):
    for i, at in enumerate((0, B - 1)):
        faces[i] = field[at]
        faces[i, :, 0, :] = faces[i, :, 0, :] + low(rim, 2, z0[at], z1[at])
        faces[i, :, B - 1, :] = faces[i, :, B - 1, :] + high(rim, 2, z0[at], z1[at])
        faces[i, 0] = faces[i, 0] + low(rim, 1, y0[at], y1[at])
        faces[i, B - 1] = faces[i, B - 1] + high(rim, 1, y0[at], y1[at])
    send(rim, 0, faces[0], faces[1], a, b)


def whole(rim, field, x0, x1, y0, y1, z0, z1, work):
    work[...] = field[...]
    add_x(rim, (x0, x1), work)
    add_y(rim, (y0, y1), work)
    add_z(rim, (z0, z1), work)
    return work[...].reshape(N, W)


def node_kernel(
    rim, field, x0, x1, y0, y1, z0, z1, inverse, begun, upstream, w_in, w_back,
    local, xa, xb, gathered, slope, hidden, work,
):
    inv = inverse[...]
    agg = (whole(rim, field, x0, x1, y0, y1, z0, z1, work) * inv).astype(BF16)
    gathered[...] = agg
    pre = begun[...] + dot(agg, w_in[W:])
    sigma = jax.nn.sigmoid(pre)
    hidden[...] = (pre * sigma).astype(BF16)
    slo = (upstream[...] * (sigma * (1.0 + pre * (1.0 - sigma)))).astype(BF16)
    slope[...] = slo
    part = (dot(slo, w_back[...]) * inv).reshape(CUBE)
    local[...] = part
    send(rim, 0, part[0], part[B - 1], xa, xb)


def node_grads_kernel(nodes, gathered, slope, hidden, cot, w_in, grads, base):
    slo = slope[...]
    grads[:W] = dot(nodes[...].T, slo)
    grads[W : 2 * W] = dot(gathered[...].T, slo)
    grads[2 * W :] = dot(hidden[...].T, cot[...])
    base[...] = cot[...].astype(F32) + dot_t(slo, w_in[:W])


def edge_kernel(
    rim, field, x0, x1, y0, y1, z0, z1, dact, hidden_t, left, w_out_t, node_grads, slopes, grads, work
):
    agg = whole(rim, field, x0, x1, y0, y1, z0, z1, work).astype(BF16)
    back = dot(agg, w_out_t[...])
    for k in range(K):
        slopes[k * N : (k + 1) * N] = (back * dact[k]).astype(BF16)
    outer = dot(hidden_t[...], agg)
    grads[3 * W : 4 * W] = (outer[:W] + outer[W : 2 * W]) + (outer[2 * W : 3 * W] + outer[3 * W :])
    grads[4 * W :] = node_grads[...]
    grads[: 3 * W] = dot(left[...], slopes[...])


def node_part_kernel(offs, rim, slopes, base, w_back, local, za, zb, pad):
    part = base[...]
    for k in range(K):
        slo = slopes[k * N : (k + 1) * N]
        fill_ring(pad, slo.astype(F32).reshape(CUBE))
        sent = ring_shift(pad, -offs[k, 0], -offs[k, 1], -offs[k, 2]).astype(BF16)
        part = part + dot(jnp.concatenate([slo, sent], axis=1), w_back[...])
    local[...] = part.reshape(CUBE)
    send(rim, 2, local[:, :, 0, :], local[:, :, B - 1, :], za, zb)


def edge_grad_kernel(slopes, w_in, out):
    out[...] = dot_t(slopes[...], w_in[2 * W :]).astype(BF16)


def last_kernel(rim, field, z0, z1, y0, y1, x0, x1, clipped, out, work):
    work[...] = field[...]
    add_z(rim, (z0, z1), work)
    add_y(rim, (y0, y1), work)
    add_x(rim, (x0, x1), work)
    out[...] = work[...].reshape(N, W).astype(BF16)


def fold(rows, pairs, copies, arrived, out):
    total = arrived[: 2 * rows]
    for i in range(1, pairs):
        total = total + arrived[2 * rows * i : 2 * rows * (i + 1)]
    total = total + jnp.concatenate([total[rows:], total[:rows]], axis=0)
    for i in range(copies):
        out[2 * rows * i : 2 * rows * (i + 1)] = total


def fold_with_faces_kernel(faces, rows, pairs, copies, arrived, *refs):
    fold(rows, pairs, copies, arrived, refs[-2])
    faces(*refs[:-2], refs[-1])


def clip_kernel(grads, edge_in, edge_out, node_in, node_out):
    total = grads[...]
    squares = jnp.sum(jnp.sum(total * total, axis=0, keepdims=True), axis=1, keepdims=True)
    factor = math.sqrt(7 * W * W) / jnp.sqrt(squares)
    edge_in[...] = total[: 3 * W] * factor
    edge_out[...] = total[3 * W : 4 * W] * factor
    node_in[...] = total[4 * W : 6 * W] * factor
    node_out[...] = total[6 * W :] * factor


def exchange(a, b, axis):
    count = lax.axis_size(axis)
    first = [(i, i ^ 1) for i in range(count)]
    second = [(i, min(max((i + 1) ^ 1, 1) - 1, count - 1)) for i in range(count)]
    b = lax.ppermute(b, axis, second)
    return lax.ppermute(a, axis, first), b


FACES = [(FACE, F32), (FACE, F32)]
BOTH = pltpu.VMEM((2, *FACE), F32)


def arrivals(rim, field, xa, xb, tag):
    x = exchange(xa, xb, GX)
    a, b = call(y_faces_after_x, FACES, [VMEM] * 4, "after_x" + tag, [BOTH])(rim, field, *x)
    y = exchange(a, b, GY)
    a, b = call(z_faces_after_y, FACES, [VMEM] * 6, "after_y" + tag, [BOTH])(rim, field, *x, *y)
    return (*x, *y, *exchange(a, b, GZ))


def swap(rows, axes):
    return lax.all_to_all(rows.reshape(lax.axis_size(axes), -1), axes, 0, 0, tiled=True).reshape(-1, W)


def arrivals_and_sum(rim, field, za, zb, grads):
    near, far = lax.axis_size(NEAR), lax.axis_size(FAR)
    rows = grads.shape[0] // near
    got = swap(grads, NEAR)
    z = exchange(za, zb, GZ)
    a, b, spread = call(
        functools.partial(fold_with_faces_kernel, y_faces_after_z, rows, near // 2, far // 2),
        FACES + [((rows * far, W), F32)],
        [VMEM] * 5,
        "after_z_fold",
        [BOTH],
    )(got, rim, field, *z)
    got = swap(spread, FAR)
    y = exchange(a, b, GY)
    a, b, spread = call(
        functools.partial(fold_with_faces_kernel, x_faces_after_y, rows, far // 2, near // 2),
        FACES + [((rows * near, W), F32)],
        [VMEM] * 7,
        "after_y_fold",
        [BOTH],
    )(got, rim, field, *z, *y)
    total = swap(spread, NEAR)
    return (*z, *y, *exchange(a, b, GX)), total


def on_device(node_feat, edge_feat, copies, offsets, w_edge_in, w_edge_out, w_node_in, w_node_out, node_cot):
    cot = node_cot.reshape(N, W)
    inverse = jnp.broadcast_to(1.0 / copies.reshape(N, 1).astype(F32), (N, W))
    square = ((W, W), BF16)
    many = ((K, N, W), BF16)

    local, xa, xb, preact, hidden, nodes, edges, w_in, w_out, rim = call(
        forward_kernel,
        [(CUBE, F32)] + FACES + [((K, N, W), F32), many, ((N, W), BF16), many, ((3 * W, W), BF16), square, ((9, B, W), F32)],
        [HBM] * 5,
        "forward",
        [PAD, pltpu.SMEM((K, 3), jnp.int32), pltpu.SemaphoreType.DMA((4 + K,))],
    )(*map(in_hbm, (node_feat.reshape(N, W), edge_feat.reshape(K, N, W), w_edge_in, w_edge_out, offsets)))
    begun, upstream, w_node_back = call(
        prepare_node_kernel, [((N, W), F32), ((N, W), F32), square], [VMEM] * 4, "prepare_node"
    )(nodes, cot, w_node_in, w_node_out)
    arrived = arrivals(rim, local, xa, xb, "_1")
    dact, hidden_t, left, w_out_t, w_back = call(
        prepare_edge_kernel,
        [((K, N, W), F32), ((K * W, N), BF16), ((3 * W, K * N), BF16), square, ((2 * W, W), BF16)],
        [SMEM] + [VMEM] * 6,
        "prepare_edge",
        [PAD],
    )(offsets, preact, hidden, nodes, edges, w_in, w_out)
    local, xa, xb, gathered, slope, node_hidden = call(
        node_kernel, [(CUBE, F32)] + FACES + [((N, W), BF16)] * 3, [VMEM] * 13, "node", [WORK]
    )(rim, local, *arrived, inverse, begun, upstream, w_node_in, w_node_back)
    arrived = arrivals(rim, local, xa, xb, "_2")
    node_grads, base = call(node_grads_kernel, [((3 * W, W), F32), ((N, W), F32)], [VMEM] * 6, "node_grads")(
        nodes, gathered, slope, node_hidden, cot, w_node_in
    )
    slopes, grads = call(
        edge_kernel, [((K * N, W), BF16), ((7 * W, W), F32)], [VMEM] * 13, "edge", [WORK]
    )(rim, local, *arrived, dact, hidden_t, left, w_out_t, node_grads)
    local, za, zb = call(
        node_part_kernel, [(CUBE, F32)] + FACES, [SMEM] + [VMEM] * 4, "node_part", [PAD]
    )(offsets, rim, slopes, base, w_back)
    arrived, total = arrivals_and_sum(rim, local, za, zb, grads)
    (edge_grad,) = call(edge_grad_kernel, [((K * N, W), BF16)], [VMEM] * 2, "edge_grad")(slopes, w_in)
    clipped = call(
        clip_kernel, [((3 * W, W), F32), ((W, W), F32), ((2 * W, W), F32), ((W, W), F32)], [VMEM], "clip"
    )(total)
    (node_grad,) = call(last_kernel, [((N, W), BF16)], [VMEM] * 8 + [HBM], "last", [WORK])(
        rim, local, *arrived, in_hbm(clipped[1])
    )
    return (node_grad.reshape(node_feat.shape), edge_grad.reshape(edge_feat.shape), *clipped)


def solution(mesh):
    split = Mesh(mesh.devices.reshape(8, 2, 2, 2, 4), ("z", "yh", "yl", "c", "x"))
    place = (GX, GY, GZ)
    placed = (
        P(*place, None),
        P(None, *place, None),
        P(*place),
        P(),
        P(),
        P(),
        P(),
        P(),
        P(*place, None),
    )
    return jax.shard_map(
        on_device,
        mesh=split,
        in_specs=placed,
        out_specs=(P(*place, None), P(None, *place, None), P(), P(), P(), P()),
        check_vma=False,
    )
```

```python
import functools
import itertools
import math

import jax
import jax.numpy as jnp
from jax import lax
from jax.experimental import pallas as pl
from jax.experimental.pallas import tpu as pltpu
from jax.sharding import Mesh
from jax.sharding import PartitionSpec as P

B = 8
W = 128
K = 4
N = B * B * B
CUBE = (B, B, B, W)
FACE = (B, B, W)
F32 = jnp.float32
BF16 = jnp.bfloat16
GRANT = 12 * 1024 * 1024

VMEM = pl.BlockSpec(memory_space=pltpu.VMEM)
SMEM = pl.BlockSpec(memory_space=pltpu.SMEM)
HBM = pl.BlockSpec(memory_space=pltpu.HBM)
PAD = pltpu.VMEM((B + 2, B + 2, B, W), F32)
WORK = pltpu.VMEM(CUBE, F32)

GX, GY, GZ = ("z", "yh"), ("yl", "c"), ("x",)
NEAR, FAR = ("yh", "yl", "c", "x"), ("z",)


def call(body, outs, specs, name, scratch=()):
    return pl.pallas_call(
        body,
        out_shape=[jax.ShapeDtypeStruct(s, t) for s, t in outs],
        in_specs=specs,
        out_specs=[VMEM] * len(outs),
        scratch_shapes=list(scratch),
        compiler_params=pltpu.CompilerParams(vmem_limit_bytes=GRANT),
        name=name,
    )


def in_hbm(array):
    return pltpu.with_memory_space_constraint(array, pltpu.HBM)


def dot(a, b):
    return jnp.dot(a, b, preferred_element_type=F32)


def dot_t(a, b):
    return lax.dot_general(a, b, (((1,), (1,)), ((), ())), preferred_element_type=F32)


def fill_ring(pad, value):
    pad[1:9, 1:9] = value
    pad[0, 1:9] = value[7]
    pad[9, 1:9] = value[0]
    pad[:, 0] = pad[:, 8]
    pad[:, 9] = pad[:, 1]


def ring_shift(pad, o0, o1, o2):
    moved = pad[pl.ds(1 + o0, B), pl.ds(1 + o1, B)].reshape(B * B, B, W)
    moved = pltpu.roll(moved, lax.rem(B - o2, B), 1)
    return moved.reshape(N, W)


def inside(offs, k):
    ok = None
    for which in range(3):
        at = lax.broadcasted_iota(jnp.int32, CUBE, which) + offs[k, which]
        one = (at >= 0) & (at < B)
        ok = one if ok is None else ok & one
    return ok


def fill_masks(rim):
    for d, axis in enumerate((GX, GY, GZ)):
        at, count = jnp.int32(0), 1
        for name in axis:
            size = lax.axis_size(name)
            at, count = at * size + lax.axis_index(name), count * size
        odd = at & 1
        flags = (1 - odd, jnp.where(at > 0, 1 - odd, 0), jnp.where(at < count - 1, odd, 0))
        for i, flag in enumerate(flags):
            rim[3 * d + i] = jnp.full((B, W), flag.astype(F32))


def forward_kernel(
    nodes_h, edges_h, w_in_h, w_out_h, offs_h,
    local, xa, xb, preact, hidden, nodes, edges, w_in, w_out, rim,
    pad, offs, sems,
):
    pairs = [(nodes_h, nodes), (w_in_h, w_in), (offs_h, offs), (w_out_h, w_out)]
    pairs += [(edges_h.at[k], edges.at[k]) for k in range(K)]
    copies = [pltpu.make_async_copy(a, b, sems.at[i]) for i, (a, b) in enumerate(pairs)]
    for copy in copies:
        copy.start()
    fill_masks(rim)
    for copy in copies[:3]:
        copy.wait()
    node = nodes[...]
    fill_ring(pad, dot(node, w_in[:W]).reshape(CUBE))
    receiver = dot(node, w_in[W : 2 * W])
    copies[3].wait()
    total = jnp.zeros((N, W), F32)
    for k in range(K):
        copies[4 + k].wait()
        pre = ring_shift(pad, offs[k, 0], offs[k, 1], offs[k, 2]) + receiver + dot(edges[k], w_in[2 * W :])
        preact[k] = pre
        act = (pre * jax.nn.sigmoid(pre)).reshape(CUBE)
        kept = jnp.where(inside(offs, k), act, 0.0).reshape(N, W).astype(BF16)
        hidden[k] = kept
        total = total + dot(kept, w_out[...])
    total = total.reshape(CUBE)
    local[...] = total
    send(rim, 0, total[0], total[B - 1], xa, xb)


def prepare_node_kernel(nodes, cot, w_in, w_out, pre, upstream, w_back):
    pre[...] = dot(nodes[...], w_in[:W])
    upstream[...] = dot_t(cot[...], w_out[...])
    w_back[...] = w_in[W:].T


def prepare_edge_kernel(offs, preact, hidden, nodes, edges, w_in, w_out, dact, hidden_t, left, w_out_t, w_back, pad):
    node = nodes[...]
    node_t = node.T
    fill_ring(pad, node.astype(F32).reshape(CUBE))
    for k in range(K):
        pre = preact[k]
        sigma = jax.nn.sigmoid(pre)
        rate = (sigma * (1.0 + pre * (1.0 - sigma))).reshape(CUBE)
        dact[k] = jnp.where(inside(offs, k), rate, 0.0).reshape(N, W)
        hidden_t[k * W : (k + 1) * W] = hidden[k].T
        here = pl.ds(k * N, N)
        left[:W, here] = ring_shift(pad, offs[k, 0], offs[k, 1], offs[k, 2]).astype(BF16).T
        left[W : 2 * W, here] = node_t
        left[2 * W :, here] = edges[k].T
    w_out_t[...] = w_out[...].T
    w_back[:W] = w_in[W : 2 * W].T
    w_back[W:] = w_in[:W].T


def low(rim, d, a, b):
    return jnp.where(rim[3 * d] > 0, jnp.where(rim[3 * d + 1] > 0, a, 0.0), b)


def high(rim, d, a, b):
    return jnp.where(rim[3 * d] > 0, b, jnp.where(rim[3 * d + 2] > 0, a, 0.0))


def send(rim, d, lo, hi, a, b):
    even = rim[3 * d] > 0
    a[...] = jnp.where(even, lo, hi)
    b[...] = jnp.where(even, hi, lo)


def add_x(rim, x, out):
    out[0] = out[0] + low(rim, 0, x[0][...], x[1][...])
    out[B - 1] = out[B - 1] + high(rim, 0, x[0][...], x[1][...])


def add_y(rim, y, out):
    out[:, 0] = out[:, 0] + low(rim, 1, y[0][...], y[1][...])
    out[:, B - 1] = out[:, B - 1] + high(rim, 1, y[0][...], y[1][...])


def add_z(rim, z, out):
    out[:, :, 0, :] = out[:, :, 0, :] + low(rim, 2, z[0][...], z[1][...])
    out[:, :, B - 1, :] = out[:, :, B - 1, :] + high(rim, 2, z[0][...], z[1][...])


def y_faces_after_x(rim, field, x0, x1, a, b, faces):
    for i, at in enumerate((0, B - 1)):
        faces[i] = field[:, at]
        faces[i, 0] = faces[i, 0] + low(rim, 0, x0[at], x1[at])
        faces[i, B - 1] = faces[i, B - 1] + high(rim, 0, x0[at], x1[at])
    send(rim, 1, faces[0], faces[1], a, b)


def z_faces_after_y(rim, field, x0, x1, y0, y1, a, b, faces):
    for i, at in enumerate((0, B - 1)):
        faces[i] = field[:, :, at, :]
        faces[i, 0] = faces[i, 0] + low(rim, 0, x0[:, at, :], x1[:, at, :])
        faces[i, B - 1] = faces[i, B - 1] + high(rim, 0, x0[:, at, :], x1[:, at, :])
        faces[i, :, 0, :] = faces[i, :, 0, :] + low(rim, 1, y0[:, at, :], y1[:, at, :])
        faces[i, :, B - 1, :] = faces[i, :, B - 1, :] + high(rim, 1, y0[:, at, :], y1[:, at, :])
    send(rim, 2, faces[0], faces[1], a, b)


def y_faces_after_z(rim, field, z0, z1, a, b, faces):
    for i, at in enumerate((0, B - 1)):
        faces[i] = field[:, at]
        faces[i, :, 0, :] = faces[i, :, 0, :] + low(rim, 2, z0[:, at, :], z1[:, at, :])
        faces[i, :, B - 1, :] = faces[i, :, B - 1, :] + high(rim, 2, z0[:, at, :], z1[:, at, :])
    send(rim, 1, faces[0], faces[1], a, b)


def x_faces_after_y(rim, field, z0, z1, y0, y1, a, b, faces):
    for i, at in enumerate((0, B - 1)):
        faces[i] = field[at]
        faces[i, :, 0, :] = faces[i, :, 0, :] + low(rim, 2, z0[at], z1[at])
        faces[i, :, B - 1, :] = faces[i, :, B - 1, :] + high(rim, 2, z0[at], z1[at])
        faces[i, 0] = faces[i, 0] + low(rim, 1, y0[at], y1[at])
        faces[i, B - 1] = faces[i, B - 1] + high(rim, 1, y0[at], y1[at])
    send(rim, 0, faces[0], faces[1], a, b)


def whole(rim, field, x0, x1, y0, y1, z0, z1, work):
    work[...] = field[...]
    add_x(rim, (x0, x1), work)
    add_y(rim, (y0, y1), work)
    add_z(rim, (z0, z1), work)
    return work[...].reshape(N, W)


def node_kernel(
    rim, field, x0, x1, y0, y1, z0, z1, inverse, begun, upstream, w_in, w_back,
    local, xa, xb, gathered, slope, hidden, work,
):
    inv = inverse[...]
    agg = (whole(rim, field, x0, x1, y0, y1, z0, z1, work) * inv).astype(BF16)
    gathered[...] = agg
    pre = begun[...] + dot(agg, w_in[W:])
    sigma = jax.nn.sigmoid(pre)
    hidden[...] = (pre * sigma).astype(BF16)
    slo = (upstream[...] * (sigma * (1.0 + pre * (1.0 - sigma)))).astype(BF16)
    slope[...] = slo
    part = (dot(slo, w_back[...]) * inv).reshape(CUBE)
    local[...] = part
    send(rim, 0, part[0], part[B - 1], xa, xb)


def node_grads_kernel(nodes, gathered, slope, hidden, cot, w_in, grads, base):
    slo = slope[...]
    grads[:W] = dot(nodes[...].T, slo)
    grads[W : 2 * W] = dot(gathered[...].T, slo)
    grads[2 * W :] = dot(hidden[...].T, cot[...])
    base[...] = cot[...].astype(F32) + dot_t(slo, w_in[:W])


def edge_kernel(
    rim, field, x0, x1, y0, y1, z0, z1, dact, hidden_t, left, w_out_t, node_grads, slopes, grads, work
):
    agg = whole(rim, field, x0, x1, y0, y1, z0, z1, work).astype(BF16)
    back = dot(agg, w_out_t[...])
    for k in range(K):
        slopes[k * N : (k + 1) * N] = (back * dact[k]).astype(BF16)
    outer = dot(hidden_t[...], agg)
    grads[3 * W : 4 * W] = (outer[:W] + outer[W : 2 * W]) + (outer[2 * W : 3 * W] + outer[3 * W :])
    grads[4 * W :] = node_grads[...]
    grads[: 3 * W] = dot(left[...], slopes[...])


def node_part_kernel(offs, rim, slopes, base, w_back, local, za, zb, pad):
    part = base[...]
    for k in range(K):
        slo = slopes[k * N : (k + 1) * N]
        fill_ring(pad, slo.astype(F32).reshape(CUBE))
        sent = ring_shift(pad, -offs[k, 0], -offs[k, 1], -offs[k, 2]).astype(BF16)
        part = part + dot(jnp.concatenate([slo, sent], axis=1), w_back[...])
    local[...] = part.reshape(CUBE)
    send(rim, 2, local[:, :, 0, :], local[:, :, B - 1, :], za, zb)


def edge_grad_kernel(slopes, w_in, out):
    out[...] = dot_t(slopes[...], w_in[2 * W :]).astype(BF16)


def last_kernel(rim, field, z0, z1, y0, y1, x0, x1, clipped, out, work):
    work[...] = field[...]
    add_z(rim, (z0, z1), work)
    add_y(rim, (y0, y1), work)
    add_x(rim, (x0, x1), work)
    out[...] = work[...].reshape(N, W).astype(BF16)


def fold(rows, pairs, copies, arrived, out):
    total = arrived[: 2 * rows]
    for i in range(1, pairs):
        total = total + arrived[2 * rows * i : 2 * rows * (i + 1)]
    total = total + jnp.concatenate([total[rows:], total[:rows]], axis=0)
    for i in range(copies):
        out[2 * rows * i : 2 * rows * (i + 1)] = total


def fold_with_faces_kernel(faces, rows, pairs, copies, arrived, *refs):
    fold(rows, pairs, copies, arrived, refs[-2])
    faces(*refs[:-2], refs[-1])


def clip_kernel(grads, edge_in, edge_out, node_in, node_out):
    total = grads[...]
    squares = jnp.sum(jnp.sum(total * total, axis=0, keepdims=True), axis=1, keepdims=True)
    factor = math.sqrt(7 * W * W) / jnp.sqrt(squares)
    edge_in[...] = total[: 3 * W] * factor
    edge_out[...] = total[3 * W : 4 * W] * factor
    node_in[...] = total[4 * W : 6 * W] * factor
    node_out[...] = total[6 * W :] * factor


def exchange(a, b, which):
    sizes = [lax.axis_size(axis) for axis in (GX, GY, GZ)]
    aside = {0: 1, 1: 2, 2: 1}[which]
    first, second = [], []
    for me in itertools.product(*map(range, sizes)):
        at = ((me[which] + 1) ^ 1) - 1
        end = at < 0 or at >= sizes[which]
        first.append(moved_to(me, aside, me[aside] ^ 1) if end else moved_to(me, which, at))
        second.append(moved_to(me, which, me[which] ^ 1))
    ranks = {me: rank for rank, me in enumerate(itertools.product(*map(range, sizes)))}
    a, b = (
        lax.ppermute(face, GX + GY + GZ, [(rank, ranks[to]) for rank, to in enumerate(targets)])
        for face, targets in ((a, first), (b, second))
    )
    return a, b


def moved_to(me, which, at):
    return me[:which] + (at,) + me[which + 1 :]


FACES = [(FACE, F32), (FACE, F32)]
BOTH = pltpu.VMEM((2, *FACE), F32)


def arrivals(rim, field, xa, xb, tag):
    x = exchange(xa, xb, 0)
    a, b = call(y_faces_after_x, FACES, [VMEM] * 4, "after_x" + tag, [BOTH])(rim, field, *x)
    y = exchange(a, b, 1)
    a, b = call(z_faces_after_y, FACES, [VMEM] * 6, "after_y" + tag, [BOTH])(rim, field, *x, *y)
    return (*x, *y, *exchange(a, b, 2))


def swap(rows, axes):
    return lax.all_to_all(rows.reshape(lax.axis_size(axes), -1), axes, 0, 0, tiled=True).reshape(-1, W)


def arrivals_and_sum(rim, field, za, zb, grads):
    near, far = lax.axis_size(NEAR), lax.axis_size(FAR)
    rows = grads.shape[0] // near
    got = swap(grads, NEAR)
    z = exchange(za, zb, 2)
    a, b, spread = call(
        functools.partial(fold_with_faces_kernel, y_faces_after_z, rows, near // 2, far // 2),
        FACES + [((rows * far, W), F32)],
        [VMEM] * 5,
        "after_z_fold",
        [BOTH],
    )(got, rim, field, *z)
    got = swap(spread, FAR)
    y = exchange(a, b, 1)
    a, b, spread = call(
        functools.partial(fold_with_faces_kernel, x_faces_after_y, rows, far // 2, near // 2),
        FACES + [((rows * near, W), F32)],
        [VMEM] * 7,
        "after_y_fold",
        [BOTH],
    )(got, rim, field, *z, *y)
    total = swap(spread, NEAR)
    return (*z, *y, *exchange(a, b, 0)), total


def on_device(node_feat, edge_feat, copies, offsets, w_edge_in, w_edge_out, w_node_in, w_node_out, node_cot):
    cot = node_cot.reshape(N, W)
    inverse = jnp.broadcast_to(1.0 / copies.reshape(N, 1).astype(F32), (N, W))
    square = ((W, W), BF16)
    many = ((K, N, W), BF16)

    local, xa, xb, preact, hidden, nodes, edges, w_in, w_out, rim = call(
        forward_kernel,
        [(CUBE, F32)] + FACES + [((K, N, W), F32), many, ((N, W), BF16), many, ((3 * W, W), BF16), square, ((9, B, W), F32)],
        [HBM] * 5,
        "forward",
        [PAD, pltpu.SMEM((K, 3), jnp.int32), pltpu.SemaphoreType.DMA((4 + K,))],
    )(*map(in_hbm, (node_feat.reshape(N, W), edge_feat.reshape(K, N, W), w_edge_in, w_edge_out, offsets)))
    begun, upstream, w_node_back = call(
        prepare_node_kernel, [((N, W), F32), ((N, W), F32), square], [VMEM] * 4, "prepare_node"
    )(nodes, cot, w_node_in, w_node_out)
    arrived = arrivals(rim, local, xa, xb, "_1")
    dact, hidden_t, left, w_out_t, w_back = call(
        prepare_edge_kernel,
        [((K, N, W), F32), ((K * W, N), BF16), ((3 * W, K * N), BF16), square, ((2 * W, W), BF16)],
        [SMEM] + [VMEM] * 6,
        "prepare_edge",
        [PAD],
    )(offsets, preact, hidden, nodes, edges, w_in, w_out)
    local, xa, xb, gathered, slope, node_hidden = call(
        node_kernel, [(CUBE, F32)] + FACES + [((N, W), BF16)] * 3, [VMEM] * 13, "node", [WORK]
    )(rim, local, *arrived, inverse, begun, upstream, w_node_in, w_node_back)
    arrived = arrivals(rim, local, xa, xb, "_2")
    node_grads, base = call(node_grads_kernel, [((3 * W, W), F32), ((N, W), F32)], [VMEM] * 6, "node_grads")(
        nodes, gathered, slope, node_hidden, cot, w_node_in
    )
    slopes, grads = call(
        edge_kernel, [((K * N, W), BF16), ((7 * W, W), F32)], [VMEM] * 13, "edge", [WORK]
    )(rim, local, *arrived, dact, hidden_t, left, w_out_t, node_grads)
    local, za, zb = call(
        node_part_kernel, [(CUBE, F32)] + FACES, [SMEM] + [VMEM] * 4, "node_part", [PAD]
    )(offsets, rim, slopes, base, w_back)
    arrived, total = arrivals_and_sum(rim, local, za, zb, grads)
    (edge_grad,) = call(edge_grad_kernel, [((K * N, W), BF16)], [VMEM] * 2, "edge_grad")(slopes, w_in)
    clipped = call(
        clip_kernel, [((3 * W, W), F32), ((W, W), F32), ((2 * W, W), F32), ((W, W), F32)], [VMEM], "clip"
    )(total)
    (node_grad,) = call(last_kernel, [((N, W), BF16)], [VMEM] * 8 + [HBM], "last", [WORK])(
        rim, local, *arrived, in_hbm(clipped[1])
    )
    return (node_grad.reshape(node_feat.shape), edge_grad.reshape(edge_feat.shape), *clipped)


def solution(mesh):
    split = Mesh(mesh.devices.reshape(8, 2, 2, 2, 4), ("z", "yh", "yl", "c", "x"))
    place = (GX, GY, GZ)
    placed = (
        P(*place, None),
        P(None, *place, None),
        P(*place),
        P(),
        P(),
        P(),
        P(),
        P(),
        P(*place, None),
    )
    return jax.shard_map(
        on_device,
        mesh=split,
        in_specs=placed,
        out_specs=(P(*place, None), P(None, *place, None), P(), P(), P(), P()),
        check_vma=False,
    )
```

```python
import functools
import itertools
import math

import jax
import jax.numpy as jnp
from jax import lax
from jax.experimental import pallas as pl
from jax.experimental.pallas import tpu as pltpu
from jax.sharding import Mesh
from jax.sharding import PartitionSpec as P

B = 8
W = 128
K = 4
N = B * B * B
CUBE = (B, B, B, W)
FACE = (B, B, W)
F32 = jnp.float32
BF16 = jnp.bfloat16
GRANT = 12 * 1024 * 1024

VMEM = pl.BlockSpec(memory_space=pltpu.VMEM)
SMEM = pl.BlockSpec(memory_space=pltpu.SMEM)
HBM = pl.BlockSpec(memory_space=pltpu.HBM)
PAD = pltpu.VMEM((B + 2, B + 2, B, W), F32)
WORK = pltpu.VMEM(CUBE, F32)

GX, GY, GZ = ("z", "yh"), ("yl", "c"), ("x",)
NEAR, FAR = ("yh", "yl", "x"), ("z",)


def call(body, outs, specs, name, scratch=()):
    return pl.pallas_call(
        body,
        out_shape=[jax.ShapeDtypeStruct(s, t) for s, t in outs],
        in_specs=specs,
        out_specs=[VMEM] * len(outs),
        scratch_shapes=list(scratch),
        compiler_params=pltpu.CompilerParams(vmem_limit_bytes=GRANT),
        name=name,
    )


def in_hbm(array):
    return pltpu.with_memory_space_constraint(array, pltpu.HBM)


def dot(a, b):
    return jnp.dot(a, b, preferred_element_type=F32)


def dot_t(a, b):
    return lax.dot_general(a, b, (((1,), (1,)), ((), ())), preferred_element_type=F32)


def fill_ring(pad, value):
    pad[1:9, 1:9] = value
    pad[0, 1:9] = value[7]
    pad[9, 1:9] = value[0]
    pad[:, 0] = pad[:, 8]
    pad[:, 9] = pad[:, 1]


def ring_shift(pad, o0, o1, o2):
    moved = pad[pl.ds(1 + o0, B), pl.ds(1 + o1, B)].reshape(B * B, B, W)
    moved = pltpu.roll(moved, lax.rem(B - o2, B), 1)
    return moved.reshape(N, W)


def inside(offs, k):
    ok = None
    for which in range(3):
        at = lax.broadcasted_iota(jnp.int32, CUBE, which) + offs[k, which]
        one = (at >= 0) & (at < B)
        ok = one if ok is None else ok & one
    return ok


def fill_masks(rim):
    for d, axis in enumerate((GX, GY, GZ)):
        at, count = jnp.int32(0), 1
        for name in axis:
            size = lax.axis_size(name)
            at, count = at * size + lax.axis_index(name), count * size
        odd = at & 1
        flags = (1 - odd, jnp.where(at > 0, 1 - odd, 0), jnp.where(at < count - 1, odd, 0))
        for i, flag in enumerate(flags):
            rim[3 * d + i] = jnp.full((B, W), flag.astype(F32))


def forward_kernel(
    nodes_h, edges_h, w_in_h, w_out_h, offs_h,
    local, xa, xb, preact, hidden, nodes, edges, w_in, w_out, rim,
    pad, offs, sems,
):
    pairs = [(nodes_h, nodes), (w_in_h, w_in), (offs_h, offs), (w_out_h, w_out)]
    pairs += [(edges_h.at[k], edges.at[k]) for k in range(K)]
    copies = [pltpu.make_async_copy(a, b, sems.at[i]) for i, (a, b) in enumerate(pairs)]
    for copy in copies:
        copy.start()
    fill_masks(rim)
    for copy in copies[:3]:
        copy.wait()
    node = nodes[...]
    fill_ring(pad, dot(node, w_in[:W]).reshape(CUBE))
    receiver = dot(node, w_in[W : 2 * W])
    copies[3].wait()
    total = jnp.zeros((N, W), F32)
    for k in range(K):
        copies[4 + k].wait()
        pre = ring_shift(pad, offs[k, 0], offs[k, 1], offs[k, 2]) + receiver + dot(edges[k], w_in[2 * W :])
        preact[k] = pre
        act = (pre * jax.nn.sigmoid(pre)).reshape(CUBE)
        kept = jnp.where(inside(offs, k), act, 0.0).reshape(N, W).astype(BF16)
        hidden[k] = kept
        total = total + dot(kept, w_out[...])
    total = total.reshape(CUBE)
    local[...] = total
    send(rim, 0, total[0], total[B - 1], xa, xb)


def prepare_node_kernel(nodes, cot, w_in, w_out, pre, upstream, w_back):
    pre[...] = dot(nodes[...], w_in[:W])
    upstream[...] = dot_t(cot[...], w_out[...])
    w_back[...] = w_in[W:].T


def prepare_edge_kernel(offs, preact, hidden, nodes, edges, w_in, w_out, dact, hidden_t, left, w_out_t, w_back, pad):
    node = nodes[...]
    node_t = node.T
    fill_ring(pad, node.astype(F32).reshape(CUBE))
    for k in range(K):
        pre = preact[k]
        sigma = jax.nn.sigmoid(pre)
        rate = (sigma * (1.0 + pre * (1.0 - sigma))).reshape(CUBE)
        dact[k] = jnp.where(inside(offs, k), rate, 0.0).reshape(N, W)
        hidden_t[k * W : (k + 1) * W] = hidden[k].T
        here = pl.ds(k * N, N)
        left[:W, here] = ring_shift(pad, offs[k, 0], offs[k, 1], offs[k, 2]).astype(BF16).T
        left[W : 2 * W, here] = node_t
        left[2 * W :, here] = edges[k].T
    w_out_t[...] = w_out[...].T
    w_back[:W] = w_in[W : 2 * W].T
    w_back[W:] = w_in[:W].T


def low(rim, d, a, b):
    return jnp.where(rim[3 * d] > 0, jnp.where(rim[3 * d + 1] > 0, a, 0.0), b)


def high(rim, d, a, b):
    return jnp.where(rim[3 * d] > 0, b, jnp.where(rim[3 * d + 2] > 0, a, 0.0))


def send(rim, d, lo, hi, a, b):
    even = rim[3 * d] > 0
    a[...] = jnp.where(even, lo, hi)
    b[...] = jnp.where(even, hi, lo)


def own(rim, top, bottom):
    first = jnp.broadcast_to(rim[3, :1, :], top.shape) > 0
    return jnp.where(first, top, bottom)


def add_kernel(keep, got, after, out):
    out[...] = keep[...] + got[...]


def add_x(rim, x, out):
    out[0] = out[0] + low(rim, 0, x[0][...], x[1][...])
    out[B - 1] = out[B - 1] + high(rim, 0, x[0][...], x[1][...])


def add_y(rim, y, out):
    out[:, 0] = out[:, 0] + low(rim, 1, y[0][...], y[1][...])
    out[:, B - 1] = out[:, B - 1] + high(rim, 1, y[0][...], y[1][...])


def add_z(rim, z, out):
    out[:, :, 0, :] = out[:, :, 0, :] + low(rim, 2, z[0][...], z[1][...])
    out[:, :, B - 1, :] = out[:, :, B - 1, :] + high(rim, 2, z[0][...], z[1][...])


def y_faces_after_x(rim, field, x0, x1, a, b, faces):
    for i, at in enumerate((0, B - 1)):
        faces[i] = field[:, at]
        faces[i, 0] = faces[i, 0] + low(rim, 0, x0[at], x1[at])
        faces[i, B - 1] = faces[i, B - 1] + high(rim, 0, x0[at], x1[at])
    send(rim, 1, faces[0], faces[1], a, b)


def z_faces_after_y(rim, field, x0, x1, y0, y1, a, b, faces):
    for i, at in enumerate((0, B - 1)):
        faces[i] = field[:, :, at, :]
        faces[i, 0] = faces[i, 0] + low(rim, 0, x0[:, at, :], x1[:, at, :])
        faces[i, B - 1] = faces[i, B - 1] + high(rim, 0, x0[:, at, :], x1[:, at, :])
        faces[i, :, 0, :] = faces[i, :, 0, :] + low(rim, 1, y0[:, at, :], y1[:, at, :])
        faces[i, :, B - 1, :] = faces[i, :, B - 1, :] + high(rim, 1, y0[:, at, :], y1[:, at, :])
    send(rim, 2, faces[0], faces[1], a, b)


def y_faces_after_z(rim, field, z0, z1, a, b, faces):
    for i, at in enumerate((0, B - 1)):
        faces[i] = field[:, at]
        faces[i, :, 0, :] = faces[i, :, 0, :] + low(rim, 2, z0[:, at, :], z1[:, at, :])
        faces[i, :, B - 1, :] = faces[i, :, B - 1, :] + high(rim, 2, z0[:, at, :], z1[:, at, :])
    send(rim, 1, faces[0], faces[1], a, b)


def x_faces_after_y(rim, field, z0, z1, y0, y1, a, b, faces):
    for i, at in enumerate((0, B - 1)):
        faces[i] = field[at]
        faces[i, :, 0, :] = faces[i, :, 0, :] + low(rim, 2, z0[at], z1[at])
        faces[i, :, B - 1, :] = faces[i, :, B - 1, :] + high(rim, 2, z0[at], z1[at])
        faces[i, 0] = faces[i, 0] + low(rim, 1, y0[at], y1[at])
        faces[i, B - 1] = faces[i, B - 1] + high(rim, 1, y0[at], y1[at])
    send(rim, 0, faces[0], faces[1], a, b)


def whole(rim, field, x0, x1, y0, y1, z0, z1, work):
    work[...] = field[...]
    add_x(rim, (x0, x1), work)
    add_y(rim, (y0, y1), work)
    add_z(rim, (z0, z1), work)
    return work[...].reshape(N, W)


def node_kernel(
    rim, field, x0, x1, y0, y1, z0, z1, inverse, begun, upstream, w_in, w_back,
    local, xa, xb, gathered, slope, hidden, work,
):
    inv = inverse[...]
    agg = (whole(rim, field, x0, x1, y0, y1, z0, z1, work) * inv).astype(BF16)
    gathered[...] = agg
    pre = begun[...] + dot(agg, w_in[W:])
    sigma = jax.nn.sigmoid(pre)
    hidden[...] = (pre * sigma).astype(BF16)
    slo = (upstream[...] * (sigma * (1.0 + pre * (1.0 - sigma)))).astype(BF16)
    slope[...] = slo
    part = (dot(slo, w_back[...]) * inv).reshape(CUBE)
    local[...] = part
    send(rim, 0, part[0], part[B - 1], xa, xb)


def node_grads_kernel(nodes, gathered, slope, hidden, cot, w_in, grads, base):
    slo = slope[...]
    grads[:W] = dot(nodes[...].T, slo)
    grads[W : 2 * W] = dot(gathered[...].T, slo)
    grads[2 * W :] = dot(hidden[...].T, cot[...])
    base[...] = cot[...].astype(F32) + dot_t(slo, w_in[:W])


def edge_kernel(
    rim, field, x0, x1, y0, y1, z0, z1, dact, hidden_t, left, w_out_t, node_grads, slopes, keep, give, work, grads
):
    agg = whole(rim, field, x0, x1, y0, y1, z0, z1, work).astype(BF16)
    back = dot(agg, w_out_t[...])
    for k in range(K):
        slopes[k * N : (k + 1) * N] = (back * dact[k]).astype(BF16)
    outer = dot(hidden_t[...], agg)
    grads[3 * W : 4 * W] = (outer[:W] + outer[W : 2 * W]) + (outer[2 * W : 3 * W] + outer[3 * W :])
    grads[4 * W :] = node_grads[...]
    grads[: 3 * W] = dot(left[...], slopes[...])
    half = keep.shape[0]
    keep[...] = own(rim, grads[:half], grads[half:])
    give[...] = own(rim, grads[half:], grads[:half])


def node_part_kernel(offs, rim, slopes, base, w_back, local, za, zb, pad):
    part = base[...]
    for k in range(K):
        slo = slopes[k * N : (k + 1) * N]
        fill_ring(pad, slo.astype(F32).reshape(CUBE))
        sent = ring_shift(pad, -offs[k, 0], -offs[k, 1], -offs[k, 2]).astype(BF16)
        part = part + dot(jnp.concatenate([slo, sent], axis=1), w_back[...])
    local[...] = part.reshape(CUBE)
    send(rim, 2, local[:, :, 0, :], local[:, :, B - 1, :], za, zb)


def edge_grad_kernel(slopes, w_in, out):
    out[...] = dot_t(slopes[...], w_in[2 * W :]).astype(BF16)


def last_kernel(rim, field, z0, z1, y0, y1, x0, x1, out, work):
    work[...] = field[...]
    add_z(rim, (z0, z1), work)
    add_y(rim, (y0, y1), work)
    add_x(rim, (x0, x1), work)
    out[...] = work[...].reshape(N, W).astype(BF16)


def fold(rows, pairs, copies, arrived, out):
    total = arrived[: 2 * rows]
    for i in range(1, pairs):
        total = total + arrived[2 * rows * i : 2 * rows * (i + 1)]
    total = total + jnp.concatenate([total[rows:], total[:rows]], axis=0)
    for i in range(copies):
        out[2 * rows * i : 2 * rows * (i + 1)] = total


def fold_with_faces_kernel(faces, rows, pairs, copies, arrived, *refs):
    fold(rows, pairs, copies, arrived, refs[-2])
    faces(*refs[:-2], refs[-1])


def clip_kernel(rim, mine, other, edge_in, edge_out, node_in, node_out):
    total = jnp.concatenate([own(rim, mine[...], other[...]), own(rim, other[...], mine[...])], axis=0)
    squares = jnp.sum(jnp.sum(total * total, axis=0, keepdims=True), axis=1, keepdims=True)
    factor = math.sqrt(7 * W * W) / jnp.sqrt(squares)
    edge_in[...] = total[: 3 * W] * factor
    edge_out[...] = total[3 * W : 4 * W] * factor
    node_in[...] = total[4 * W : 6 * W] * factor
    node_out[...] = total[6 * W :] * factor


def exchange(a, b, which):
    sizes = [lax.axis_size(axis) for axis in (GX, GY, GZ)]
    aside = {0: 1, 1: 2, 2: 1}[which]
    first, second = [], []
    for me in itertools.product(*map(range, sizes)):
        at = ((me[which] + 1) ^ 1) - 1
        end = at < 0 or at >= sizes[which]
        first.append(moved_to(me, aside, me[aside] ^ 1) if end else moved_to(me, which, at))
        second.append(moved_to(me, which, me[which] ^ 1))
    ranks = {me: rank for rank, me in enumerate(itertools.product(*map(range, sizes)))}
    a, b = (
        lax.ppermute(face, GX + GY + GZ, [(rank, ranks[to]) for rank, to in enumerate(targets)])
        for face, targets in ((a, first), (b, second))
    )
    return a, b


def other_core(half):
    count = math.prod(lax.axis_size(axis) for axis in (GX, GY, GZ))
    step = lax.axis_size(GZ)
    return lax.ppermute(half, GX + GY + GZ, [(rank, rank ^ step) for rank in range(count)])


def moved_to(me, which, at):
    return me[:which] + (at,) + me[which + 1 :]


FACES = [(FACE, F32), (FACE, F32)]
BOTH = pltpu.VMEM((2, *FACE), F32)


def arrivals(rim, field, xa, xb, tag):
    x = exchange(xa, xb, 0)
    a, b = call(y_faces_after_x, FACES, [VMEM] * 4, "after_x" + tag, [BOTH])(rim, field, *x)
    y = exchange(a, b, 1)
    a, b = call(z_faces_after_y, FACES, [VMEM] * 6, "after_y" + tag, [BOTH])(rim, field, *x, *y)
    return (*x, *y, *exchange(a, b, 2))


def swap(rows, axes):
    return lax.all_to_all(rows.reshape(lax.axis_size(axes), -1), axes, 0, 0, tiled=True).reshape(-1, W)


def arrivals_and_sum(rim, field, za, zb, keep, give, edge_grad):
    near, far = lax.axis_size(NEAR), lax.axis_size(FAR)
    rows = keep.shape[0] // near
    (half,) = call(add_kernel, [(keep.shape, F32)], [VMEM] * 3, "add_core")(keep, other_core(give), za)
    got = swap(half, NEAR)
    z = exchange(za, zb, 2)
    a, b, spread = call(
        functools.partial(fold_with_faces_kernel, y_faces_after_z, rows, near // 2, far // 2),
        FACES + [((rows * far, W), F32)],
        [VMEM] * 5,
        "after_z_fold",
        [BOTH],
    )(got, rim, field, *z)
    got = swap(spread, FAR)
    y = exchange(a, b, 1)
    a, b, spread = call(
        functools.partial(fold_with_faces_kernel, x_faces_after_y, rows, far // 2, near // 2),
        FACES + [((rows * near, W), F32)],
        [VMEM] * 7,
        "after_y_fold",
        [BOTH],
    )(got, rim, field, *z, *y)
    mine = swap(spread, NEAR)
    x = exchange(a, b, 0)
    mine, edge_grad, *x = lax.optimization_barrier((mine, edge_grad, *x))
    return (*z, *y, *x), (mine, other_core(mine)), edge_grad


def on_device(node_feat, edge_feat, copies, offsets, w_edge_in, w_edge_out, w_node_in, w_node_out, node_cot):
    cot = node_cot.reshape(N, W)
    inverse = jnp.broadcast_to(1.0 / copies.reshape(N, 1).astype(F32), (N, W))
    square = ((W, W), BF16)
    many = ((K, N, W), BF16)

    local, xa, xb, preact, hidden, nodes, edges, w_in, w_out, rim = call(
        forward_kernel,
        [(CUBE, F32)] + FACES + [((K, N, W), F32), many, ((N, W), BF16), many, ((3 * W, W), BF16), square, ((9, B, W), F32)],
        [HBM] * 5,
        "forward",
        [PAD, pltpu.SMEM((K, 3), jnp.int32), pltpu.SemaphoreType.DMA((4 + K,))],
    )(*map(in_hbm, (node_feat.reshape(N, W), edge_feat.reshape(K, N, W), w_edge_in, w_edge_out, offsets)))
    begun, upstream, w_node_back = call(
        prepare_node_kernel, [((N, W), F32), ((N, W), F32), square], [VMEM] * 4, "prepare_node"
    )(nodes, cot, w_node_in, w_node_out)
    arrived = arrivals(rim, local, xa, xb, "_1")
    dact, hidden_t, left, w_out_t, w_back = call(
        prepare_edge_kernel,
        [((K, N, W), F32), ((K * W, N), BF16), ((3 * W, K * N), BF16), square, ((2 * W, W), BF16)],
        [SMEM] + [VMEM] * 6,
        "prepare_edge",
        [PAD],
    )(offsets, preact, hidden, nodes, edges, w_in, w_out)
    local, xa, xb, gathered, slope, node_hidden = call(
        node_kernel, [(CUBE, F32)] + FACES + [((N, W), BF16)] * 3, [VMEM] * 13, "node", [WORK]
    )(rim, local, *arrived, inverse, begun, upstream, w_node_in, w_node_back)
    arrived = arrivals(rim, local, xa, xb, "_2")
    node_grads, base = call(node_grads_kernel, [((3 * W, W), F32), ((N, W), F32)], [VMEM] * 6, "node_grads")(
        nodes, gathered, slope, node_hidden, cot, w_node_in
    )
    half = ((7 * W // 2, W), F32)
    slopes, keep, give = call(
        edge_kernel,
        [((K * N, W), BF16), half, half],
        [VMEM] * 13,
        "edge",
        [WORK, pltpu.VMEM((7 * W, W), F32)],
    )(rim, local, *arrived, dact, hidden_t, left, w_out_t, node_grads)
    local, za, zb = call(
        node_part_kernel, [(CUBE, F32)] + FACES, [SMEM] + [VMEM] * 4, "node_part", [PAD]
    )(offsets, rim, slopes, base, w_back)
    (edge_grad,) = call(edge_grad_kernel, [((K * N, W), BF16)], [VMEM] * 2, "edge_grad")(slopes, w_in)
    arrived, halves, edge_grad = arrivals_and_sum(rim, local, za, zb, keep, give, edge_grad)
    clipped = call(
        clip_kernel, [((3 * W, W), F32), ((W, W), F32), ((2 * W, W), F32), ((W, W), F32)], [VMEM] * 3, "clip"
    )(rim, *halves)
    (node_grad,) = call(last_kernel, [((N, W), BF16)], [VMEM] * 8, "last", [WORK])(rim, local, *arrived)
    return (node_grad.reshape(node_feat.shape), edge_grad.reshape(edge_feat.shape), *clipped)


def solution(mesh):
    split = Mesh(mesh.devices.reshape(8, 2, 2, 2, 4), ("z", "yh", "yl", "c", "x"))
    place = (GX, GY, GZ)
    placed = (
        P(*place, None),
        P(None, *place, None),
        P(*place),
        P(),
        P(),
        P(),
        P(),
        P(),
        P(*place, None),
    )
    return jax.shard_map(
        on_device,
        mesh=split,
        in_specs=placed,
        out_specs=(P(*place, None), P(None, *place, None), P(), P(), P(), P()),
        check_vma=False,
    )
```

```python
import functools
import itertools
import math

import jax
import jax.numpy as jnp
from jax import lax
from jax.experimental import pallas as pl
from jax.experimental.pallas import tpu as pltpu
from jax.sharding import Mesh
from jax.sharding import PartitionSpec as P

B = 8
W = 128
K = 4
N = B * B * B
CUBE = (B, B, B, W)
FACE = (B, B, W)
F32 = jnp.float32
BF16 = jnp.bfloat16
GRANT = 12 * 1024 * 1024

VMEM = pl.BlockSpec(memory_space=pltpu.VMEM)
SMEM = pl.BlockSpec(memory_space=pltpu.SMEM)
HBM = pl.BlockSpec(memory_space=pltpu.HBM)
PAD = pltpu.VMEM((B + 2, B + 2, B, W), F32)
WORK = pltpu.VMEM(CUBE, F32)

GX, GY, GZ = ("z", "yh"), ("yl", "c"), ("x",)
NEAR, FAR = ("yh", "yl", "x"), ("z",)


def call(body, outs, specs, name, scratch=()):
    return pl.pallas_call(
        body,
        out_shape=[jax.ShapeDtypeStruct(s, t) for s, t in outs],
        in_specs=specs,
        out_specs=[VMEM] * len(outs),
        scratch_shapes=list(scratch),
        compiler_params=pltpu.CompilerParams(vmem_limit_bytes=GRANT),
        name=name,
    )


def in_hbm(array):
    return pltpu.with_memory_space_constraint(array, pltpu.HBM)


def dot(a, b):
    return jnp.dot(a, b, preferred_element_type=F32)


def sigmoid(v):
    return 0.5 + 0.5 * jnp.tanh(0.5 * v)


def dot_t(a, b):
    return lax.dot_general(a, b, (((1,), (1,)), ((), ())), preferred_element_type=F32)


def fill_ring(pad, value):
    pad[1:9, 1:9] = value
    pad[0, 1:9] = value[7]
    pad[9, 1:9] = value[0]
    pad[:, 0] = pad[:, 8]
    pad[:, 9] = pad[:, 1]


def ring_shift(pad, o0, o1, o2):
    moved = pad[pl.ds(1 + o0, B), pl.ds(1 + o1, B)].reshape(B * B, B, W)
    moved = pltpu.roll(moved, lax.rem(B - o2, B), 1)
    return moved.reshape(N, W)


def inside(offs, k):
    ok = None
    for which in range(3):
        at = lax.broadcasted_iota(jnp.int32, CUBE, which) + offs[k, which]
        one = (at >= 0) & (at < B)
        ok = one if ok is None else ok & one
    return ok


def fill_masks(rim):
    for d, axis in enumerate((GX, GY, GZ)):
        at, count = jnp.int32(0), 1
        for name in axis:
            size = lax.axis_size(name)
            at, count = at * size + lax.axis_index(name), count * size
        odd = at & 1
        flags = (1 - odd, jnp.where(at > 0, 1 - odd, 0), jnp.where(at < count - 1, odd, 0))
        for i, flag in enumerate(flags):
            rim[3 * d + i] = jnp.full((B, W), flag.astype(F32))


def forward_kernel(
    nodes_h, edges_h, w_in_h, w_out_h, offs_h,
    local, xa, xb, preact, hidden, nodes, edges, w_in, w_out, rim,
    pad, offs, sems,
):
    pairs = [(nodes_h, nodes), (w_in_h, w_in), (offs_h, offs), (w_out_h, w_out)]
    pairs += [(edges_h.at[k], edges.at[k]) for k in range(K)]
    copies = [pltpu.make_async_copy(a, b, sems.at[i]) for i, (a, b) in enumerate(pairs)]
    for copy in copies:
        copy.start()
    fill_masks(rim)
    for copy in copies[:3]:
        copy.wait()
    node = nodes[...]
    fill_ring(pad, dot(node, w_in[:W]).reshape(CUBE))
    receiver = dot(node, w_in[W : 2 * W])
    copies[3].wait()
    total = jnp.zeros((N, W), F32)
    for k in range(K):
        copies[4 + k].wait()
        pre = ring_shift(pad, offs[k, 0], offs[k, 1], offs[k, 2]) + receiver + dot(edges[k], w_in[2 * W :])
        preact[k] = pre
        act = (pre * sigmoid(pre)).reshape(CUBE)
        kept = jnp.where(inside(offs, k), act, 0.0).reshape(N, W).astype(BF16)
        hidden[k] = kept
        total = total + dot(kept, w_out[...])
    total = total.reshape(CUBE)
    local[...] = total
    send(rim, 0, total[0], total[B - 1], xa, xb)


def prepare_node_kernel(nodes, cot, w_in, w_out, pre, upstream, w_back):
    pre[...] = dot(nodes[...], w_in[:W])
    upstream[...] = dot_t(cot[...], w_out[...])
    w_back[...] = w_in[W:].T


def prepare_edge_kernel(offs, preact, hidden, nodes, edges, w_in, w_out, dact, hidden_t, left, w_out_t, w_back, pad):
    node = nodes[...]
    node_t = node.T
    fill_ring(pad, node.astype(F32).reshape(CUBE))
    for k in range(K):
        pre = preact[k]
        sigma = sigmoid(pre)
        rate = (sigma * (1.0 + pre * (1.0 - sigma))).reshape(CUBE)
        dact[k] = jnp.where(inside(offs, k), rate, 0.0).reshape(N, W)
        hidden_t[k * W : (k + 1) * W] = hidden[k].T
        here = pl.ds(k * N, N)
        left[:W, here] = ring_shift(pad, offs[k, 0], offs[k, 1], offs[k, 2]).astype(BF16).T
        left[W : 2 * W, here] = node_t
        left[2 * W :, here] = edges[k].T
    w_out_t[...] = w_out[...].T
    w_back[:W] = w_in[W : 2 * W].T
    w_back[W:] = w_in[:W].T


def low(rim, d, a, b):
    return jnp.where(rim[3 * d] > 0, jnp.where(rim[3 * d + 1] > 0, a, 0.0), b)


def high(rim, d, a, b):
    return jnp.where(rim[3 * d] > 0, b, jnp.where(rim[3 * d + 2] > 0, a, 0.0))


def send(rim, d, lo, hi, a, b):
    even = rim[3 * d] > 0
    a[...] = jnp.where(even, lo, hi)
    b[...] = jnp.where(even, hi, lo)


def own(rim, top, bottom):
    first = jnp.broadcast_to(rim[3, :1, :], top.shape) > 0
    return jnp.where(first, top, bottom)


def add_kernel(keep, got, after, out):
    out[...] = keep[...] + got[...]


def add_x(rim, x, out):
    out[0] = out[0] + low(rim, 0, x[0][...], x[1][...])
    out[B - 1] = out[B - 1] + high(rim, 0, x[0][...], x[1][...])


def add_y(rim, y, out):
    out[:, 0] = out[:, 0] + low(rim, 1, y[0][...], y[1][...])
    out[:, B - 1] = out[:, B - 1] + high(rim, 1, y[0][...], y[1][...])


def add_z(rim, z, out):
    out[:, :, 0, :] = out[:, :, 0, :] + low(rim, 2, z[0][...], z[1][...])
    out[:, :, B - 1, :] = out[:, :, B - 1, :] + high(rim, 2, z[0][...], z[1][...])


def y_faces_after_x(rim, field, x0, x1, a, b, faces):
    for i, at in enumerate((0, B - 1)):
        faces[i] = field[:, at]
        faces[i, 0] = faces[i, 0] + low(rim, 0, x0[at], x1[at])
        faces[i, B - 1] = faces[i, B - 1] + high(rim, 0, x0[at], x1[at])
    send(rim, 1, faces[0], faces[1], a, b)


def z_faces_after_y(rim, field, x0, x1, y0, y1, a, b, faces):
    for i, at in enumerate((0, B - 1)):
        faces[i] = field[:, :, at, :]
        faces[i, 0] = faces[i, 0] + low(rim, 0, x0[:, at, :], x1[:, at, :])
        faces[i, B - 1] = faces[i, B - 1] + high(rim, 0, x0[:, at, :], x1[:, at, :])
        faces[i, :, 0, :] = faces[i, :, 0, :] + low(rim, 1, y0[:, at, :], y1[:, at, :])
        faces[i, :, B - 1, :] = faces[i, :, B - 1, :] + high(rim, 1, y0[:, at, :], y1[:, at, :])
    send(rim, 2, faces[0], faces[1], a, b)


def whole(rim, field, x0, x1, y0, y1, z0, z1, work):
    work[...] = field[...]
    add_x(rim, (x0, x1), work)
    add_y(rim, (y0, y1), work)
    add_z(rim, (z0, z1), work)
    return work[...].reshape(N, W)


def node_kernel(
    rim, field, x0, x1, y0, y1, z0, z1, inverse, begun, upstream, w_in, w_back,
    local, xa, xb, gathered, slope, hidden, work,
):
    inv = inverse[...]
    agg = (whole(rim, field, x0, x1, y0, y1, z0, z1, work) * inv).astype(BF16)
    gathered[...] = agg
    pre = begun[...] + dot(agg, w_in[W:])
    sigma = sigmoid(pre)
    hidden[...] = (pre * sigma).astype(BF16)
    slo = (upstream[...] * (sigma * (1.0 + pre * (1.0 - sigma)))).astype(BF16)
    slope[...] = slo
    part = (dot(slo, w_back[...]) * inv).reshape(CUBE)
    local[...] = part
    send(rim, 0, part[0], part[B - 1], xa, xb)


def node_grads_kernel(nodes, gathered, slope, hidden, cot, w_in, grads, base):
    slo = slope[...]
    grads[:W] = dot(nodes[...].T, slo)
    grads[W : 2 * W] = dot(gathered[...].T, slo)
    grads[2 * W :] = dot(hidden[...].T, cot[...])
    base[...] = cot[...].astype(F32) + dot_t(slo, w_in[:W])


def edge_kernel(
    rim, field, x0, x1, y0, y1, z0, z1, dact, hidden_t, left, w_out_t, node_grads, slopes, keep, give, work, grads
):
    agg = whole(rim, field, x0, x1, y0, y1, z0, z1, work).astype(BF16)
    back = dot(agg, w_out_t[...])
    for k in range(K):
        slopes[k * N : (k + 1) * N] = (back * dact[k]).astype(BF16)
    outer = dot(hidden_t[...], agg)
    grads[3 * W : 4 * W] = (outer[:W] + outer[W : 2 * W]) + (outer[2 * W : 3 * W] + outer[3 * W :])
    grads[4 * W :] = node_grads[...]
    grads[: 3 * W] = dot(left[...], slopes[...])
    half = keep.shape[0]
    keep[...] = own(rim, grads[:half], grads[half:])
    give[...] = own(rim, grads[half:], grads[:half])


def node_part_kernel(offs, rim, slopes, base, w_back, local, xa, xb, pad):
    part = base[...]
    for k in range(K):
        slo = slopes[k * N : (k + 1) * N]
        fill_ring(pad, slo.astype(F32).reshape(CUBE))
        sent = ring_shift(pad, -offs[k, 0], -offs[k, 1], -offs[k, 2]).astype(BF16)
        part = part + dot(jnp.concatenate([slo, sent], axis=1), w_back[...])
    local[...] = part.reshape(CUBE)
    send(rim, 0, local[0], local[B - 1], xa, xb)


def edge_grad_kernel(slopes, w_in, out):
    out[...] = dot_t(slopes[...], w_in[2 * W :]).astype(BF16)


def last_kernel(rim, field, x0, x1, y0, y1, z0, z1, out, work):
    out[...] = whole(rim, field, x0, x1, y0, y1, z0, z1, work).astype(BF16)


def fold(rows, pairs, copies, arrived, out):
    total = arrived[: 2 * rows]
    for i in range(1, pairs):
        total = total + arrived[2 * rows * i : 2 * rows * (i + 1)]
    total = total + jnp.concatenate([total[rows:], total[:rows]], axis=0)
    for i in range(copies):
        out[2 * rows * i : 2 * rows * (i + 1)] = total


def fold_with_faces_kernel(faces, rows, pairs, copies, arrived, *refs):
    fold(rows, pairs, copies, arrived, refs[-2])
    faces(*refs[:-2], refs[-1])


def clip_kernel(rim, mine, other, edge_in, edge_out, node_in, node_out):
    total = jnp.concatenate([own(rim, mine[...], other[...]), own(rim, other[...], mine[...])], axis=0)
    squares = jnp.sum(jnp.sum(total * total, axis=0, keepdims=True), axis=1, keepdims=True)
    factor = math.sqrt(7 * W * W) / jnp.sqrt(squares)
    edge_in[...] = total[: 3 * W] * factor
    edge_out[...] = total[3 * W : 4 * W] * factor
    node_in[...] = total[4 * W : 6 * W] * factor
    node_out[...] = total[6 * W :] * factor


def exchange(a, b, which):
    sizes = [lax.axis_size(axis) for axis in (GX, GY, GZ)]
    aside = {0: 1, 1: 2, 2: 1}[which]
    first, second = [], []
    for me in itertools.product(*map(range, sizes)):
        at = ((me[which] + 1) ^ 1) - 1
        end = at < 0 or at >= sizes[which]
        first.append(moved_to(me, aside, me[aside] ^ 1) if end else moved_to(me, which, at))
        second.append(moved_to(me, which, me[which] ^ 1))
    ranks = {me: rank for rank, me in enumerate(itertools.product(*map(range, sizes)))}
    a, b = (
        lax.ppermute(face, GX + GY + GZ, [(rank, ranks[to]) for rank, to in enumerate(targets)])
        for face, targets in ((a, first), (b, second))
    )
    return a, b


def other_core(half):
    count = math.prod(lax.axis_size(axis) for axis in (GX, GY, GZ))
    step = lax.axis_size(GZ)
    return lax.ppermute(half, GX + GY + GZ, [(rank, rank ^ step) for rank in range(count)])


def moved_to(me, which, at):
    return me[:which] + (at,) + me[which + 1 :]


FACES = [(FACE, F32), (FACE, F32)]
BOTH = pltpu.VMEM((2, *FACE), F32)


def arrivals(rim, field, xa, xb, tag):
    x = exchange(xa, xb, 0)
    a, b = call(y_faces_after_x, FACES, [VMEM] * 4, "after_x" + tag, [BOTH])(rim, field, *x)
    y = exchange(a, b, 1)
    a, b = call(z_faces_after_y, FACES, [VMEM] * 6, "after_y" + tag, [BOTH])(rim, field, *x, *y)
    return (*x, *y, *exchange(a, b, 2))


def swap(rows, axes):
    return lax.all_to_all(rows.reshape(lax.axis_size(axes), -1), axes, 0, 0, tiled=True).reshape(-1, W)


def arrivals_and_sum(rim, field, xa, xb, keep, give, edge_grad):
    near, far = lax.axis_size(NEAR), lax.axis_size(FAR)
    rows = keep.shape[0] // near
    (half,) = call(add_kernel, [(keep.shape, F32)], [VMEM] * 3, "add_core")(keep, other_core(give), xa)
    got = swap(half, NEAR)
    x = exchange(xa, xb, 0)
    a, b, spread = call(
        functools.partial(fold_with_faces_kernel, y_faces_after_x, rows, near // 2, far // 2),
        FACES + [((rows * far, W), F32)],
        [VMEM] * 5,
        "after_x_fold",
        [BOTH],
    )(got, rim, field, *x)
    got = swap(spread, FAR)
    y = exchange(a, b, 1)
    a, b, spread = call(
        functools.partial(fold_with_faces_kernel, z_faces_after_y, rows, far // 2, near // 2),
        FACES + [((rows * near, W), F32)],
        [VMEM] * 7,
        "after_y_fold",
        [BOTH],
    )(got, rim, field, *x, *y)
    mine = swap(spread, NEAR)
    z = exchange(a, b, 2)
    mine, edge_grad, *z = lax.optimization_barrier((mine, edge_grad, *z))
    return (*x, *y, *z), (mine, other_core(mine)), edge_grad


def on_device(node_feat, edge_feat, copies, offsets, w_edge_in, w_edge_out, w_node_in, w_node_out, node_cot):
    cot = node_cot.reshape(N, W)
    inverse = jnp.broadcast_to(1.0 / copies.reshape(N, 1).astype(F32), (N, W))
    square = ((W, W), BF16)
    many = ((K, N, W), BF16)

    local, xa, xb, preact, hidden, nodes, edges, w_in, w_out, rim = call(
        forward_kernel,
        [(CUBE, F32)] + FACES + [((K, N, W), F32), many, ((N, W), BF16), many, ((3 * W, W), BF16), square, ((9, B, W), F32)],
        [HBM] * 5,
        "forward",
        [PAD, pltpu.SMEM((K, 3), jnp.int32), pltpu.SemaphoreType.DMA((4 + K,))],
    )(*map(in_hbm, (node_feat.reshape(N, W), edge_feat.reshape(K, N, W), w_edge_in, w_edge_out, offsets)))
    begun, upstream, w_node_back = call(
        prepare_node_kernel, [((N, W), F32), ((N, W), F32), square], [VMEM] * 4, "prepare_node"
    )(nodes, cot, w_node_in, w_node_out)
    arrived = arrivals(rim, local, xa, xb, "_1")
    dact, hidden_t, left, w_out_t, w_back = call(
        prepare_edge_kernel,
        [((K, N, W), F32), ((K * W, N), BF16), ((3 * W, K * N), BF16), square, ((2 * W, W), BF16)],
        [SMEM] + [VMEM] * 6,
        "prepare_edge",
        [PAD],
    )(offsets, preact, hidden, nodes, edges, w_in, w_out)
    local, xa, xb, gathered, slope, node_hidden = call(
        node_kernel, [(CUBE, F32)] + FACES + [((N, W), BF16)] * 3, [VMEM] * 13, "node", [WORK]
    )(rim, local, *arrived, inverse, begun, upstream, w_node_in, w_node_back)
    arrived = arrivals(rim, local, xa, xb, "_2")
    node_grads, base = call(node_grads_kernel, [((3 * W, W), F32), ((N, W), F32)], [VMEM] * 6, "node_grads")(
        nodes, gathered, slope, node_hidden, cot, w_node_in
    )
    half = ((7 * W // 2, W), F32)
    slopes, keep, give = call(
        edge_kernel,
        [((K * N, W), BF16), half, half],
        [VMEM] * 13,
        "edge",
        [WORK, pltpu.VMEM((7 * W, W), F32)],
    )(rim, local, *arrived, dact, hidden_t, left, w_out_t, node_grads)
    local, xa, xb = call(
        node_part_kernel, [(CUBE, F32)] + FACES, [SMEM] + [VMEM] * 4, "node_part", [PAD]
    )(offsets, rim, slopes, base, w_back)
    (edge_grad,) = call(edge_grad_kernel, [((K * N, W), BF16)], [VMEM] * 2, "edge_grad")(slopes, w_in)
    arrived, halves, edge_grad = arrivals_and_sum(rim, local, xa, xb, keep, give, edge_grad)
    clipped = call(
        clip_kernel, [((3 * W, W), F32), ((W, W), F32), ((2 * W, W), F32), ((W, W), F32)], [VMEM] * 3, "clip"
    )(rim, *halves)
    (node_grad,) = call(last_kernel, [((N, W), BF16)], [VMEM] * 8, "last", [WORK])(rim, local, *arrived)
    return (node_grad.reshape(node_feat.shape), edge_grad.reshape(edge_feat.shape), *clipped)


def solution(mesh):
    split = Mesh(mesh.devices.reshape(8, 2, 2, 2, 4), ("z", "yh", "yl", "c", "x"))
    place = (GX, GY, GZ)
    placed = (
        P(*place, None),
        P(None, *place, None),
        P(*place),
        P(),
        P(),
        P(),
        P(),
        P(),
        P(*place, None),
    )
    return jax.shard_map(
        on_device,
        mesh=split,
        in_specs=placed,
        out_specs=(P(*place, None), P(None, *place, None), P(), P(), P(), P()),
        check_vma=False,
    )
```

```python
import functools
import itertools
import math

import jax
import jax.numpy as jnp
from jax import lax
from jax.experimental import pallas as pl
from jax.experimental.pallas import tpu as pltpu
from jax.sharding import Mesh
from jax.sharding import PartitionSpec as P


B = 8
W = 128
K = 4
N = B * B * B
CUBE = (B, B, B, W)
FACE = (B, B, W)
F32 = jnp.float32
BF16 = jnp.bfloat16
GRANT = 12 * 1024 * 1024

VMEM = pl.BlockSpec(memory_space=pltpu.VMEM)
SMEM = pl.BlockSpec(memory_space=pltpu.SMEM)
HBM = pl.BlockSpec(memory_space=pltpu.HBM)
PAD = pltpu.VMEM((B + 2, B + 2, B, W), F32)
WORK = pltpu.VMEM(CUBE, F32)

GX, GY, GZ = ("z", "yh"), ("yl", "c"), ("x",)
NEAR, FAR = ("yh", "yl", "x"), ("z",)


def call(body, outs, specs, scratch=()):
    return pl.pallas_call(
        body,
        out_shape=[jax.ShapeDtypeStruct(s, t) for s, t in outs],
        in_specs=specs,
        out_specs=[VMEM] * len(outs),
        scratch_shapes=list(scratch),
        compiler_params=pltpu.CompilerParams(vmem_limit_bytes=GRANT),
    )


def in_hbm(array):
    return pltpu.with_memory_space_constraint(array, pltpu.HBM)


def dot(a, b):
    return jnp.dot(a, b, preferred_element_type=F32)


def dot_t(a, b):
    return lax.dot_general(a, b, (((1,), (1,)), ((), ())), preferred_element_type=F32)


def fill_ring(pad, value):
    pad[1:9, 1:9] = value
    pad[0, 1:9] = value[7]
    pad[9, 1:9] = value[0]
    pad[:, 0] = pad[:, 8]
    pad[:, 9] = pad[:, 1]


def ring_shift(pad, o0, o1, o2):
    moved = pad[pl.ds(1 + o0, B), pl.ds(1 + o1, B)].reshape(B * B, B, W)
    moved = pltpu.roll(moved, lax.rem(B - o2, B), 1)
    return moved.reshape(N, W)


def inside(offs, k):
    ok = None
    for which in range(3):
        at = lax.broadcasted_iota(jnp.int32, CUBE, which) + offs[k, which]
        one = (at >= 0) & (at < B)
        ok = one if ok is None else ok & one
    return ok


def fill_masks(rim):
    for d, axis in enumerate((GX, GY, GZ)):
        at, count = jnp.int32(0), 1
        for name in axis:
            size = lax.axis_size(name)
            at, count = at * size + lax.axis_index(name), count * size
        odd = at & 1
        flags = (1 - odd, jnp.where(at > 0, 1 - odd, 0), jnp.where(at < count - 1, odd, 0))
        for i, flag in enumerate(flags):
            rim[3 * d + i] = jnp.full((B, W), flag.astype(F32))


def forward_kernel(
    nodes_h, edges_h, w_in_h, w_out_h, offs_h,
    local, xa, xb, preact, hidden, nodes, edges, w_in, w_out, rim,
    pad, offs, sems,
):
    pairs = [(nodes_h, nodes), (w_in_h, w_in), (offs_h, offs), (w_out_h, w_out)]
    pairs += [(edges_h.at[k], edges.at[k]) for k in range(K)]
    copies = [pltpu.make_async_copy(a, b, sems.at[i]) for i, (a, b) in enumerate(pairs)]
    for copy in copies:
        copy.start()
    fill_masks(rim)
    for copy in copies[:3]:
        copy.wait()
    node = nodes[...]
    fill_ring(pad, dot(node, w_in[:W]).reshape(CUBE))
    receiver = dot(node, w_in[W : 2 * W])
    copies[3].wait()
    total = jnp.zeros((N, W), F32)
    for k in range(K):
        copies[4 + k].wait()
        pre = ring_shift(pad, offs[k, 0], offs[k, 1], offs[k, 2]) + receiver + dot(edges[k], w_in[2 * W :])
        preact[k] = pre
        act = (pre * jax.nn.sigmoid(pre)).reshape(CUBE)
        kept = jnp.where(inside(offs, k), act, 0.0).reshape(N, W).astype(BF16)
        hidden[k] = kept
        total = total + dot(kept, w_out[...])
    total = total.reshape(CUBE)
    local[...] = total
    send(rim, 0, total[0], total[B - 1], xa, xb)


def prepare_node_kernel(nodes, cot, w_in, w_out, pre, upstream, w_back):
    pre[...] = dot(nodes[...], w_in[:W])
    upstream[...] = dot_t(cot[...], w_out[...])
    w_back[...] = w_in[W:].T


def prepare_edge_kernel(offs, preact, hidden, nodes, edges, w_in, w_out, dact, hidden_t, left, w_out_t, w_back, pad):
    node = nodes[...]
    node_t = node.T
    fill_ring(pad, node.astype(F32).reshape(CUBE))
    for k in range(K):
        pre = preact[k]
        sigma = jax.nn.sigmoid(pre)
        rate = (sigma * (1.0 + pre * (1.0 - sigma))).reshape(CUBE)
        dact[k] = jnp.where(inside(offs, k), rate, 0.0).reshape(N, W)
        hidden_t[k * W : (k + 1) * W] = hidden[k].T
        here = pl.ds(k * N, N)
        left[:W, here] = ring_shift(pad, offs[k, 0], offs[k, 1], offs[k, 2]).astype(BF16).T
        left[W : 2 * W, here] = node_t
        left[2 * W :, here] = edges[k].T
    w_out_t[...] = w_out[...].T
    w_back[:W] = w_in[W : 2 * W].T
    w_back[W:] = w_in[:W].T


def low(rim, d, a, b):
    return jnp.where(rim[3 * d] > 0, jnp.where(rim[3 * d + 1] > 0, a, 0.0), b)


def high(rim, d, a, b):
    return jnp.where(rim[3 * d] > 0, b, jnp.where(rim[3 * d + 2] > 0, a, 0.0))


def send(rim, d, lo, hi, a, b):
    even = rim[3 * d] > 0
    a[...] = jnp.where(even, lo, hi)
    b[...] = jnp.where(even, hi, lo)


def own(rim, top, bottom):
    first = jnp.broadcast_to(rim[3, :1, :], top.shape) > 0
    return jnp.where(first, top, bottom)


def add_kernel(keep, got, after, out):
    out[...] = keep[...] + got[...]


def add_x(rim, x, out):
    out[0] = out[0] + low(rim, 0, x[0][...], x[1][...])
    out[B - 1] = out[B - 1] + high(rim, 0, x[0][...], x[1][...])


def add_y(rim, y, out):
    out[:, 0] = out[:, 0] + low(rim, 1, y[0][...], y[1][...])
    out[:, B - 1] = out[:, B - 1] + high(rim, 1, y[0][...], y[1][...])


def add_z(rim, z, out):
    out[:, :, 0, :] = out[:, :, 0, :] + low(rim, 2, z[0][...], z[1][...])
    out[:, :, B - 1, :] = out[:, :, B - 1, :] + high(rim, 2, z[0][...], z[1][...])


def y_faces_after_x(rim, field, x0, x1, a, b, faces):
    for i, at in enumerate((0, B - 1)):
        faces[i] = field[:, at]
        faces[i, 0] = faces[i, 0] + low(rim, 0, x0[at], x1[at])
        faces[i, B - 1] = faces[i, B - 1] + high(rim, 0, x0[at], x1[at])
    send(rim, 1, faces[0], faces[1], a, b)


def z_faces_after_y(rim, field, x0, x1, y0, y1, a, b, faces):
    for i, at in enumerate((0, B - 1)):
        faces[i] = field[:, :, at, :]
        faces[i, 0] = faces[i, 0] + low(rim, 0, x0[:, at, :], x1[:, at, :])
        faces[i, B - 1] = faces[i, B - 1] + high(rim, 0, x0[:, at, :], x1[:, at, :])
        faces[i, :, 0, :] = faces[i, :, 0, :] + low(rim, 1, y0[:, at, :], y1[:, at, :])
        faces[i, :, B - 1, :] = faces[i, :, B - 1, :] + high(rim, 1, y0[:, at, :], y1[:, at, :])
    send(rim, 2, faces[0], faces[1], a, b)


def y_faces_after_z(rim, field, z0, z1, a, b, faces):
    for i, at in enumerate((0, B - 1)):
        faces[i] = field[:, at]
        faces[i, :, 0, :] = faces[i, :, 0, :] + low(rim, 2, z0[:, at, :], z1[:, at, :])
        faces[i, :, B - 1, :] = faces[i, :, B - 1, :] + high(rim, 2, z0[:, at, :], z1[:, at, :])
    send(rim, 1, faces[0], faces[1], a, b)


def x_faces_after_y(rim, field, z0, z1, y0, y1, a, b, faces):
    for i, at in enumerate((0, B - 1)):
        faces[i] = field[at]
        faces[i, :, 0, :] = faces[i, :, 0, :] + low(rim, 2, z0[at], z1[at])
        faces[i, :, B - 1, :] = faces[i, :, B - 1, :] + high(rim, 2, z0[at], z1[at])
        faces[i, 0] = faces[i, 0] + low(rim, 1, y0[at], y1[at])
        faces[i, B - 1] = faces[i, B - 1] + high(rim, 1, y0[at], y1[at])
    send(rim, 0, faces[0], faces[1], a, b)


def whole(rim, field, x0, x1, y0, y1, z0, z1, work):
    work[...] = field[...]
    add_x(rim, (x0, x1), work)
    add_y(rim, (y0, y1), work)
    add_z(rim, (z0, z1), work)
    return work[...].reshape(N, W)


def node_kernel(
    rim, field, x0, x1, y0, y1, z0, z1, inverse, begun, upstream, w_in, w_back,
    local, xa, xb, gathered, slope, hidden, work,
):
    inv = inverse[...]
    agg = (whole(rim, field, x0, x1, y0, y1, z0, z1, work) * inv).astype(BF16)
    gathered[...] = agg
    pre = begun[...] + dot(agg, w_in[W:])
    sigma = jax.nn.sigmoid(pre)
    hidden[...] = (pre * sigma).astype(BF16)
    slo = (upstream[...] * (sigma * (1.0 + pre * (1.0 - sigma)))).astype(BF16)
    slope[...] = slo
    part = (dot(slo, w_back[...]) * inv).reshape(CUBE)
    local[...] = part
    send(rim, 0, part[0], part[B - 1], xa, xb)


def node_grads_kernel(nodes, gathered, slope, hidden, cot, w_in, grads, base):
    slo = slope[...]
    grads[:W] = dot(nodes[...].T, slo)
    grads[W : 2 * W] = dot(gathered[...].T, slo)
    grads[2 * W :] = dot(hidden[...].T, cot[...])
    base[...] = cot[...].astype(F32) + dot_t(slo, w_in[:W])


def edge_kernel(
    rim, field, x0, x1, y0, y1, z0, z1, dact, hidden_t, left, w_out_t, node_grads, slopes, keep, give, work, grads
):
    agg = whole(rim, field, x0, x1, y0, y1, z0, z1, work).astype(BF16)
    back = dot(agg, w_out_t[...])
    for k in range(K):
        slopes[k * N : (k + 1) * N] = (back * dact[k]).astype(BF16)
    outer = dot(hidden_t[...], agg)
    grads[3 * W : 4 * W] = (outer[:W] + outer[W : 2 * W]) + (outer[2 * W : 3 * W] + outer[3 * W :])
    grads[4 * W :] = node_grads[...]
    grads[: 3 * W] = dot(left[...], slopes[...])
    half = keep.shape[0]
    keep[...] = own(rim, grads[:half], grads[half:])
    give[...] = own(rim, grads[half:], grads[:half])


def node_part_kernel(offs, rim, slopes, base, w_back, local, za, zb, pad):
    part = base[...]
    for k in range(K):
        slo = slopes[k * N : (k + 1) * N]
        fill_ring(pad, slo.astype(F32).reshape(CUBE))
        sent = ring_shift(pad, -offs[k, 0], -offs[k, 1], -offs[k, 2]).astype(BF16)
        part = part + dot(jnp.concatenate([slo, sent], axis=1), w_back[...])
    local[...] = part.reshape(CUBE)
    send(rim, 2, local[:, :, 0, :], local[:, :, B - 1, :], za, zb)


def edge_grad_kernel(slopes, w_in, out):
    out[...] = dot_t(slopes[...], w_in[2 * W :]).astype(BF16)


def last_kernel(rim, field, z0, z1, y0, y1, x0, x1, clipped, out, work):
    work[...] = field[...]
    add_z(rim, (z0, z1), work)
    add_y(rim, (y0, y1), work)
    add_x(rim, (x0, x1), work)
    out[...] = work[...].reshape(N, W).astype(BF16)


def fold(rows, pairs, copies, arrived, out):
    total = arrived[: 2 * rows]
    for i in range(1, pairs):
        total = total + arrived[2 * rows * i : 2 * rows * (i + 1)]
    total = total + jnp.concatenate([total[rows:], total[:rows]], axis=0)
    for i in range(copies):
        out[2 * rows * i : 2 * rows * (i + 1)] = total


def fold_with_faces_kernel(faces, rows, pairs, copies, arrived, *refs):
    fold(rows, pairs, copies, arrived, refs[-2])
    faces(*refs[:-2], refs[-1])


def clip_kernel(rim, mine, other, edge_in, edge_out, node_in, node_out):
    total = jnp.concatenate([own(rim, mine[...], other[...]), own(rim, other[...], mine[...])], axis=0)
    squares = jnp.sum(jnp.sum(total * total, axis=0, keepdims=True), axis=1, keepdims=True)
    factor = math.sqrt(7 * W * W) / jnp.sqrt(squares)
    edge_in[...] = total[: 3 * W] * factor
    edge_out[...] = total[3 * W : 4 * W] * factor
    node_in[...] = total[4 * W : 6 * W] * factor
    node_out[...] = total[6 * W :] * factor


def exchange(a, b, which):
    sizes = [lax.axis_size(axis) for axis in (GX, GY, GZ)]
    aside = {0: 1, 1: 2, 2: 1}[which]
    first, second = [], []
    for me in itertools.product(*map(range, sizes)):
        at = ((me[which] + 1) ^ 1) - 1
        end = at < 0 or at >= sizes[which]
        first.append(moved_to(me, aside, me[aside] ^ 1) if end else moved_to(me, which, at))
        second.append(moved_to(me, which, me[which] ^ 1))
    ranks = {me: rank for rank, me in enumerate(itertools.product(*map(range, sizes)))}
    a, b = (
        lax.ppermute(face, GX + GY + GZ, [(rank, ranks[to]) for rank, to in enumerate(targets)])
        for face, targets in ((a, first), (b, second))
    )
    return a, b


def other_core(half):
    count = math.prod(lax.axis_size(axis) for axis in (GX, GY, GZ))
    step = lax.axis_size(GZ)
    return lax.ppermute(half, GX + GY + GZ, [(rank, rank ^ step) for rank in range(count)])


def moved_to(me, which, at):
    return me[:which] + (at,) + me[which + 1 :]


FACES = [(FACE, F32), (FACE, F32)]
BOTH = pltpu.VMEM((2, *FACE), F32)


def arrivals(rim, field, xa, xb):
    x = exchange(xa, xb, 0)
    a, b = call(y_faces_after_x, FACES, [VMEM] * 4, [BOTH])(rim, field, *x)
    y = exchange(a, b, 1)
    a, b = call(z_faces_after_y, FACES, [VMEM] * 6, [BOTH])(rim, field, *x, *y)
    return (*x, *y, *exchange(a, b, 2))


def swap(rows, axes):
    return lax.all_to_all(rows.reshape(lax.axis_size(axes), -1), axes, 0, 0, tiled=True).reshape(-1, W)


def arrivals_and_sum(rim, field, za, zb, keep, give):
    near, far = lax.axis_size(NEAR), lax.axis_size(FAR)
    rows = keep.shape[0] // near
    (half,) = call(add_kernel, [(keep.shape, F32)], [VMEM] * 3)(keep, other_core(give), za)
    got = swap(half, NEAR)
    z = exchange(za, zb, 2)
    a, b, spread = call(
        functools.partial(fold_with_faces_kernel, y_faces_after_z, rows, near // 2, far // 2),
        FACES + [((rows * far, W), F32)],
        [VMEM] * 5,
        [BOTH],
    )(got, rim, field, *z)
    got = swap(spread, FAR)
    y = exchange(a, b, 1)
    a, b, spread = call(
        functools.partial(fold_with_faces_kernel, x_faces_after_y, rows, far // 2, near // 2),
        FACES + [((rows * near, W), F32)],
        [VMEM] * 7,
        [BOTH],
    )(got, rim, field, *z, *y)
    mine = swap(spread, NEAR)
    x = exchange(a, b, 0)
    return (*z, *y, *x), (mine, other_core(mine))


def on_device(node_feat, edge_feat, copies, offsets, w_edge_in, w_edge_out, w_node_in, w_node_out, node_cot):
    cot = node_cot.reshape(N, W)
    inverse = jnp.broadcast_to(1.0 / copies.reshape(N, 1).astype(F32), (N, W))
    square = ((W, W), BF16)
    many = ((K, N, W), BF16)

    local, xa, xb, preact, hidden, nodes, edges, w_in, w_out, rim = call(
        forward_kernel,
        [(CUBE, F32)] + FACES + [((K, N, W), F32), many, ((N, W), BF16), many, ((3 * W, W), BF16), square, ((9, B, W), F32)],
        [HBM] * 5,
        [PAD, pltpu.SMEM((K, 3), jnp.int32), pltpu.SemaphoreType.DMA((4 + K,))],
    )(*map(in_hbm, (node_feat.reshape(N, W), edge_feat.reshape(K, N, W), w_edge_in, w_edge_out, offsets)))
    begun, upstream, w_node_back = call(
        prepare_node_kernel, [((N, W), F32), ((N, W), F32), square], [VMEM] * 4
    )(nodes, cot, w_node_in, w_node_out)
    arrived = arrivals(rim, local, xa, xb)
    dact, hidden_t, left, w_out_t, w_back = call(
        prepare_edge_kernel,
        [((K, N, W), F32), ((K * W, N), BF16), ((3 * W, K * N), BF16), square, ((2 * W, W), BF16)],
        [SMEM] + [VMEM] * 6,
        [PAD],
    )(offsets, preact, hidden, nodes, edges, w_in, w_out)
    local, xa, xb, gathered, slope, node_hidden = call(
        node_kernel, [(CUBE, F32)] + FACES + [((N, W), BF16)] * 3, [VMEM] * 13, [WORK]
    )(rim, local, *arrived, inverse, begun, upstream, w_node_in, w_node_back)
    arrived = arrivals(rim, local, xa, xb)
    node_grads, base = call(node_grads_kernel, [((3 * W, W), F32), ((N, W), F32)], [VMEM] * 6)(
        nodes, gathered, slope, node_hidden, cot, w_node_in
    )
    half = ((7 * W // 2, W), F32)
    slopes, keep, give = call(
        edge_kernel, [((K * N, W), BF16), half, half], [VMEM] * 13, [WORK, pltpu.VMEM((7 * W, W), F32)]
    )(rim, local, *arrived, dact, hidden_t, left, w_out_t, node_grads)
    local, za, zb = call(
        node_part_kernel, [(CUBE, F32)] + FACES, [SMEM] + [VMEM] * 4, [PAD]
    )(offsets, rim, slopes, base, w_back)
    (edge_grad,) = call(edge_grad_kernel, [((K * N, W), BF16)], [VMEM] * 2)(slopes, w_in)
    arrived, halves = arrivals_and_sum(rim, local, za, zb, keep, give)
    clipped = call(
        clip_kernel, [((3 * W, W), F32), ((W, W), F32), ((2 * W, W), F32), ((W, W), F32)], [VMEM] * 3
    )(rim, *halves)
    (node_grad,) = call(last_kernel, [((N, W), BF16)], [VMEM] * 8 + [HBM], [WORK])(
        rim, local, *arrived, in_hbm(clipped[1])
    )
    return (node_grad.reshape(node_feat.shape), edge_grad.reshape(edge_feat.shape), *clipped)


def solution(mesh):
    split = Mesh(mesh.devices.reshape(8, 2, 2, 2, 4), ("z", "yh", "yl", "c", "x"))
    place = (GX, GY, GZ)
    placed = (
        P(*place, None),
        P(None, *place, None),
        P(*place),
        P(),
        P(),
        P(),
        P(),
        P(),
        P(*place, None),
    )

    return jax.shard_map(
        on_device,
        mesh=split,
        in_specs=placed,
        out_specs=(P(*place, None), P(None, *place, None), P(), P(), P(), P()),
        check_vma=False,
    )
```

```python
import functools
import itertools
import math

import jax
import jax.numpy as jnp
from jax import lax
from jax.experimental import pallas as pl
from jax.experimental.pallas import tpu as pltpu
from jax.sharding import Mesh
from jax.sharding import PartitionSpec as P

B = 8
W = 128
K = 4
N = B * B * B
CUBE = (B, B, B, W)
FACE = (B, B, W)
F32 = jnp.float32
BF16 = jnp.bfloat16
GRANT = 12 * 1024 * 1024

VMEM = pl.BlockSpec(memory_space=pltpu.VMEM)
SMEM = pl.BlockSpec(memory_space=pltpu.SMEM)
HBM = pl.BlockSpec(memory_space=pltpu.HBM)
PAD = pltpu.VMEM((B + 2, B + 2, B, W), F32)
WORK = pltpu.VMEM(CUBE, F32)

GX, GY, GZ = ("z", "yh"), ("yl", "c"), ("x",)
NEAR, FAR, BACK = ("yh", "yl", "x"), ("z",), ("yh", "yl", "c", "x")
GROUPS = 4


def call(body, outs, specs, name, scratch=()):
    return pl.pallas_call(
        body,
        out_shape=[jax.ShapeDtypeStruct(s, t) for s, t in outs],
        in_specs=specs,
        out_specs=[VMEM] * len(outs),
        scratch_shapes=list(scratch),
        compiler_params=pltpu.CompilerParams(vmem_limit_bytes=GRANT),
        name=name,
    )


def in_hbm(array):
    return pltpu.with_memory_space_constraint(array, pltpu.HBM)


def dot(a, b):
    return jnp.dot(a, b, preferred_element_type=F32)


def dot_t(a, b):
    return lax.dot_general(a, b, (((1,), (1,)), ((), ())), preferred_element_type=F32)


def fill_ring(pad, value):
    pad[1:9, 1:9] = value
    pad[0, 1:9] = value[7]
    pad[9, 1:9] = value[0]
    pad[:, 0] = pad[:, 8]
    pad[:, 9] = pad[:, 1]


def ring_shift(pad, o0, o1, o2):
    moved = pad[pl.ds(1 + o0, B), pl.ds(1 + o1, B)].reshape(B * B, B, W)
    moved = pltpu.roll(moved, lax.rem(B - o2, B), 1)
    return moved.reshape(N, W)


def inside(offs, k, rims=False):
    ok = None
    shape = (2, *FACE) if rims else CUBE
    for which in range(3):
        at = lax.broadcasted_iota(jnp.int32, shape, which)
        at = (at * (B - 1) if rims and which == 0 else at) + offs[k, which]
        one = (at >= 0) & (at < B)
        ok = one if ok is None else ok & one
    return ok


def fill_masks(rim):
    for d, axis in enumerate((GX, GY, GZ)):
        at, count = jnp.int32(0), 1
        for name in axis:
            size = lax.axis_size(name)
            at, count = at * size + lax.axis_index(name), count * size
        odd = at & 1
        flags = (1 - odd, jnp.where(at > 0, 1 - odd, 0), jnp.where(at < count - 1, odd, 0))
        for i, flag in enumerate(flags):
            rim[3 * d + i] = jnp.full((B, W), flag.astype(F32))


RIMS = (0, (B - 1) * B * B)


def first_rims_kernel(
    nodes_h, edges_h, w_in_h, w_out_h, offs_h, xa, xb, rim, nodes, edges, w_in, w_out, pad, offs, sems
):
    plane = B * B
    pairs = [(nodes_h, nodes), (w_in_h, w_in), (offs_h, offs), (w_out_h, w_out)]
    pairs += [(edges_h.at[k], edges.at[k]) for k in range(K)]
    copies = [pltpu.make_async_copy(a, b, sems.at[i]) for i, (a, b) in enumerate(pairs)]
    for copy in copies:
        copy.start()
    fill_masks(rim)
    for copy in copies[:3]:
        copy.wait()
    node = nodes[...]
    fill_ring(pad, dot(node, w_in[:W]).reshape(CUBE))
    rims = jnp.concatenate([node[at : at + plane] for at in RIMS], axis=0)
    receiver = dot(rims, w_in[W : 2 * W])
    copies[3].wait()
    total = jnp.zeros((2 * plane, W), F32)
    for k in range(K):
        copies[4 + k].wait()
        o0, o1, o2 = offs[k, 0], offs[k, 1], offs[k, 2]
        sent = jnp.concatenate([pad[pl.ds(1 + at + o0, 1), pl.ds(1 + o1, B)] for at in (0, B - 1)], axis=0)
        sent = pltpu.roll(sent.reshape(2 * B, B, W), lax.rem(B - o2, B), 1).reshape(2 * plane, W)
        edge = jnp.concatenate([edges[k, at : at + plane] for at in RIMS], axis=0)
        pre = sent + receiver + dot(edge, w_in[2 * W :])
        act = (pre * jax.nn.sigmoid(pre)).reshape(2, B, B, W)
        kept = jnp.where(inside(offs, k, True), act, 0.0).reshape(2 * plane, W).astype(BF16)
        total = total + dot(kept, w_out[...])
    total = total.reshape(2, B, B, W)
    send(rim, 0, total[0], total[1], xa, xb)


def forward_kernel(offs, nodes, edges, w_in, w_out, after, local, preact, hidden, pad):
    node = nodes[...]
    fill_ring(pad, dot(node, w_in[:W]).reshape(CUBE))
    receiver = dot(node, w_in[W : 2 * W])
    total = jnp.zeros((N, W), F32)
    for k in range(K):
        pre = ring_shift(pad, offs[k, 0], offs[k, 1], offs[k, 2]) + receiver + dot(edges[k], w_in[2 * W :])
        preact[k] = pre
        act = (pre * jax.nn.sigmoid(pre)).reshape(CUBE)
        kept = jnp.where(inside(offs, k), act, 0.0).reshape(N, W).astype(BF16)
        hidden[k] = kept
        total = total + dot(kept, w_out[...])
    local[...] = total.reshape(CUBE)


def prepare_node_kernel(nodes, cot, w_in, w_out, after, pre, upstream, w_back):
    pre[...] = dot(nodes[...], w_in[:W])
    upstream[...] = dot_t(cot[...], w_out[...])
    w_back[...] = w_in[W:].T


def prepare_edge_kernel(offs, preact, hidden, nodes, edges, w_in, w_out, dact, hidden_t, left, w_out_t, w_back, pad):
    node = nodes[...]
    node_t = node.T
    fill_ring(pad, node.astype(F32).reshape(CUBE))
    for k in range(K):
        pre = preact[k]
        sigma = jax.nn.sigmoid(pre)
        rate = (sigma * (1.0 + pre * (1.0 - sigma))).reshape(CUBE)
        dact[k] = jnp.where(inside(offs, k), rate, 0.0).reshape(N, W)
        hidden_t[k * W : (k + 1) * W] = hidden[k].T
        here = pl.ds(k * N, N)
        left[:W, here] = ring_shift(pad, offs[k, 0], offs[k, 1], offs[k, 2]).astype(BF16).T
        left[W : 2 * W, here] = node_t
        left[2 * W :, here] = edges[k].T
    w_out_t[...] = w_out[...].T
    w_back[:W] = w_in[W : 2 * W].T
    w_back[W:] = w_in[:W].T


def low(rim, d, a, b):
    return jnp.where(rim[3 * d] > 0, jnp.where(rim[3 * d + 1] > 0, a, 0.0), b)


def high(rim, d, a, b):
    return jnp.where(rim[3 * d] > 0, b, jnp.where(rim[3 * d + 2] > 0, a, 0.0))


def send(rim, d, lo, hi, a, b):
    even = rim[3 * d] > 0
    a[...] = jnp.where(even, lo, hi)
    b[...] = jnp.where(even, hi, lo)


def own(rim, grads, out, first):
    step = grads.shape[0] // (2 * GROUPS)
    mask = jnp.broadcast_to(rim[3, :1, :], (step, W)) > 0
    for g in range(GROUPS):
        even, odd = grads[2 * g * step : (2 * g + 1) * step], grads[(2 * g + 1) * step : (2 * g + 2) * step]
        out[g * step : (g + 1) * step] = jnp.where(mask, even, odd) if first else jnp.where(mask, odd, even)


def add_kernel(keep, got, after, out):
    out[...] = keep[...] + got[...]


def add_x(rim, x, out):
    out[0] = out[0] + low(rim, 0, x[0][...], x[1][...])
    out[B - 1] = out[B - 1] + high(rim, 0, x[0][...], x[1][...])


def add_y(rim, y, out):
    out[:, 0] = out[:, 0] + low(rim, 1, y[0][...], y[1][...])
    out[:, B - 1] = out[:, B - 1] + high(rim, 1, y[0][...], y[1][...])


def add_z(rim, z, out):
    out[:, :, 0, :] = out[:, :, 0, :] + low(rim, 2, z[0][...], z[1][...])
    out[:, :, B - 1, :] = out[:, :, B - 1, :] + high(rim, 2, z[0][...], z[1][...])


def y_faces_after_x(rim, field, x0, x1, a, b, faces):
    for i, at in enumerate((0, B - 1)):
        faces[i] = field[:, at]
        faces[i, 0] = faces[i, 0] + low(rim, 0, x0[at], x1[at])
        faces[i, B - 1] = faces[i, B - 1] + high(rim, 0, x0[at], x1[at])
    send(rim, 1, faces[0], faces[1], a, b)


def z_faces_after_y(rim, field, x0, x1, y0, y1, a, b, faces):
    for i, at in enumerate((0, B - 1)):
        faces[i] = field[:, :, at, :]
        faces[i, 0] = faces[i, 0] + low(rim, 0, x0[:, at, :], x1[:, at, :])
        faces[i, B - 1] = faces[i, B - 1] + high(rim, 0, x0[:, at, :], x1[:, at, :])
        faces[i, :, 0, :] = faces[i, :, 0, :] + low(rim, 1, y0[:, at, :], y1[:, at, :])
        faces[i, :, B - 1, :] = faces[i, :, B - 1, :] + high(rim, 1, y0[:, at, :], y1[:, at, :])
    send(rim, 2, faces[0], faces[1], a, b)


def y_faces_after_z(rim, field, z0, z1, a, b, faces):
    for i, at in enumerate((0, B - 1)):
        faces[i] = field[:, at]
        faces[i, :, 0, :] = faces[i, :, 0, :] + low(rim, 2, z0[:, at, :], z1[:, at, :])
        faces[i, :, B - 1, :] = faces[i, :, B - 1, :] + high(rim, 2, z0[:, at, :], z1[:, at, :])
    send(rim, 1, faces[0], faces[1], a, b)


def x_faces_after_y(rim, field, z0, z1, y0, y1, a, b, faces):
    for i, at in enumerate((0, B - 1)):
        faces[i] = field[at]
        faces[i, :, 0, :] = faces[i, :, 0, :] + low(rim, 2, z0[at], z1[at])
        faces[i, :, B - 1, :] = faces[i, :, B - 1, :] + high(rim, 2, z0[at], z1[at])
        faces[i, 0] = faces[i, 0] + low(rim, 1, y0[at], y1[at])
        faces[i, B - 1] = faces[i, B - 1] + high(rim, 1, y0[at], y1[at])
    send(rim, 0, faces[0], faces[1], a, b)


def whole(rim, field, x0, x1, y0, y1, z0, z1, work):
    work[...] = field[...]
    add_x(rim, (x0, x1), work)
    add_y(rim, (y0, y1), work)
    add_z(rim, (z0, z1), work)
    return work[...].reshape(N, W)


def node_kernel(
    rim, field, x0, x1, y0, y1, z0, z1, inverse, begun, upstream, w_in, w_back,
    local, xa, xb, gathered, slope, hidden, work,
):
    inv = inverse[...]
    agg = (whole(rim, field, x0, x1, y0, y1, z0, z1, work) * inv).astype(BF16)
    gathered[...] = agg
    pre = begun[...] + dot(agg, w_in[W:])
    sigma = jax.nn.sigmoid(pre)
    hidden[...] = (pre * sigma).astype(BF16)
    slo = (upstream[...] * (sigma * (1.0 + pre * (1.0 - sigma)))).astype(BF16)
    slope[...] = slo
    part = (dot(slo, w_back[...]) * inv).reshape(CUBE)
    local[...] = part
    send(rim, 0, part[0], part[B - 1], xa, xb)


def node_grads_kernel(nodes, gathered, slope, hidden, cot, w_in, grads, base):
    slo = slope[...]
    grads[:W] = dot(nodes[...].T, slo)
    grads[W : 2 * W] = dot(gathered[...].T, slo)
    grads[2 * W :] = dot(hidden[...].T, cot[...])
    base[...] = cot[...].astype(F32) + dot_t(slo, w_in[:W])


def edge_kernel(
    rim, field, x0, x1, y0, y1, z0, z1, dact, hidden_t, left, w_out_t, node_grads, slopes, keep, give, work, grads
):
    agg = whole(rim, field, x0, x1, y0, y1, z0, z1, work).astype(BF16)
    back = dot(agg, w_out_t[...])
    for k in range(K):
        slopes[k * N : (k + 1) * N] = (back * dact[k]).astype(BF16)
    outer = dot(hidden_t[...], agg)
    grads[3 * W : 4 * W] = (outer[:W] + outer[W : 2 * W]) + (outer[2 * W : 3 * W] + outer[3 * W :])
    grads[4 * W :] = node_grads[...]
    grads[: 3 * W] = dot(left[...], slopes[...])
    own(rim, grads, keep, True)
    own(rim, grads, give, False)


def node_part_kernel(offs, rim, slopes, base, w_back, local, za, zb, pad):
    part = base[...]
    for k in range(K):
        slo = slopes[k * N : (k + 1) * N]
        fill_ring(pad, slo.astype(F32).reshape(CUBE))
        sent = ring_shift(pad, -offs[k, 0], -offs[k, 1], -offs[k, 2]).astype(BF16)
        part = part + dot(jnp.concatenate([slo, sent], axis=1), w_back[...])
    local[...] = part.reshape(CUBE)
    send(rim, 2, local[:, :, 0, :], local[:, :, B - 1, :], za, zb)


def edge_grad_kernel(slopes, w_in, out):
    out[...] = dot_t(slopes[...], w_in[2 * W :]).astype(BF16)


def last_kernel(rim, field, z0, z1, y0, y1, x0, x1, out, work):
    work[...] = field[...]
    add_z(rim, (z0, z1), work)
    add_y(rim, (y0, y1), work)
    add_x(rim, (x0, x1), work)
    out[...] = work[...].reshape(N, W).astype(BF16)


def fold(rows, pairs, copies, arrived, out):
    total = arrived[: 2 * rows]
    for i in range(1, pairs):
        total = total + arrived[2 * rows * i : 2 * rows * (i + 1)]
    total = total + jnp.concatenate([total[rows:], total[:rows]], axis=0)
    for i in range(copies):
        out[2 * rows * i : 2 * rows * (i + 1)] = total


def fold_with_faces_kernel(faces, rows, pairs, copies, arrived, *refs):
    fold(rows, pairs, copies, arrived, refs[-2])
    faces(*refs[:-2], refs[-1])


def clip_kernel(grads, edge_in, edge_out, node_in, node_out):
    total = grads[...]
    squares = jnp.sum(jnp.sum(total * total, axis=0, keepdims=True), axis=1, keepdims=True)
    factor = math.sqrt(7 * W * W) / jnp.sqrt(squares)
    edge_in[...] = total[: 3 * W] * factor
    edge_out[...] = total[3 * W : 4 * W] * factor
    node_in[...] = total[4 * W : 6 * W] * factor
    node_out[...] = total[6 * W :] * factor


def exchange(a, b, which):
    sizes = [lax.axis_size(axis) for axis in (GX, GY, GZ)]
    aside = {0: 1, 1: 2, 2: 1}[which]
    first, second = [], []
    for me in itertools.product(*map(range, sizes)):
        at = ((me[which] + 1) ^ 1) - 1
        end = at < 0 or at >= sizes[which]
        first.append(moved_to(me, aside, me[aside] ^ 1) if end else moved_to(me, which, at))
        second.append(moved_to(me, which, me[which] ^ 1))
    ranks = {me: rank for rank, me in enumerate(itertools.product(*map(range, sizes)))}
    a, b = (
        lax.ppermute(face, GX + GY + GZ, [(rank, ranks[to]) for rank, to in enumerate(targets)])
        for face, targets in ((a, first), (b, second))
    )
    return a, b


def other_core(half):
    count = math.prod(lax.axis_size(axis) for axis in (GX, GY, GZ))
    step = lax.axis_size(GZ)
    return lax.ppermute(half, GX + GY + GZ, [(rank, rank ^ step) for rank in range(count)])


def moved_to(me, which, at):
    return me[:which] + (at,) + me[which + 1 :]


FACES = [(FACE, F32), (FACE, F32)]
BOTH = pltpu.VMEM((2, *FACE), F32)


def arrivals(rim, field, xa, xb, tag):
    x = exchange(xa, xb, 0)
    a, b = call(y_faces_after_x, FACES, [VMEM] * 4, "after_x" + tag, [BOTH])(rim, field, *x)
    y = exchange(a, b, 1)
    a, b = call(z_faces_after_y, FACES, [VMEM] * 6, "after_y" + tag, [BOTH])(rim, field, *x, *y)
    return (*x, *y, *exchange(a, b, 2))


def swap(rows, axes):
    return lax.all_to_all(rows.reshape(lax.axis_size(axes), -1), axes, 0, 0, tiled=True).reshape(-1, W)


def arrivals_and_sum(rim, field, za, zb, keep, give):
    near, far = lax.axis_size(NEAR), lax.axis_size(FAR)
    rows = keep.shape[0] // near
    (half,) = call(add_kernel, [(keep.shape, F32)], [VMEM] * 3, "add_core")(keep, other_core(give), za)
    got = swap(half, NEAR)
    z = exchange(za, zb, 2)
    a, b, spread = call(
        functools.partial(fold_with_faces_kernel, y_faces_after_z, rows, near // 2, far // 2),
        FACES + [((rows * far, W), F32)],
        [VMEM] * 5,
        "after_z_fold",
        [BOTH],
    )(got, rim, field, *z)
    got = swap(spread, FAR)
    y = exchange(a, b, 1)
    a, b, spread = call(
        functools.partial(fold_with_faces_kernel, x_faces_after_y, rows, far // 2, near),
        FACES + [((2 * rows * near, W), F32)],
        [VMEM] * 7,
        "after_y_fold",
        [BOTH],
    )(got, rim, field, *z, *y)
    total = swap(spread, BACK)
    return (*z, *y, *exchange(a, b, 0)), total


def on_device(node_feat, edge_feat, copies, offsets, w_edge_in, w_edge_out, w_node_in, w_node_out, node_cot):
    cot = node_cot.reshape(N, W)
    inverse = jnp.broadcast_to(1.0 / copies.reshape(N, 1).astype(F32), (N, W))
    square = ((W, W), BF16)
    many = ((K, N, W), BF16)

    xa, xb, rim, nodes, edges, w_in, w_out = call(
        first_rims_kernel,
        FACES + [((9, B, W), F32), ((N, W), BF16), many, ((3 * W, W), BF16), square],
        [HBM] * 5,
        "first_rims",
        [PAD, pltpu.SMEM((K, 3), jnp.int32), pltpu.SemaphoreType.DMA((4 + K,))],
    )(*map(in_hbm, (node_feat.reshape(N, W), edge_feat.reshape(K, N, W), w_edge_in, w_edge_out, offsets)))
    local, preact, hidden = call(
        forward_kernel, [(CUBE, F32), ((K, N, W), F32), many], [SMEM] + [VMEM] * 5, "forward", [PAD]
    )(offsets, nodes, edges, w_in, w_out, rim)
    begun, upstream, w_node_back = call(
        prepare_node_kernel, [((N, W), F32), ((N, W), F32), square], [VMEM] * 5, "prepare_node"
    )(nodes, cot, w_node_in, w_node_out, local)
    arrived = arrivals(rim, local, xa, xb, "_1")
    dact, hidden_t, left, w_out_t, w_back = call(
        prepare_edge_kernel,
        [((K, N, W), F32), ((K * W, N), BF16), ((3 * W, K * N), BF16), square, ((2 * W, W), BF16)],
        [SMEM] + [VMEM] * 6,
        "prepare_edge",
        [PAD],
    )(offsets, preact, hidden, nodes, edges, w_in, w_out)
    local, xa, xb, gathered, slope, node_hidden = call(
        node_kernel, [(CUBE, F32)] + FACES + [((N, W), BF16)] * 3, [VMEM] * 13, "node", [WORK]
    )(rim, local, *arrived, inverse, begun, upstream, w_node_in, w_node_back)
    arrived = arrivals(rim, local, xa, xb, "_2")
    node_grads, base = call(node_grads_kernel, [((3 * W, W), F32), ((N, W), F32)], [VMEM] * 6, "node_grads")(
        nodes, gathered, slope, node_hidden, cot, w_node_in
    )
    half = ((7 * W // 2, W), F32)
    slopes, keep, give = call(
        edge_kernel,
        [((K * N, W), BF16), half, half],
        [VMEM] * 13,
        "edge",
        [WORK, pltpu.VMEM((7 * W, W), F32)],
    )(rim, local, *arrived, dact, hidden_t, left, w_out_t, node_grads)
    local, za, zb = call(
        node_part_kernel, [(CUBE, F32)] + FACES, [SMEM] + [VMEM] * 4, "node_part", [PAD]
    )(offsets, rim, slopes, base, w_back)
    (edge_grad,) = call(edge_grad_kernel, [((K * N, W), BF16)], [VMEM] * 2, "edge_grad")(slopes, w_in)
    arrived, total = arrivals_and_sum(rim, local, za, zb, keep, give)
    clipped = call(
        clip_kernel, [((3 * W, W), F32), ((W, W), F32), ((2 * W, W), F32), ((W, W), F32)], [VMEM], "clip"
    )(total)
    (node_grad,) = call(last_kernel, [((N, W), BF16)], [VMEM] * 8, "last", [WORK])(rim, local, *arrived)
    return (node_grad.reshape(node_feat.shape), edge_grad.reshape(edge_feat.shape), *clipped)


def solution(mesh):
    split = Mesh(mesh.devices.reshape(8, 2, 2, 2, 4), ("z", "yh", "yl", "c", "x"))
    place = (GX, GY, GZ)
    placed = (
        P(*place, None),
        P(None, *place, None),
        P(*place),
        P(),
        P(),
        P(),
        P(),
        P(),
        P(*place, None),
    )
    return jax.shard_map(
        on_device,
        mesh=split,
        in_specs=placed,
        out_specs=(P(*place, None), P(None, *place, None), P(), P(), P(), P()),
        check_vma=False,
    )
```

```python
import functools
import itertools
import math

import jax
import jax.numpy as jnp
from jax import lax
from jax.experimental import pallas as pl
from jax.experimental.pallas import tpu as pltpu
from jax.sharding import Mesh
from jax.sharding import PartitionSpec as P


B = 8
W = 128
K = 4
N = B * B * B
CUBE = (B, B, B, W)
FACE = (B, B, W)
F32 = jnp.float32
BF16 = jnp.bfloat16
GRANT = 12 * 1024 * 1024

VMEM = pl.BlockSpec(memory_space=pltpu.VMEM)
SMEM = pl.BlockSpec(memory_space=pltpu.SMEM)
HBM = pl.BlockSpec(memory_space=pltpu.HBM)
PAD = pltpu.VMEM((B + 2, B + 2, B, W), F32)
WORK = pltpu.VMEM(CUBE, F32)

GX, GY, GZ = ("z", "yh"), ("yl", "c"), ("x",)
NEAR, FAR = ("yh", "yl", "x"), ("z",)


def call(body, outs, specs, scratch=()):
    return pl.pallas_call(
        body,
        out_shape=[jax.ShapeDtypeStruct(s, t) for s, t in outs],
        in_specs=specs,
        out_specs=[VMEM] * len(outs),
        scratch_shapes=list(scratch),
        compiler_params=pltpu.CompilerParams(vmem_limit_bytes=GRANT),
    )


def in_hbm(array):
    return pltpu.with_memory_space_constraint(array, pltpu.HBM)


def dot(a, b):
    return jnp.dot(a, b, preferred_element_type=F32)


def dot_t(a, b):
    return lax.dot_general(a, b, (((1,), (1,)), ((), ())), preferred_element_type=F32)


def fill_ring(pad, value):
    pad[1:9, 1:9] = value
    pad[0, 1:9] = value[7]
    pad[9, 1:9] = value[0]
    pad[:, 0] = pad[:, 8]
    pad[:, 9] = pad[:, 1]


def ring_shift(pad, o0, o1, o2):
    moved = pad[pl.ds(1 + o0, B), pl.ds(1 + o1, B)].reshape(B * B, B, W)
    moved = pltpu.roll(moved, lax.rem(B - o2, B), 1)
    return moved.reshape(N, W)


def inside(offs, k, rims=False):
    ok = None
    shape = (2, *FACE) if rims else CUBE
    for which in range(3):
        at = lax.broadcasted_iota(jnp.int32, shape, which)
        at = (at * (B - 1) if rims and which == 0 else at) + offs[k, which]
        one = (at >= 0) & (at < B)
        ok = one if ok is None else ok & one
    return ok


def fill_masks(rim):
    for d, axis in enumerate((GX, GY, GZ)):
        at, count = jnp.int32(0), 1
        for name in axis:
            size = lax.axis_size(name)
            at, count = at * size + lax.axis_index(name), count * size
        odd = at & 1
        flags = (1 - odd, jnp.where(at > 0, 1 - odd, 0), jnp.where(at < count - 1, odd, 0))
        for i, flag in enumerate(flags):
            rim[3 * d + i] = jnp.full((B, W), flag.astype(F32))


RIMS = (0, (B - 1) * B * B)


def first_rims_kernel(
    nodes_h, edges_h, w_in_h, w_out_h, offs_h, xa, xb, rim, nodes, w_in, w_out, edges, pad, offs, sems
):
    plane = B * B
    pairs = [(nodes_h, nodes), (w_in_h, w_in), (offs_h, offs), (w_out_h, w_out)]
    for k in range(K):
        for i, at in enumerate(RIMS):
            pairs.append((edges_h.at[k, pl.ds(at, plane)], edges.at[k, pl.ds(i * plane, plane)]))
    copies = [pltpu.make_async_copy(a, b, sems.at[i]) for i, (a, b) in enumerate(pairs)]
    for copy in copies:
        copy.start()
    fill_masks(rim)
    for copy in copies[:3]:
        copy.wait()
    node = nodes[...]
    fill_ring(pad, dot(node, w_in[:W]).reshape(CUBE))
    rims = jnp.concatenate([node[at : at + plane] for at in RIMS], axis=0)
    receiver = dot(rims, w_in[W : 2 * W])
    copies[3].wait()
    total = jnp.zeros((2 * plane, W), F32)
    for k in range(K):
        copies[4 + 2 * k].wait()
        copies[5 + 2 * k].wait()
        o0, o1, o2 = offs[k, 0], offs[k, 1], offs[k, 2]
        sent = jnp.concatenate([pad[pl.ds(1 + at + o0, 1), pl.ds(1 + o1, B)] for at in (0, B - 1)], axis=0)
        sent = pltpu.roll(sent.reshape(2 * B, B, W), lax.rem(B - o2, B), 1).reshape(2 * plane, W)
        pre = sent + receiver + dot(edges[k], w_in[2 * W :])
        act = (pre * jax.nn.sigmoid(pre)).reshape(2, B, B, W)
        kept = jnp.where(inside(offs, k, True), act, 0.0).reshape(2 * plane, W).astype(BF16)
        total = total + dot(kept, w_out[...])
    total = total.reshape(2, B, B, W)
    send(rim, 0, total[0], total[1], xa, xb)


def forward_kernel(edges_h, offs, nodes, w_in, w_out, after, local, preact, hidden, edges, pad, sems):
    copies = [pltpu.make_async_copy(edges_h.at[k], edges.at[k], sems.at[k]) for k in range(K)]
    for copy in copies:
        copy.start()
    node = nodes[...]
    fill_ring(pad, dot(node, w_in[:W]).reshape(CUBE))
    receiver = dot(node, w_in[W : 2 * W])
    total = jnp.zeros((N, W), F32)
    for k in range(K):
        copies[k].wait()
        pre = ring_shift(pad, offs[k, 0], offs[k, 1], offs[k, 2]) + receiver + dot(edges[k], w_in[2 * W :])
        preact[k] = pre
        act = (pre * jax.nn.sigmoid(pre)).reshape(CUBE)
        kept = jnp.where(inside(offs, k), act, 0.0).reshape(N, W).astype(BF16)
        hidden[k] = kept
        total = total + dot(kept, w_out[...])
    local[...] = total.reshape(CUBE)


def prepare_node_kernel(nodes, cot, w_in, w_out, after, pre, upstream, w_back):
    pre[...] = dot(nodes[...], w_in[:W])
    upstream[...] = dot_t(cot[...], w_out[...])
    w_back[...] = w_in[W:].T


def prepare_edge_kernel(offs, preact, hidden, nodes, edges, w_in, w_out, dact, hidden_t, left, w_out_t, w_back, pad):
    node = nodes[...]
    node_t = node.T
    fill_ring(pad, node.astype(F32).reshape(CUBE))
    for k in range(K):
        pre = preact[k]
        sigma = jax.nn.sigmoid(pre)
        rate = (sigma * (1.0 + pre * (1.0 - sigma))).reshape(CUBE)
        dact[k] = jnp.where(inside(offs, k), rate, 0.0).reshape(N, W)
        hidden_t[k * W : (k + 1) * W] = hidden[k].T
        here = pl.ds(k * N, N)
        left[:W, here] = ring_shift(pad, offs[k, 0], offs[k, 1], offs[k, 2]).astype(BF16).T
        left[W : 2 * W, here] = node_t
        left[2 * W :, here] = edges[k].T
    w_out_t[...] = w_out[...].T
    w_back[:W] = w_in[W : 2 * W].T
    w_back[W:] = w_in[:W].T


def low(rim, d, a, b):
    return jnp.where(rim[3 * d] > 0, jnp.where(rim[3 * d + 1] > 0, a, 0.0), b)


def high(rim, d, a, b):
    return jnp.where(rim[3 * d] > 0, b, jnp.where(rim[3 * d + 2] > 0, a, 0.0))


def send(rim, d, lo, hi, a, b):
    even = rim[3 * d] > 0
    a[...] = jnp.where(even, lo, hi)
    b[...] = jnp.where(even, hi, lo)


def own(rim, top, bottom):
    first = jnp.broadcast_to(rim[3, :1, :], top.shape) > 0
    return jnp.where(first, top, bottom)


def add_kernel(keep, got, after, out):
    out[...] = keep[...] + got[...]


def add_x(rim, x, out):
    out[0] = out[0] + low(rim, 0, x[0][...], x[1][...])
    out[B - 1] = out[B - 1] + high(rim, 0, x[0][...], x[1][...])


def add_y(rim, y, out):
    out[:, 0] = out[:, 0] + low(rim, 1, y[0][...], y[1][...])
    out[:, B - 1] = out[:, B - 1] + high(rim, 1, y[0][...], y[1][...])


def add_z(rim, z, out):
    out[:, :, 0, :] = out[:, :, 0, :] + low(rim, 2, z[0][...], z[1][...])
    out[:, :, B - 1, :] = out[:, :, B - 1, :] + high(rim, 2, z[0][...], z[1][...])


def y_faces_after_x(rim, field, x0, x1, a, b, faces):
    for i, at in enumerate((0, B - 1)):
        faces[i] = field[:, at]
        faces[i, 0] = faces[i, 0] + low(rim, 0, x0[at], x1[at])
        faces[i, B - 1] = faces[i, B - 1] + high(rim, 0, x0[at], x1[at])
    send(rim, 1, faces[0], faces[1], a, b)


def z_faces_after_y(rim, field, x0, x1, y0, y1, a, b, faces):
    for i, at in enumerate((0, B - 1)):
        faces[i] = field[:, :, at, :]
        faces[i, 0] = faces[i, 0] + low(rim, 0, x0[:, at, :], x1[:, at, :])
        faces[i, B - 1] = faces[i, B - 1] + high(rim, 0, x0[:, at, :], x1[:, at, :])
        faces[i, :, 0, :] = faces[i, :, 0, :] + low(rim, 1, y0[:, at, :], y1[:, at, :])
        faces[i, :, B - 1, :] = faces[i, :, B - 1, :] + high(rim, 1, y0[:, at, :], y1[:, at, :])
    send(rim, 2, faces[0], faces[1], a, b)


def y_faces_after_z(rim, field, z0, z1, a, b, faces):
    for i, at in enumerate((0, B - 1)):
        faces[i] = field[:, at]
        faces[i, :, 0, :] = faces[i, :, 0, :] + low(rim, 2, z0[:, at, :], z1[:, at, :])
        faces[i, :, B - 1, :] = faces[i, :, B - 1, :] + high(rim, 2, z0[:, at, :], z1[:, at, :])
    send(rim, 1, faces[0], faces[1], a, b)


def x_faces_after_y(rim, field, z0, z1, y0, y1, a, b, faces):
    for i, at in enumerate((0, B - 1)):
        faces[i] = field[at]
        faces[i, :, 0, :] = faces[i, :, 0, :] + low(rim, 2, z0[at], z1[at])
        faces[i, :, B - 1, :] = faces[i, :, B - 1, :] + high(rim, 2, z0[at], z1[at])
        faces[i, 0] = faces[i, 0] + low(rim, 1, y0[at], y1[at])
        faces[i, B - 1] = faces[i, B - 1] + high(rim, 1, y0[at], y1[at])
    send(rim, 0, faces[0], faces[1], a, b)


def whole(rim, field, x0, x1, y0, y1, z0, z1, work):
    work[...] = field[...]
    add_x(rim, (x0, x1), work)
    add_y(rim, (y0, y1), work)
    add_z(rim, (z0, z1), work)
    return work[...].reshape(N, W)


def node_kernel(
    rim, field, x0, x1, y0, y1, z0, z1, inverse, begun, upstream, w_in, w_back,
    local, xa, xb, gathered, slope, hidden, work,
):
    inv = inverse[...]
    agg = (whole(rim, field, x0, x1, y0, y1, z0, z1, work) * inv).astype(BF16)
    gathered[...] = agg
    pre = begun[...] + dot(agg, w_in[W:])
    sigma = jax.nn.sigmoid(pre)
    hidden[...] = (pre * sigma).astype(BF16)
    slo = (upstream[...] * (sigma * (1.0 + pre * (1.0 - sigma)))).astype(BF16)
    slope[...] = slo
    part = (dot(slo, w_back[...]) * inv).reshape(CUBE)
    local[...] = part
    send(rim, 0, part[0], part[B - 1], xa, xb)


def node_grads_kernel(nodes, gathered, slope, hidden, cot, w_in, grads, base):
    slo = slope[...]
    grads[:W] = dot(nodes[...].T, slo)
    grads[W : 2 * W] = dot(gathered[...].T, slo)
    grads[2 * W :] = dot(hidden[...].T, cot[...])
    base[...] = cot[...].astype(F32) + dot_t(slo, w_in[:W])


def edge_kernel(
    rim, field, x0, x1, y0, y1, z0, z1, dact, hidden_t, left, w_out_t, node_grads, slopes, keep, give, work, grads
):
    agg = whole(rim, field, x0, x1, y0, y1, z0, z1, work).astype(BF16)
    back = dot(agg, w_out_t[...])
    for k in range(K):
        slopes[k * N : (k + 1) * N] = (back * dact[k]).astype(BF16)
    outer = dot(hidden_t[...], agg)
    grads[3 * W : 4 * W] = (outer[:W] + outer[W : 2 * W]) + (outer[2 * W : 3 * W] + outer[3 * W :])
    grads[4 * W :] = node_grads[...]
    grads[: 3 * W] = dot(left[...], slopes[...])
    half = keep.shape[0]
    keep[...] = own(rim, grads[:half], grads[half:])
    give[...] = own(rim, grads[half:], grads[:half])


def node_part_kernel(offs, rim, slopes, base, w_back, local, za, zb, pad):
    part = base[...]
    for k in range(K):
        slo = slopes[k * N : (k + 1) * N]
        fill_ring(pad, slo.astype(F32).reshape(CUBE))
        sent = ring_shift(pad, -offs[k, 0], -offs[k, 1], -offs[k, 2]).astype(BF16)
        part = part + dot(jnp.concatenate([slo, sent], axis=1), w_back[...])
    local[...] = part.reshape(CUBE)
    send(rim, 2, local[:, :, 0, :], local[:, :, B - 1, :], za, zb)


def edge_grad_kernel(slopes, w_in, out):
    out[...] = dot_t(slopes[...], w_in[2 * W :]).astype(BF16)


def last_kernel(rim, field, z0, z1, y0, y1, x0, x1, out, work):
    work[...] = field[...]
    add_z(rim, (z0, z1), work)
    add_y(rim, (y0, y1), work)
    add_x(rim, (x0, x1), work)
    out[...] = work[...].reshape(N, W).astype(BF16)


def fold(rows, pairs, copies, arrived, out):
    total = arrived[: 2 * rows]
    for i in range(1, pairs):
        total = total + arrived[2 * rows * i : 2 * rows * (i + 1)]
    total = total + jnp.concatenate([total[rows:], total[:rows]], axis=0)
    for i in range(copies):
        out[2 * rows * i : 2 * rows * (i + 1)] = total


def fold_with_faces_kernel(faces, rows, pairs, copies, arrived, *refs):
    fold(rows, pairs, copies, arrived, refs[-2])
    faces(*refs[:-2], refs[-1])


def clip_kernel(rim, mine, other, edge_in, edge_out, node_in, node_out):
    total = jnp.concatenate([own(rim, mine[...], other[...]), own(rim, other[...], mine[...])], axis=0)
    squares = jnp.sum(jnp.sum(total * total, axis=0, keepdims=True), axis=1, keepdims=True)
    factor = math.sqrt(7 * W * W) / jnp.sqrt(squares)
    edge_in[...] = total[: 3 * W] * factor
    edge_out[...] = total[3 * W : 4 * W] * factor
    node_in[...] = total[4 * W : 6 * W] * factor
    node_out[...] = total[6 * W :] * factor


def exchange(a, b, which):
    sizes = [lax.axis_size(axis) for axis in (GX, GY, GZ)]
    aside = {0: 1, 1: 2, 2: 1}[which]
    first, second = [], []
    for me in itertools.product(*map(range, sizes)):
        at = ((me[which] + 1) ^ 1) - 1
        end = at < 0 or at >= sizes[which]
        first.append(moved_to(me, aside, me[aside] ^ 1) if end else moved_to(me, which, at))
        second.append(moved_to(me, which, me[which] ^ 1))
    ranks = {me: rank for rank, me in enumerate(itertools.product(*map(range, sizes)))}
    a, b = (
        lax.ppermute(face, GX + GY + GZ, [(rank, ranks[to]) for rank, to in enumerate(targets)])
        for face, targets in ((a, first), (b, second))
    )
    return a, b


def other_core(half):
    count = math.prod(lax.axis_size(axis) for axis in (GX, GY, GZ))
    step = lax.axis_size(GZ)
    return lax.ppermute(half, GX + GY + GZ, [(rank, rank ^ step) for rank in range(count)])


def moved_to(me, which, at):
    return me[:which] + (at,) + me[which + 1 :]


FACES = [(FACE, F32), (FACE, F32)]
BOTH = pltpu.VMEM((2, *FACE), F32)


def arrivals(rim, field, xa, xb):
    x = exchange(xa, xb, 0)
    a, b = call(y_faces_after_x, FACES, [VMEM] * 4, [BOTH])(rim, field, *x)
    y = exchange(a, b, 1)
    a, b = call(z_faces_after_y, FACES, [VMEM] * 6, [BOTH])(rim, field, *x, *y)
    return (*x, *y, *exchange(a, b, 2))


def swap(rows, axes):
    return lax.all_to_all(rows.reshape(lax.axis_size(axes), -1), axes, 0, 0, tiled=True).reshape(-1, W)


def arrivals_and_sum(rim, field, za, zb, keep, give):
    near, far = lax.axis_size(NEAR), lax.axis_size(FAR)
    rows = keep.shape[0] // near
    (half,) = call(add_kernel, [(keep.shape, F32)], [VMEM] * 3)(keep, other_core(give), za)
    got = swap(half, NEAR)
    z = exchange(za, zb, 2)
    a, b, spread = call(
        functools.partial(fold_with_faces_kernel, y_faces_after_z, rows, near // 2, far // 2),
        FACES + [((rows * far, W), F32)],
        [VMEM] * 5,
        [BOTH],
    )(got, rim, field, *z)
    got = swap(spread, FAR)
    y = exchange(a, b, 1)
    a, b, spread = call(
        functools.partial(fold_with_faces_kernel, x_faces_after_y, rows, far // 2, near // 2),
        FACES + [((rows * near, W), F32)],
        [VMEM] * 7,
        [BOTH],
    )(got, rim, field, *z, *y)
    mine = swap(spread, NEAR)
    x = exchange(a, b, 0)
    return (*z, *y, *x), (mine, other_core(mine))


def on_device(node_feat, edge_feat, copies, offsets, w_edge_in, w_edge_out, w_node_in, w_node_out, node_cot):
    cot = node_cot.reshape(N, W)
    inverse = jnp.broadcast_to(1.0 / copies.reshape(N, 1).astype(F32), (N, W))
    square = ((W, W), BF16)
    many = ((K, N, W), BF16)

    edges_all = in_hbm(edge_feat.reshape(K, N, W))
    xa, xb, rim, nodes, w_in, w_out = call(
        first_rims_kernel,
        FACES + [((9, B, W), F32), ((N, W), BF16), ((3 * W, W), BF16), square],
        [HBM] * 5,
        [
            pltpu.VMEM((K, 2 * B * B, W), BF16),
            PAD,
            pltpu.SMEM((K, 3), jnp.int32),
            pltpu.SemaphoreType.DMA((4 + 2 * K,)),
        ],
    )(in_hbm(node_feat.reshape(N, W)), edges_all, in_hbm(w_edge_in), in_hbm(w_edge_out), in_hbm(offsets))
    local, preact, hidden, edges = call(
        forward_kernel,
        [(CUBE, F32), ((K, N, W), F32), many, many],
        [HBM, SMEM] + [VMEM] * 4,
        [PAD, pltpu.SemaphoreType.DMA((K,))],
    )(edges_all, offsets, nodes, w_in, w_out, rim)
    begun, upstream, w_node_back = call(
        prepare_node_kernel, [((N, W), F32), ((N, W), F32), square], [VMEM] * 5
    )(nodes, cot, w_node_in, w_node_out, local)
    arrived = arrivals(rim, local, xa, xb)
    dact, hidden_t, left, w_out_t, w_back = call(
        prepare_edge_kernel,
        [((K, N, W), F32), ((K * W, N), BF16), ((3 * W, K * N), BF16), square, ((2 * W, W), BF16)],
        [SMEM] + [VMEM] * 6,
        [PAD],
    )(offsets, preact, hidden, nodes, edges, w_in, w_out)
    local, xa, xb, gathered, slope, node_hidden = call(
        node_kernel, [(CUBE, F32)] + FACES + [((N, W), BF16)] * 3, [VMEM] * 13, [WORK]
    )(rim, local, *arrived, inverse, begun, upstream, w_node_in, w_node_back)
    arrived = arrivals(rim, local, xa, xb)
    node_grads, base = call(node_grads_kernel, [((3 * W, W), F32), ((N, W), F32)], [VMEM] * 6)(
        nodes, gathered, slope, node_hidden, cot, w_node_in
    )
    half = ((7 * W // 2, W), F32)
    slopes, keep, give = call(
        edge_kernel, [((K * N, W), BF16), half, half], [VMEM] * 13, [WORK, pltpu.VMEM((7 * W, W), F32)]
    )(rim, local, *arrived, dact, hidden_t, left, w_out_t, node_grads)
    local, za, zb = call(
        node_part_kernel, [(CUBE, F32)] + FACES, [SMEM] + [VMEM] * 4, [PAD]
    )(offsets, rim, slopes, base, w_back)
    (edge_grad,) = call(edge_grad_kernel, [((K * N, W), BF16)], [VMEM] * 2)(slopes, w_in)
    arrived, halves = arrivals_and_sum(rim, local, za, zb, keep, give)
    clipped = call(
        clip_kernel, [((3 * W, W), F32), ((W, W), F32), ((2 * W, W), F32), ((W, W), F32)], [VMEM] * 3
    )(rim, *halves)
    (node_grad,) = call(last_kernel, [((N, W), BF16)], [VMEM] * 8, [WORK])(rim, local, *arrived)
    return (node_grad.reshape(node_feat.shape), edge_grad.reshape(edge_feat.shape), *clipped)


def solution(mesh):
    split = Mesh(mesh.devices.reshape(8, 2, 2, 2, 4), ("z", "yh", "yl", "c", "x"))
    place = (GX, GY, GZ)
    placed = (
        P(*place, None),
        P(None, *place, None),
        P(*place),
        P(),
        P(),
        P(),
        P(),
        P(),
        P(*place, None),
    )

    return jax.shard_map(
        on_device,
        mesh=split,
        in_specs=placed,
        out_specs=(P(*place, None), P(None, *place, None), P(), P(), P(), P()),
        check_vma=False,
    )
```

```python
import functools
import itertools
import math

import jax
import jax.numpy as jnp
from jax import lax
from jax.experimental import pallas as pl
from jax.experimental.pallas import tpu as pltpu
from jax.sharding import Mesh
from jax.sharding import PartitionSpec as P


B = 8
W = 128
K = 4
N = B * B * B
CUBE = (B, B, B, W)
FACE = (B, B, W)
F32 = jnp.float32
BF16 = jnp.bfloat16
GRANT = 12 * 1024 * 1024

VMEM = pl.BlockSpec(memory_space=pltpu.VMEM)
SMEM = pl.BlockSpec(memory_space=pltpu.SMEM)
HBM = pl.BlockSpec(memory_space=pltpu.HBM)
PAD = pltpu.VMEM((B + 2, B + 2, B, W), F32)
WORK = pltpu.VMEM(CUBE, F32)

GX, GY, GZ = ("z", "yh"), ("yl", "c"), ("x",)
NEAR, FAR = ("yh", "yl", "x"), ("z",)


def call(body, outs, specs, scratch=()):
    return pl.pallas_call(
        body,
        out_shape=[jax.ShapeDtypeStruct(s, t) for s, t in outs],
        in_specs=specs,
        out_specs=[VMEM] * len(outs),
        scratch_shapes=list(scratch),
        compiler_params=pltpu.CompilerParams(vmem_limit_bytes=GRANT),
    )


def in_hbm(array):
    return pltpu.with_memory_space_constraint(array, pltpu.HBM)


def dot(a, b):
    return jnp.dot(a, b, preferred_element_type=F32)


def dot_t(a, b):
    return lax.dot_general(a, b, (((1,), (1,)), ((), ())), preferred_element_type=F32)


def fill_ring(pad, value):
    pad[1:9, 1:9] = value
    pad[0, 1:9] = value[7]
    pad[9, 1:9] = value[0]
    pad[:, 0] = pad[:, 8]
    pad[:, 9] = pad[:, 1]


def ring_shift(pad, o0, o1, o2):
    moved = pad[pl.ds(1 + o0, B), pl.ds(1 + o1, B)].reshape(B * B, B, W)
    moved = pltpu.roll(moved, lax.rem(B - o2, B), 1)
    return moved.reshape(N, W)


def inside(offs, k, rims=False):
    ok = None
    shape = (2, *FACE) if rims else CUBE
    for which in range(3):
        at = lax.broadcasted_iota(jnp.int32, shape, which)
        at = (at * (B - 1) if rims and which == 0 else at) + offs[k, which]
        one = (at >= 0) & (at < B)
        ok = one if ok is None else ok & one
    return ok


def fill_masks(rim):
    for d, axis in enumerate((GX, GY, GZ)):
        at, count = jnp.int32(0), 1
        for name in axis:
            size = lax.axis_size(name)
            at, count = at * size + lax.axis_index(name), count * size
        odd = at & 1
        flags = (1 - odd, jnp.where(at > 0, 1 - odd, 0), jnp.where(at < count - 1, odd, 0))
        for i, flag in enumerate(flags):
            rim[3 * d + i] = jnp.full((B, W), flag.astype(F32))


RIMS = (0, (B - 1) * B * B)


def first_rims_kernel(
    nodes_h, edges_h, w_in_h, w_out_h, offs_h, xa, xb, rim, nodes, edges, w_in, w_out, pad, offs, sems
):
    plane = B * B
    pairs = [(nodes_h, nodes), (w_in_h, w_in), (offs_h, offs), (w_out_h, w_out)]
    pairs += [(edges_h.at[k], edges.at[k]) for k in range(K)]
    copies = [pltpu.make_async_copy(a, b, sems.at[i]) for i, (a, b) in enumerate(pairs)]
    for copy in copies:
        copy.start()
    fill_masks(rim)
    for copy in copies[:3]:
        copy.wait()
    node = nodes[...]
    fill_ring(pad, dot(node, w_in[:W]).reshape(CUBE))
    rims = jnp.concatenate([node[at : at + plane] for at in RIMS], axis=0)
    receiver = dot(rims, w_in[W : 2 * W])
    copies[3].wait()
    total = jnp.zeros((2 * plane, W), F32)
    for k in range(K):
        copies[4 + k].wait()
        o0, o1, o2 = offs[k, 0], offs[k, 1], offs[k, 2]
        sent = jnp.concatenate([pad[pl.ds(1 + at + o0, 1), pl.ds(1 + o1, B)] for at in (0, B - 1)], axis=0)
        sent = pltpu.roll(sent.reshape(2 * B, B, W), lax.rem(B - o2, B), 1).reshape(2 * plane, W)
        edge = jnp.concatenate([edges[k, at : at + plane] for at in RIMS], axis=0)
        pre = sent + receiver + dot(edge, w_in[2 * W :])
        act = (pre * jax.nn.sigmoid(pre)).reshape(2, B, B, W)
        kept = jnp.where(inside(offs, k, True), act, 0.0).reshape(2 * plane, W).astype(BF16)
        total = total + dot(kept, w_out[...])
    total = total.reshape(2, B, B, W)
    send(rim, 0, total[0], total[1], xa, xb)


def forward_kernel(offs, nodes, edges, w_in, w_out, after, local, preact, hidden, pad):
    node = nodes[...]
    fill_ring(pad, dot(node, w_in[:W]).reshape(CUBE))
    receiver = dot(node, w_in[W : 2 * W])
    total = jnp.zeros((N, W), F32)
    for k in range(K):
        pre = ring_shift(pad, offs[k, 0], offs[k, 1], offs[k, 2]) + receiver + dot(edges[k], w_in[2 * W :])
        preact[k] = pre
        act = (pre * jax.nn.sigmoid(pre)).reshape(CUBE)
        kept = jnp.where(inside(offs, k), act, 0.0).reshape(N, W).astype(BF16)
        hidden[k] = kept
        total = total + dot(kept, w_out[...])
    local[...] = total.reshape(CUBE)


def prepare_node_kernel(nodes, cot, w_in, w_out, after, pre, upstream, w_back):
    pre[...] = dot(nodes[...], w_in[:W])
    upstream[...] = dot_t(cot[...], w_out[...])
    w_back[...] = w_in[W:].T


def prepare_edge_kernel(offs, preact, hidden, nodes, edges, w_in, w_out, dact, hidden_t, left, w_out_t, w_back, pad):
    node = nodes[...]
    node_t = node.T
    fill_ring(pad, node.astype(F32).reshape(CUBE))
    for k in range(K):
        pre = preact[k]
        sigma = jax.nn.sigmoid(pre)
        rate = (sigma * (1.0 + pre * (1.0 - sigma))).reshape(CUBE)
        dact[k] = jnp.where(inside(offs, k), rate, 0.0).reshape(N, W)
        hidden_t[k * W : (k + 1) * W] = hidden[k].T
        here = pl.ds(k * N, N)
        left[:W, here] = ring_shift(pad, offs[k, 0], offs[k, 1], offs[k, 2]).astype(BF16).T
        left[W : 2 * W, here] = node_t
        left[2 * W :, here] = edges[k].T
    w_out_t[...] = w_out[...].T
    w_back[:W] = w_in[W : 2 * W].T
    w_back[W:] = w_in[:W].T


def low(rim, d, a, b):
    return jnp.where(rim[3 * d] > 0, jnp.where(rim[3 * d + 1] > 0, a, 0.0), b)


def high(rim, d, a, b):
    return jnp.where(rim[3 * d] > 0, b, jnp.where(rim[3 * d + 2] > 0, a, 0.0))


def send(rim, d, lo, hi, a, b):
    even = rim[3 * d] > 0
    a[...] = jnp.where(even, lo, hi)
    b[...] = jnp.where(even, hi, lo)


def own(rim, top, bottom):
    first = jnp.broadcast_to(rim[3, :1, :], top.shape) > 0
    return jnp.where(first, top, bottom)


def add_kernel(keep, got, after, out):
    out[...] = keep[...] + got[...]


def add_x(rim, x, out):
    out[0] = out[0] + low(rim, 0, x[0][...], x[1][...])
    out[B - 1] = out[B - 1] + high(rim, 0, x[0][...], x[1][...])


def add_y(rim, y, out):
    out[:, 0] = out[:, 0] + low(rim, 1, y[0][...], y[1][...])
    out[:, B - 1] = out[:, B - 1] + high(rim, 1, y[0][...], y[1][...])


def add_z(rim, z, out):
    out[:, :, 0, :] = out[:, :, 0, :] + low(rim, 2, z[0][...], z[1][...])
    out[:, :, B - 1, :] = out[:, :, B - 1, :] + high(rim, 2, z[0][...], z[1][...])


def y_faces_after_x(rim, field, x0, x1, a, b, faces):
    for i, at in enumerate((0, B - 1)):
        faces[i] = field[:, at]
        faces[i, 0] = faces[i, 0] + low(rim, 0, x0[at], x1[at])
        faces[i, B - 1] = faces[i, B - 1] + high(rim, 0, x0[at], x1[at])
    send(rim, 1, faces[0], faces[1], a, b)


def z_faces_after_y(rim, field, x0, x1, y0, y1, a, b, faces):
    for i, at in enumerate((0, B - 1)):
        faces[i] = field[:, :, at, :]
        faces[i, 0] = faces[i, 0] + low(rim, 0, x0[:, at, :], x1[:, at, :])
        faces[i, B - 1] = faces[i, B - 1] + high(rim, 0, x0[:, at, :], x1[:, at, :])
        faces[i, :, 0, :] = faces[i, :, 0, :] + low(rim, 1, y0[:, at, :], y1[:, at, :])
        faces[i, :, B - 1, :] = faces[i, :, B - 1, :] + high(rim, 1, y0[:, at, :], y1[:, at, :])
    send(rim, 2, faces[0], faces[1], a, b)


def y_faces_after_z(rim, field, z0, z1, a, b, faces):
    for i, at in enumerate((0, B - 1)):
        faces[i] = field[:, at]
        faces[i, :, 0, :] = faces[i, :, 0, :] + low(rim, 2, z0[:, at, :], z1[:, at, :])
        faces[i, :, B - 1, :] = faces[i, :, B - 1, :] + high(rim, 2, z0[:, at, :], z1[:, at, :])
    send(rim, 1, faces[0], faces[1], a, b)


def x_faces_after_y(rim, field, z0, z1, y0, y1, a, b, faces):
    for i, at in enumerate((0, B - 1)):
        faces[i] = field[at]
        faces[i, :, 0, :] = faces[i, :, 0, :] + low(rim, 2, z0[at], z1[at])
        faces[i, :, B - 1, :] = faces[i, :, B - 1, :] + high(rim, 2, z0[at], z1[at])
        faces[i, 0] = faces[i, 0] + low(rim, 1, y0[at], y1[at])
        faces[i, B - 1] = faces[i, B - 1] + high(rim, 1, y0[at], y1[at])
    send(rim, 0, faces[0], faces[1], a, b)


def whole(rim, field, x0, x1, y0, y1, z0, z1, work):
    work[...] = field[...]
    add_x(rim, (x0, x1), work)
    add_y(rim, (y0, y1), work)
    add_z(rim, (z0, z1), work)
    return work[...].reshape(N, W)


def node_kernel(
    rim, field, x0, x1, y0, y1, z0, z1, inverse, begun, upstream, w_in, w_back,
    local, xa, xb, gathered, slope, hidden, work,
):
    inv = inverse[...]
    agg = (whole(rim, field, x0, x1, y0, y1, z0, z1, work) * inv).astype(BF16)
    gathered[...] = agg
    pre = begun[...] + dot(agg, w_in[W:])
    sigma = jax.nn.sigmoid(pre)
    hidden[...] = (pre * sigma).astype(BF16)
    slo = (upstream[...] * (sigma * (1.0 + pre * (1.0 - sigma)))).astype(BF16)
    slope[...] = slo
    part = (dot(slo, w_back[...]) * inv).reshape(CUBE)
    local[...] = part
    send(rim, 0, part[0], part[B - 1], xa, xb)


def node_grads_kernel(nodes, gathered, slope, hidden, cot, w_in, grads, base):
    slo = slope[...]
    grads[:W] = dot(nodes[...].T, slo)
    grads[W : 2 * W] = dot(gathered[...].T, slo)
    grads[2 * W :] = dot(hidden[...].T, cot[...])
    base[...] = cot[...].astype(F32) + dot_t(slo, w_in[:W])


def edge_kernel(
    rim, field, x0, x1, y0, y1, z0, z1, dact, hidden_t, left, w_out_t, node_grads, slopes, keep, give, work, grads
):
    agg = whole(rim, field, x0, x1, y0, y1, z0, z1, work).astype(BF16)
    back = dot(agg, w_out_t[...])
    for k in range(K):
        slopes[k * N : (k + 1) * N] = (back * dact[k]).astype(BF16)
    outer = dot(hidden_t[...], agg)
    grads[3 * W : 4 * W] = (outer[:W] + outer[W : 2 * W]) + (outer[2 * W : 3 * W] + outer[3 * W :])
    grads[4 * W :] = node_grads[...]
    grads[: 3 * W] = dot(left[...], slopes[...])
    half = keep.shape[0]
    keep[...] = own(rim, grads[:half], grads[half:])
    give[...] = own(rim, grads[half:], grads[:half])


def node_part_kernel(offs, rim, slopes, base, w_back, local, za, zb, pad):
    part = base[...]
    for k in range(K):
        slo = slopes[k * N : (k + 1) * N]
        fill_ring(pad, slo.astype(F32).reshape(CUBE))
        sent = ring_shift(pad, -offs[k, 0], -offs[k, 1], -offs[k, 2]).astype(BF16)
        part = part + dot(jnp.concatenate([slo, sent], axis=1), w_back[...])
    local[...] = part.reshape(CUBE)
    send(rim, 2, local[:, :, 0, :], local[:, :, B - 1, :], za, zb)


def edge_grad_kernel(slopes, w_in, out):
    out[...] = dot_t(slopes[...], w_in[2 * W :]).astype(BF16)


def last_kernel(rim, field, z0, z1, y0, y1, x0, x1, out, work):
    work[...] = field[...]
    add_z(rim, (z0, z1), work)
    add_y(rim, (y0, y1), work)
    add_x(rim, (x0, x1), work)
    out[...] = work[...].reshape(N, W).astype(BF16)


def fold(rows, pairs, copies, arrived, out):
    total = arrived[: 2 * rows]
    for i in range(1, pairs):
        total = total + arrived[2 * rows * i : 2 * rows * (i + 1)]
    total = total + jnp.concatenate([total[rows:], total[:rows]], axis=0)
    for i in range(copies):
        out[2 * rows * i : 2 * rows * (i + 1)] = total


def fold_with_faces_kernel(faces, rows, pairs, copies, arrived, *refs):
    fold(rows, pairs, copies, arrived, refs[-2])
    faces(*refs[:-2], refs[-1])


def clip_kernel(rim, mine, other, edge_in, edge_out, node_in, node_out):
    total = jnp.concatenate([own(rim, mine[...], other[...]), own(rim, other[...], mine[...])], axis=0)
    squares = jnp.sum(jnp.sum(total * total, axis=0, keepdims=True), axis=1, keepdims=True)
    factor = math.sqrt(7 * W * W) / jnp.sqrt(squares)
    edge_in[...] = total[: 3 * W] * factor
    edge_out[...] = total[3 * W : 4 * W] * factor
    node_in[...] = total[4 * W : 6 * W] * factor
    node_out[...] = total[6 * W :] * factor


def exchange(a, b, which):
    sizes = [lax.axis_size(axis) for axis in (GX, GY, GZ)]
    aside = {0: 1, 1: 2, 2: 1}[which]
    first, second = [], []
    for me in itertools.product(*map(range, sizes)):
        at = ((me[which] + 1) ^ 1) - 1
        end = at < 0 or at >= sizes[which]
        first.append(moved_to(me, aside, me[aside] ^ 1) if end else moved_to(me, which, at))
        second.append(moved_to(me, which, me[which] ^ 1))
    ranks = {me: rank for rank, me in enumerate(itertools.product(*map(range, sizes)))}
    a, b = (
        lax.ppermute(face, GX + GY + GZ, [(rank, ranks[to]) for rank, to in enumerate(targets)])
        for face, targets in ((a, first), (b, second))
    )
    return a, b


def other_core(half):
    count = math.prod(lax.axis_size(axis) for axis in (GX, GY, GZ))
    step = lax.axis_size(GZ)
    return lax.ppermute(half, GX + GY + GZ, [(rank, rank ^ step) for rank in range(count)])


def moved_to(me, which, at):
    return me[:which] + (at,) + me[which + 1 :]


FACES = [(FACE, F32), (FACE, F32)]
BOTH = pltpu.VMEM((2, *FACE), F32)


def arrivals(rim, field, xa, xb):
    x = exchange(xa, xb, 0)
    a, b = call(y_faces_after_x, FACES, [VMEM] * 4, [BOTH])(rim, field, *x)
    y = exchange(a, b, 1)
    a, b = call(z_faces_after_y, FACES, [VMEM] * 6, [BOTH])(rim, field, *x, *y)
    return (*x, *y, *exchange(a, b, 2))


def swap(rows, axes):
    return lax.all_to_all(rows.reshape(lax.axis_size(axes), -1), axes, 0, 0, tiled=True).reshape(-1, W)


def arrivals_and_sum(rim, field, za, zb, keep, give):
    near, far = lax.axis_size(NEAR), lax.axis_size(FAR)
    rows = keep.shape[0] // near
    (half,) = call(add_kernel, [(keep.shape, F32)], [VMEM] * 3)(keep, other_core(give), za)
    got = swap(half, NEAR)
    z = exchange(za, zb, 2)
    a, b, spread = call(
        functools.partial(fold_with_faces_kernel, y_faces_after_z, rows, near // 2, far // 2),
        FACES + [((rows * far, W), F32)],
        [VMEM] * 5,
        [BOTH],
    )(got, rim, field, *z)
    got = swap(spread, FAR)
    y = exchange(a, b, 1)
    a, b, spread = call(
        functools.partial(fold_with_faces_kernel, x_faces_after_y, rows, far // 2, near // 2),
        FACES + [((rows * near, W), F32)],
        [VMEM] * 7,
        [BOTH],
    )(got, rim, field, *z, *y)
    mine = swap(spread, NEAR)
    x = exchange(a, b, 0)
    return (*z, *y, *x), (mine, other_core(mine))


def on_device(node_feat, edge_feat, copies, offsets, w_edge_in, w_edge_out, w_node_in, w_node_out, node_cot):
    cot = node_cot.reshape(N, W)
    inverse = jnp.broadcast_to(1.0 / copies.reshape(N, 1).astype(F32), (N, W))
    square = ((W, W), BF16)
    many = ((K, N, W), BF16)

    xa, xb, rim, nodes, edges, w_in, w_out = call(
        first_rims_kernel,
        FACES + [((9, B, W), F32), ((N, W), BF16), many, ((3 * W, W), BF16), square],
        [HBM] * 5,
        [PAD, pltpu.SMEM((K, 3), jnp.int32), pltpu.SemaphoreType.DMA((4 + K,))],
    )(*map(in_hbm, (node_feat.reshape(N, W), edge_feat.reshape(K, N, W), w_edge_in, w_edge_out, offsets)))
    local, preact, hidden = call(
        forward_kernel, [(CUBE, F32), ((K, N, W), F32), many], [SMEM] + [VMEM] * 5, [PAD]
    )(offsets, nodes, edges, w_in, w_out, rim)
    begun, upstream, w_node_back = call(
        prepare_node_kernel, [((N, W), F32), ((N, W), F32), square], [VMEM] * 5
    )(nodes, cot, w_node_in, w_node_out, local)
    arrived = arrivals(rim, local, xa, xb)
    dact, hidden_t, left, w_out_t, w_back = call(
        prepare_edge_kernel,
        [((K, N, W), F32), ((K * W, N), BF16), ((3 * W, K * N), BF16), square, ((2 * W, W), BF16)],
        [SMEM] + [VMEM] * 6,
        [PAD],
    )(offsets, preact, hidden, nodes, edges, w_in, w_out)
    local, xa, xb, gathered, slope, node_hidden = call(
        node_kernel, [(CUBE, F32)] + FACES + [((N, W), BF16)] * 3, [VMEM] * 13, [WORK]
    )(rim, local, *arrived, inverse, begun, upstream, w_node_in, w_node_back)
    arrived = arrivals(rim, local, xa, xb)
    node_grads, base = call(node_grads_kernel, [((3 * W, W), F32), ((N, W), F32)], [VMEM] * 6)(
        nodes, gathered, slope, node_hidden, cot, w_node_in
    )
    half = ((7 * W // 2, W), F32)
    slopes, keep, give = call(
        edge_kernel, [((K * N, W), BF16), half, half], [VMEM] * 13, [WORK, pltpu.VMEM((7 * W, W), F32)]
    )(rim, local, *arrived, dact, hidden_t, left, w_out_t, node_grads)
    local, za, zb = call(
        node_part_kernel, [(CUBE, F32)] + FACES, [SMEM] + [VMEM] * 4, [PAD]
    )(offsets, rim, slopes, base, w_back)
    (edge_grad,) = call(edge_grad_kernel, [((K * N, W), BF16)], [VMEM] * 2)(slopes, w_in)
    arrived, halves = arrivals_and_sum(rim, local, za, zb, keep, give)
    clipped = call(
        clip_kernel, [((3 * W, W), F32), ((W, W), F32), ((2 * W, W), F32), ((W, W), F32)], [VMEM] * 3
    )(rim, *halves)
    (node_grad,) = call(last_kernel, [((N, W), BF16)], [VMEM] * 8, [WORK])(rim, local, *arrived)
    return (node_grad.reshape(node_feat.shape), edge_grad.reshape(edge_feat.shape), *clipped)


def solution(mesh):
    split = Mesh(mesh.devices.reshape(8, 2, 2, 2, 4), ("z", "yh", "yl", "c", "x"))
    place = (GX, GY, GZ)
    placed = (
        P(*place, None),
        P(None, *place, None),
        P(*place),
        P(),
        P(),
        P(),
        P(),
        P(),
        P(*place, None),
    )

    return jax.shard_map(
        on_device,
        mesh=split,
        in_specs=placed,
        out_specs=(P(*place, None), P(None, *place, None), P(), P(), P(), P()),
        check_vma=False,
    )
```
